32 devices in a mesh: grp: 1 (over z), dz: 4 (over y), dy: 4 (over x), dx: 2 (over core).
Axes of the slice: x: 4, y: 4, z: 1, core: 2. Of those that a mesh axis runs over, the one named last changes fastest.
The devices are a block of a 4x4x8 slice.
Arguments:
- x_in: bfloat16 [6144, 7168], P(('grp', 'dx', 'dz'), 'dy')
- w_gate: bfloat16 [7168, 20480], P('dy', ('dz', 'dx'))
- w_up: bfloat16 [7168, 20480], P('dy', ('dz', 'dx'))
- w_down: bfloat16 [20480, 7168], P('dz', ('dy', 'dx'))
Outputs:
- output: bfloat16 [6144, 7168], P(('grp', 'dx', 'dz'), 'dy')
All inputs are finite; a program needn't handle non-finite values.
Results may differ from the reference program's by a relative error of at most 0.0124762.
Values are sent between devices in bfloat16 or wider.
A program may use at most 768 MiB of HBM per device.

```python
import jax
import jax.numpy as jnp
from jax import lax

N_ROWS = 6144
D_MODEL = 7168
D_FF = 20480
ROW_TILE = 768


def setup_inputs(seed: int = 0, part: int = 0) -> dict:
    base_key = jax.random.key(seed)
    key_x = jax.random.fold_in(jax.random.fold_in(base_key, 1), part)
    key_gate = jax.random.fold_in(base_key, 2)
    key_up = jax.random.fold_in(base_key, 3)
    key_down = jax.random.fold_in(base_key, 4)
    x_in = jax.random.normal(key_x, (N_ROWS, D_MODEL), jnp.float32).astype(jnp.bfloat16)
    w_gate = (jax.random.normal(key_gate, (D_MODEL, D_FF), jnp.float32) * D_MODEL ** -0.5).astype(jnp.bfloat16)
    w_up = (jax.random.normal(key_up, (D_MODEL, D_FF), jnp.float32) * D_MODEL ** -0.5).astype(jnp.bfloat16)
    w_down = (jax.random.normal(key_down, (D_FF, D_MODEL), jnp.float32) * D_FF ** -0.5).astype(jnp.bfloat16)
    return {"x_in": x_in, "w_gate": w_gate, "w_up": w_up, "w_down": w_down}


def reference(x_in, w_gate, w_up, w_down):
    def row_tile(x_tile):
        gate_val = jnp.dot(x_tile, w_gate, preferred_element_type=jnp.float32).astype(jnp.bfloat16)
        up_val = jnp.dot(x_tile, w_up, preferred_element_type=jnp.float32).astype(jnp.bfloat16)
        hidden = (jax.nn.silu(gate_val.astype(jnp.float32)) * up_val.astype(jnp.float32)).astype(jnp.bfloat16)
        return jnp.dot(hidden, w_down, preferred_element_type=jnp.float32).astype(jnp.bfloat16)
    x_tiles = x_in.reshape(N_ROWS // ROW_TILE, ROW_TILE, D_MODEL)
    return lax.map(row_tile, x_tiles).reshape(N_ROWS, D_MODEL)
```

```python
import jax
import jax.numpy as jnp
from jax import lax
from jax.sharding import PartitionSpec as P


def solution(mesh):
    x_spec = P(("grp", "dx", "dz"), "dy")
    w_in_spec = P("dy", ("dz", "dx"))
    w_out_spec = P("dz", ("dy", "dx"))

    def local_mlp(x_blk, wg_blk, wu_blk, wd_blk):
        wg = lax.all_to_all(wg_blk, "dy", split_axis=1, concat_axis=0, tiled=True)
        wu = lax.all_to_all(wu_blk, "dy", split_axis=1, concat_axis=0, tiled=True)
        wg = lax.all_gather(wg, "dx", axis=1, tiled=True)
        wu = lax.all_gather(wu, "dx", axis=1, tiled=True)
        x_full = lax.all_gather(x_blk, "dy", axis=1, tiled=True)
        x_rows = lax.all_gather(x_full, "dz", axis=0, tiled=True)
        gate = jnp.dot(x_rows, wg, preferred_element_type=jnp.float32)
        up = jnp.dot(x_rows, wu, preferred_element_type=jnp.float32)
        gate = gate.astype(jnp.bfloat16).astype(jnp.float32)
        up = up.astype(jnp.bfloat16).astype(jnp.float32)
        hidden = (jax.nn.silu(gate) * up).astype(jnp.bfloat16)
        n_dy, half = mesh.shape["dy"], wd_blk.shape[0] // mesh.shape["dx"]
        h_rows = lax.all_gather(hidden, "dy", axis=1, tiled=True)
        wd_cols = lax.all_gather(wd_blk, "dx", axis=1, tiled=True)
        sub = half // n_dy
        wd_perm = wd_cols.reshape(mesh.shape["dx"], n_dy, sub, -1).transpose(1, 0, 2, 3).reshape(wd_cols.shape)
        out_part = jnp.dot(h_rows, wd_perm, preferred_element_type=jnp.float32)
        out_sum = lax.psum_scatter(out_part, "dz", scatter_dimension=0, tiled=True)
        return out_sum.astype(jnp.bfloat16)

    return jax.shard_map(local_mlp, mesh=mesh, in_specs=(x_spec, w_in_spec, w_in_spec, w_out_spec), out_specs=x_spec, check_vma=False)
```

```python
import functools

import jax
import jax.numpy as jnp
from jax import lax
from jax.experimental import pallas as pl
from jax.experimental.pallas import tpu as pltpu
from jax.sharding import PartitionSpec as P

MESH = pl.DeviceIdType.MESH
RING = 4
H_SLOTS = 4
Z_SLOTS = 4
LAG = 2
XL, XS, XF, YL, YS, YF, WN, W2, WF, WL, SW, SD, P1 = 0, 2, 3, 5, 9, 13, 17, 19, 21, 23, 25, 33, 34


def _tile(extent, most):
    return next(t for t in range(most, 0, -128) if extent % t == 0)


def _kernel(mb, zb, x_in, wg_in, wu_in, wd_in, out, xg, wgu, ws, hg, wd, zin,
            xbuf, wbuf, hz, wdbuf, zinb, zout, ofin, hout,
            p1s, p1r, bin_s, bout_s, xsem, wsem, hzsem, wdsem, zinsem, osem,
            ols, olr, oss, osr, fs, fr, hws, zs, zr):
    rows, kb = x_in.shape
    hc = wg_in.shape[1] // RING
    nloc = wg_in.shape[1]
    hq = 2 * hc
    mc = wd_in.shape[1]
    tn = hout.shape[2]
    zn = zout.shape[2]
    nt = hq // tn
    nz = 2 * mc // zn
    ng = RING * nt
    zpi = -(-nz // (nt - 1))
    zstart = nt + 2

    b = lax.axis_index("dz")
    a = lax.axis_index("dy")
    c = lax.axis_index("dx")
    step = 1 - 2 * c
    al = lax.rem(a + step + RING, RING)
    ash = lax.rem(a - step + RING, RING)
    a2 = lax.rem(a + 2, RING)
    bl = lax.rem(b + step + RING, RING)
    bsh = lax.rem(b - step + RING, RING)
    xl, xs_ = {"dy": al}, {"dy": ash}
    yl, ys_ = {"dz": bl}, {"dz": bsh}
    sib = {"dx": 1 - c}
    kbs = (a, ash, al, a2)
    w_in = (wg_in, wu_in)

    def dest(s):
        return lax.rem(b - step * (1 + s) + 2 * RING, RING)

    def rc(src, dst, ss, rs, dev):
        return pltpu.make_async_remote_copy(src_ref=src, dst_ref=dst, send_sem=ss, recv_sem=rs, device_id=dev, device_id_type=MESH)

    def lanes(i, n):
        return pl.ds(pl.multiple_of(i * n, 128), n)

    def krows(k):
        return pl.ds(pl.multiple_of(k * kb, 16), kb)

    half = rows // 2

    def p1(i):
        sem = (p1s.at[i], p1r.at[i])
        if i < XS:
            r = pl.ds((i - XL) * half, half)
            return rc(x_in.at[r], xg.at[b, a, r], *sem, xl)
        if i < XF:
            return rc(x_in, xg.at[b, a], *sem, xs_)
        if i < YL:
            r = pl.ds((i - XF) * half, half)
            return rc(xg.at[b, ash, r], xg.at[b, ash, r], *sem, xl)
        if i < YF:
            j = (i - YL) % RING
            src = x_in if j == 0 else xg.at[b, kbs[j]]
            return rc(src, xg.at[b, kbs[j]], *sem, yl if i < YS else ys_)
        if i < WN:
            j = i - YF
            return rc(xg.at[bsh, kbs[j]], xg.at[bsh, kbs[j]], *sem, yl)
        if i < W2:
            u = i - WN
            return rc(w_in[u].at[:, lanes(ash, hc)], wgu.at[u, krows(a), lanes(c, hc)], *sem, xs_)
        if i < WF:
            u = i - W2
            return rc(w_in[u].at[:, lanes(a2, hc)], ws.at[u], *sem, xl)
        if i < WL:
            u = i - WF
            return rc(ws.at[u], wgu.at[u, krows(ash), lanes(c, hc)], *sem, xl)
        if i < SW:
            u = i - WL
            return rc(w_in[u].at[:, lanes(al, hc)], wgu.at[u, krows(a), lanes(c, hc)], *sem, xl)
        if i < SD:
            j, u = (i - SW) // 2, (i - SW) % 2
            dst = wgu.at[u, krows(kbs[j]), lanes(c, hc)]
            return rc(w_in[u].at[:, lanes(a, hc)] if j == 0 else dst, dst, *sem, sib)
        return rc(wd_in, wd.at[:, lanes(c, mc)], *sem, sib)

    def go(*idx):
        for i in idx:
            p1(i).start()

    def got(*idx):
        for i in idx:
            p1(i).wait_recv()

    barrier = pltpu.get_barrier_semaphore()
    for dev in (xl, xs_, yl, ys_, sib):
        pl.semaphore_signal(barrier, inc=1, device_id=dev, device_id_type=MESH)
    pl.semaphore_wait(barrier, 5)

    go(XL, XL + 1, XS, YL, YS, SD, SW, SW + 1, WN, WN + 1)

    moves = [(x_in, xg.at[b, a], xbuf.at[0, :, pl.ds(0, kb)])]
    col = kb
    for u in range(2):
        for r0 in range(0, kb, rows):
            n = min(rows, kb - r0)
            src = w_in[u].at[pl.ds(r0, n), lanes(a, hc)]
            dst = wgu.at[u, pl.ds(pl.multiple_of(a * kb + r0, 16), n), lanes(c, hc)]
            moves.append((src, dst, xbuf.at[0, pl.ds(0, n), pl.ds(col, hc)]))
            col += hc
    per = max(1, min(rows, wd_in.shape[0]))
    col = 0
    for r0 in range(0, wd_in.shape[0], per):
        n = min(per, wd_in.shape[0] - r0)
        moves.append((wd_in.at[pl.ds(r0, n)], wd.at[pl.ds(r0, n), lanes(c, mc)], xbuf.at[1, pl.ds(0, n), pl.ds(col, mc)]))
        col += mc
    for i, (src, _, mid) in enumerate(moves):
        pltpu.make_async_copy(src, mid, bin_s.at[i]).start()
    for i, (src, dst, mid) in enumerate(moves):
        pltpu.make_async_copy(src, mid, bin_s.at[i]).wait()
        pltpu.make_async_copy(mid, dst, bout_s.at[i]).start()
    zinb[...] = jnp.zeros_like(zinb)
    for i, (_, dst, mid) in enumerate(moves):
        pltpu.make_async_copy(mid, dst, bout_s.at[i]).wait()

    got(XL)
    go(XF)
    got(XL + 1)
    go(XF + 1, W2, W2 + 1, YL + 1)
    got(XS)
    go(YL + 2)
    got(YL)
    go(YF)
    got(XF, XF + 1)
    go(YL + 3, WL)
    got(YL + 1)
    go(YF + 1)
    got(W2)
    go(WF)
    got(W2 + 1)
    go(WF + 1, WL + 1)
    got(YL + 2)
    go(YF + 2)
    got(WN, WN + 1)
    go(SW + 4, SW + 5)
    got(YL + 3)
    go(YF + 3)
    got(YF, YF + 1)
    go(YS + 1)
    got(WL)
    go(SW + 2)
    got(WF)
    go(SW + 6)
    got(YF + 2)
    go(YS + 2)
    got(WF + 1)
    go(SW + 7)
    got(YF + 3)
    go(YS + 3)
    got(WL + 1)
    go(SW + 3)

    def x_load(s, k):
        return pltpu.make_async_copy(xg.at[dest(s), k], xbuf.at[lax.rem(s, 2), :, pl.ds(k * kb, kb)], xsem.at[lax.rem(s, 2), k])

    def w_load(g, u):
        slot = lax.rem(g, 2)
        return pltpu.make_async_copy(wgu.at[u, :, lanes(lax.rem(g, nt), tn)], wbuf.at[slot, :, pl.ds(u * tn, tn)], wsem.at[slot, u])

    def wd_load(z, i):
        slot, n = lax.rem(z, 2), lax.rem(z, nz)
        aa, cc = i // 2, i % 2
        src = wd.at[pl.ds(cc * nloc + aa * hc, hc), lanes(n, zn)]
        return pltpu.make_async_copy(src, wdbuf.at[slot, pl.ds(i * hc, hc)], wdsem.at[slot, i])

    def zin_load(z):
        return pltpu.make_async_copy(zin.at[z // nz - 1, lax.rem(z, nz)], zinb.at[lax.rem(z, 2)], zinsem.at[lax.rem(z, 2)])

    def h_write(g):
        slot = lax.rem(g, H_SLOTS)
        return pltpu.make_async_copy(hout.at[slot], hg.at[dest(g // nt), a, lax.rem(g, nt)], hws.at[slot])

    def h_long(g):
        slot = lax.rem(g, H_SLOTS)
        return rc(hout.at[slot], hg.at[dest(g // nt), a, lax.rem(g, nt)], ols.at[slot], olr.at[g], xl)

    def h_short(g):
        slot = lax.rem(g, H_SLOTS)
        return rc(hout.at[slot], hg.at[dest(g // nt), a, lax.rem(g, nt)], oss.at[slot], osr.at[g], xs_)

    def h_fwd(g):
        blk = hg.at[dest(g // nt), ash, lax.rem(g, nt)]
        return rc(blk, blk, fs.at[g], fr.at[g], xl)

    def z_send(z):
        slot = lax.rem(z, Z_SLOTS)
        return rc(zout.at[slot], zin.at[z // nz, lax.rem(z, nz)], zs.at[slot], zr.at[z], yl)

    def o_write(z):
        slot = lax.rem(z, 2)
        return pltpu.make_async_copy(ofin.at[slot], out.at[:, lanes(lax.rem(z, nz), zn)], osem.at[slot])

    def start_w(g):
        w_load(g, 0).start()
        w_load(g, 1).start()

    for k in range(RING):
        x_load(0, k).start()
    got(*range(SW, SD + 1))
    start_w(0)
    for i in range(8):
        wd_load(0, i).start()

    def z_tile(z, carry):
        s, slot = z // nz, lax.rem(z, 2)

        @pl.when(z + 1 < RING * nz)
        def _():
            for i in range(8):
                wd_load(z + 1, i).start()

        @pl.when((z + 1 >= nz) & (z + 1 < RING * nz))
        def _():
            z_send(z + 1 - nz).wait_recv()
            zin_load(z + 1).start()

        for i in range(8):
            wd_load(z, i).wait()

        @pl.when(s > 0)
        def _():
            zin_load(z).wait()

        @pl.when((z >= Z_SLOTS) & (z - Z_SLOTS < (RING - 1) * nz))
        def _():
            z_send(z - Z_SLOTS).wait_send()

        @pl.when(z - 2 >= (RING - 1) * nz)
        def _():
            o_write(z - 2).wait()

        zslot = lax.rem(z, Z_SLOTS)

        def part(m, carry):
            r = pl.ds(pl.multiple_of(m * zb, zb), zb)
            acc = jnp.dot(hz[r, :], wdbuf[slot], preferred_element_type=jnp.float32) + zinb[slot, r, :]
            zout[zslot, r, :] = acc
            ofin[slot, r, :] = acc.astype(jnp.bfloat16)
            return carry

        lax.fori_loop(0, rows // zb, part, 0)

        @pl.when(s < RING - 1)
        def _():
            z_send(z).start()

        @pl.when(s == RING - 1)
        def _():
            o_write(z).start()

        return carry

    def body(g, carry):
        s, t = g // nt, lax.rem(g, nt)

        @pl.when(g < ng)
        def _():
            @pl.when(g + 1 < ng)
            def _():
                start_w(g + 1)

            @pl.when((t == nt - 1) & (g + 1 < ng))
            def _():
                @pl.when(s + 1 == 2)
                def _():
                    got(*range(YS, YF))

                for k in range(RING):
                    x_load(s + 1, k).start()

            @pl.when(t == 0)
            def _():
                for k in range(RING):
                    x_load(s, k).wait()

            w_load(g, 0).wait()
            w_load(g, 1).wait()

            @pl.when(g >= H_SLOTS)
            def _():
                h_long(g - H_SLOTS).wait_send()
                h_short(g - H_SLOTS).wait_send()

            xslot, wslot, hslot = lax.rem(s, 2), lax.rem(g, 2), lax.rem(g, H_SLOTS)

            def part(m, carry):
                r = pl.ds(pl.multiple_of(m * mb, mb), mb)
                gu = jnp.dot(xbuf[xslot, r, :], wbuf[wslot], preferred_element_type=jnp.float32)
                gate = gu[:, :tn].astype(jnp.bfloat16).astype(jnp.float32)
                up = gu[:, tn:].astype(jnp.bfloat16).astype(jnp.float32)
                hout[hslot, r, :] = (jax.nn.silu(gate) * up).astype(jnp.bfloat16)
                return carry

            lax.fori_loop(0, rows // mb, part, 0)
            h_long(g).start()
            h_short(g).start()
            h_write(g).start()

        @pl.when((g >= 1) & (g <= ng))
        def _():
            h_write(g - 1).wait()

        q = jnp.maximum(g - zstart, 0)
        zs_, r_ = q // nt, lax.rem(q, nt)
        lo = jnp.where(g < zstart, 0, nz * zs_ + jnp.minimum(zpi * r_, nz))
        hi = jnp.where(g < zstart, 0, nz * zs_ + jnp.minimum(zpi * (r_ + 1), nz))

        @pl.when((g >= zstart) & (r_ == 0))
        def _():
            def arrived(j, carry):
                h_short(zs_ * nt + j).wait_recv()
                h_fwd(zs_ * nt + j).wait_recv()
                return carry

            lax.fori_loop(0, nt, arrived, 0)

            def piece(i):
                return pltpu.make_async_copy(hg.at[dest(zs_), i // nt, lax.rem(i, nt)], hz.at[:, lanes(i, tn)], hzsem.at[i])

            def fetch(i, carry):
                piece(i).start()
                return carry

            def fetched(i, carry):
                piece(i).wait()
                return carry

            lax.fori_loop(0, RING * nt, fetch, 0)
            lax.fori_loop(0, RING * nt, fetched, 0)

        lax.fori_loop(lo, hi, z_tile, 0)

        @pl.when((g >= LAG) & (g - LAG < ng))
        def _():
            h_long(g - LAG).wait_recv()
            h_fwd(g - LAG).start()

        return carry

    lax.fori_loop(0, zstart + (RING - 1) * nt + -(-nz // zpi), body, 0)

    for z in range(RING * nz - 2, RING * nz):
        o_write(z).wait()
    for i in range(P1):
        p1(i).wait_send()
    for g in range(ng - H_SLOTS, ng):
        h_long(g).wait_send()
        h_short(g).wait_send()

    def drain(g, carry):
        h_fwd(g).wait_send()
        return carry

    lax.fori_loop(0, ng, drain, 0)
    for z in range(max(0, RING * nz - Z_SLOTS), (RING - 1) * nz):
        z_send(z).wait_send()


def _local(x_blk, wg_blk, wu_blk, wd_blk):
    rows, kb = x_blk.shape
    hc = wg_blk.shape[1] // RING
    mc = wd_blk.shape[1]
    tn, zn = _tile(2 * hc, 256), _tile(2 * mc, 256)
    nt, nz = 2 * hc // tn, 2 * mc // zn
    n_moves = 1 + 2 * -(-kb // rows) + -(-wd_blk.shape[0] // rows)
    bf16, f32 = jnp.bfloat16, jnp.float32
    hbm = pl.BlockSpec(memory_space=pl.ANY)
    mb = rows // 2 if rows % 256 == 0 else rows
    zb = mb
    dma = pltpu.SemaphoreType.DMA
    flops = 2 * RING * rows * (RING * kb * 4 * hc + wd_blk.shape[0] * 2 * mc)
    res = pl.pallas_call(
        functools.partial(_kernel, mb, zb),
        name="ring_mlp",
        out_shape=(
            jax.ShapeDtypeStruct((rows, 2 * mc), bf16),
            jax.ShapeDtypeStruct((RING, RING, rows, kb), bf16),
            jax.ShapeDtypeStruct((2, RING * kb, 2 * hc), bf16),
            jax.ShapeDtypeStruct((2, kb, hc), bf16),
            jax.ShapeDtypeStruct((RING, RING, nt, rows, tn), bf16),
            jax.ShapeDtypeStruct((wd_blk.shape[0], 2 * mc), bf16),
            jax.ShapeDtypeStruct((RING - 1, nz, rows, zn), f32),
        ),
        in_specs=[hbm] * 4,
        out_specs=(hbm,) * 7,
        scratch_shapes=[
            pltpu.VMEM((2, rows, RING * kb), bf16),
            pltpu.VMEM((2, RING * kb, 2 * tn), bf16),
            pltpu.VMEM((rows, wd_blk.shape[0]), bf16),
            pltpu.VMEM((2, wd_blk.shape[0], zn), bf16),
            pltpu.VMEM((2, rows, zn), f32),
            pltpu.VMEM((Z_SLOTS, rows, zn), f32),
            pltpu.VMEM((2, rows, zn), bf16),
            pltpu.VMEM((H_SLOTS, rows, tn), bf16),
            dma((P1,)), dma((P1,)), dma((n_moves,)), dma((n_moves,)),
            dma((2, RING)), dma((2, 2)), dma((RING * nt,)), dma((2, 8)), dma((2,)), dma((2,)),
            dma((H_SLOTS,)), dma((RING * nt,)), dma((H_SLOTS,)), dma((RING * nt,)),
            dma((RING * nt,)), dma((RING * nt,)), dma((H_SLOTS,)),
            dma((Z_SLOTS,)), dma(((RING - 1) * nz,)),
        ],
        compiler_params=pltpu.CompilerParams(collective_id=0, has_side_effects=True, vmem_limit_bytes=67043328),
        cost_estimate=pl.CostEstimate(flops=flops, bytes_accessed=flops // 500, transcendentals=0),
    )(x_blk, wg_blk, wu_blk, wd_blk)
    return res[0]


def solution(mesh):
    assert mesh.shape["dz"] == RING and mesh.shape["dy"] == RING and mesh.shape["dx"] == 2
    x_spec = P(("grp", "dx", "dz"), "dy")
    w_in_spec = P("dy", ("dz", "dx"))
    w_out_spec = P("dz", ("dy", "dx"))
    return jax.shard_map(_local, mesh=mesh, in_specs=(x_spec, w_in_spec, w_in_spec, w_out_spec), out_specs=x_spec, check_vma=False)
```

```python
import functools

import jax
import jax.numpy as jnp
from jax import lax
from jax.experimental import pallas as pl
from jax.experimental.pallas import tpu as pltpu
from jax.sharding import PartitionSpec as P

MESH = pl.DeviceIdType.MESH
RING = 4
H_SLOTS = 8
Z_SLOTS = 6
XL, XS, XF, YL, YS, YF, WN, W2, WF, WL, SW, SD, P1 = 0, 2, 3, 5, 9, 13, 17, 21, 25, 29, 33, 49, 50


def _tile(extent, most):
    return next(t for t in range(most, 0, -128) if extent % t == 0)


def _kernel(mb, zb, x_in, wg_in, wu_in, wd_in, out, xg, wgu, ws, hg, wd, zin,
            xbuf, wbuf, hz, wdbuf, zinb, zout, ofin, hout,
            p1s, p1r, bin_s, bout_s, xsem, wsem, hzsem, wdsem, zinsem, osem,
            ols, olr, oss, osr, fs, fr, hws, zs, zr):
    rows, kb = x_in.shape
    hc = wg_in.shape[1] // RING
    nloc = wg_in.shape[1]
    hq = 2 * hc
    mc = wd_in.shape[1]
    tn = hout.shape[2]
    zn = zout.shape[2]
    nt = hq // tn
    nz = 2 * mc // zn
    ng = RING * nt
    zpi = -(-nz // (nt - 1))
    zstart = nt + 2
    early = (nt + 1) // 2
    pc = (early * tn // 2, hc - early * tn // 2)
    p_src, p_dst = (0, pc[0]), (0, 2 * pc[0])

    b = lax.axis_index("dz")
    a = lax.axis_index("dy")
    c = lax.axis_index("dx")
    step = 1 - 2 * c
    al = lax.rem(a + step + RING, RING)
    ash = lax.rem(a - step + RING, RING)
    a2 = lax.rem(a + 2, RING)
    bl = lax.rem(b + step + RING, RING)
    bsh = lax.rem(b - step + RING, RING)
    xl, xs_ = {"dy": al}, {"dy": ash}
    yl, ys_ = {"dz": bl}, {"dz": bsh}
    sib = {"dx": 1 - c}
    kbs = (a, ash, al, a2)
    w_in = (wg_in, wu_in)

    def dest(s):
        return lax.rem(b - step * (1 + s) + 2 * RING, RING)

    def rc(src, dst, ss, rs, dev):
        return pltpu.make_async_remote_copy(src_ref=src, dst_ref=dst, send_sem=ss, recv_sem=rs, device_id=dev, device_id_type=MESH)

    def lanes(i, n):
        return pl.ds(pl.multiple_of(i * n, 128), n)

    def krows(k):
        return pl.ds(pl.multiple_of(k * kb, 16), kb)

    half = rows // 2

    def w_piece(u, p, q):
        return w_in[u].at[:, pl.ds(pl.multiple_of(q * hc + p_src[p], 128), pc[p])]

    def w_place(u, p, k):
        return wgu.at[u, krows(k), pl.ds(pl.multiple_of(p_dst[p] + c * pc[p], 128), pc[p])]

    def p1(i):
        sem = (p1s.at[i], p1r.at[i])
        if i < XS:
            r = pl.ds((i - XL) * half, half)
            return rc(x_in.at[r], xg.at[b, a, r], *sem, xl)
        if i < XF:
            return rc(x_in, xg.at[b, a], *sem, xs_)
        if i < YL:
            r = pl.ds((i - XF) * half, half)
            return rc(xg.at[b, ash, r], xg.at[b, ash, r], *sem, xl)
        if i < YF:
            j = (i - YL) % RING
            src = x_in if j == 0 else xg.at[b, kbs[j]]
            return rc(src, xg.at[b, kbs[j]], *sem, yl if i < YS else ys_)
        if i < WN:
            j = i - YF
            return rc(xg.at[bsh, kbs[j]], xg.at[bsh, kbs[j]], *sem, yl)
        if i < WF:
            u, p = (i - WN) % 2, (i - WN) % 4 // 2
            if i < W2:
                return rc(w_piece(u, p, ash), w_place(u, p, a), *sem, xs_)
            return rc(w_piece(u, p, a2), ws.at[u, :, pl.ds(p_src[p], pc[p])], *sem, xl)
        if i < WL:
            u, p = (i - WF) % 2, (i - WF) // 2
            return rc(ws.at[u, :, pl.ds(p_src[p], pc[p])], w_place(u, p, ash), *sem, xl)
        if i < SW:
            u, p = (i - WL) % 2, (i - WL) // 2
            return rc(w_piece(u, p, al), w_place(u, p, a), *sem, xl)
        if i < SD:
            j, p, u = (i - SW) // 4, (i - SW) % 4 // 2, (i - SW) % 2
            dst = w_place(u, p, kbs[j])
            return rc(w_piece(u, p, a) if j == 0 else dst, dst, *sem, sib)
        return rc(wd_in, wd.at[:, lanes(c, mc)], *sem, sib)

    def go(*idx):
        for i in idx:
            p1(i).start()

    def got(*idx):
        for i in idx:
            with jax.named_scope(f"got{i}"):
                p1(i).wait_recv()

    barrier = pltpu.get_barrier_semaphore()
    for dev in (xl, xs_, yl, ys_, sib):
        pl.semaphore_signal(barrier, inc=1, device_id=dev, device_id_type=MESH)
    with jax.named_scope("barrier"):
        pl.semaphore_wait(barrier, 5)

    go(XL, XL + 1, XS, YL, YS, SD, SW, SW + 1, SW + 2, SW + 3, WN, WN + 1)

    moves = [(x_in, xg.at[b, a], xbuf.at[0, :, pl.ds(0, kb)])]
    col = kb
    for u in range(2):
        for r0 in range(0, kb, rows):
            n = min(rows, kb - r0)
            for p in range(2):
                src = w_in[u].at[pl.ds(r0, n), pl.ds(pl.multiple_of(a * hc + p_src[p], 128), pc[p])]
                dst = wgu.at[u, pl.ds(pl.multiple_of(a * kb + r0, 16), n), pl.ds(pl.multiple_of(p_dst[p] + c * pc[p], 128), pc[p])]
                moves.append((src, dst, xbuf.at[0, pl.ds(0, n), pl.ds(col, pc[p])]))
                col += pc[p]
    per = max(1, min(rows, wd_in.shape[0]))
    col = 0
    for r0 in range(0, wd_in.shape[0], per):
        n = min(per, wd_in.shape[0] - r0)
        moves.append((wd_in.at[pl.ds(r0, n)], wd.at[pl.ds(r0, n), lanes(c, mc)], xbuf.at[1, pl.ds(0, n), pl.ds(col, mc)]))
        col += mc
    for i, (src, _, mid) in enumerate(moves):
        pltpu.make_async_copy(src, mid, bin_s.at[i]).start()
    with jax.named_scope("bounce"):
        for i, (src, dst, mid) in enumerate(moves):
            pltpu.make_async_copy(src, mid, bin_s.at[i]).wait()
            pltpu.make_async_copy(mid, dst, bout_s.at[i]).start()
        zinb[...] = jnp.zeros_like(zinb)
        for i, (_, dst, mid) in enumerate(moves):
            pltpu.make_async_copy(mid, dst, bout_s.at[i]).wait()

    got(XL)
    go(XF)
    got(XL + 1)
    go(XF + 1, W2, W2 + 1, YL + 1)
    got(XS)
    go(YL + 2, WN + 2, WN + 3)
    got(YL)
    go(YF)
    got(XF, XF + 1)
    go(YL + 3, WL)
    got(YL + 1)
    go(YF + 1)
    got(W2)
    go(WF)
    got(W2 + 1)
    go(WF + 1, WL + 1, W2 + 2, W2 + 3)
    got(YL + 2)
    go(YF + 2)
    got(WN, WN + 1)
    go(SW + 8, SW + 9)
    got(YL + 3)
    go(YF + 3)
    got(WL)
    go(SW + 4)
    got(WF, WF + 1)
    go(SW + 12, SW + 13)
    got(WL + 1)
    go(SW + 5, WL + 2, YS + 1)
    got(W2 + 2)
    go(WF + 2)
    got(W2 + 3)
    go(WF + 3, WL + 3)

    def x_load(s, k):
        return pltpu.make_async_copy(xg.at[dest(s), k], xbuf.at[lax.rem(s, 2), :, pl.ds(k * kb, kb)], xsem.at[lax.rem(s, 2), k])

    def w_load(g, u):
        slot = lax.rem(g, 2)
        return pltpu.make_async_copy(wgu.at[u, :, lanes(lax.rem(g, nt), tn)], wbuf.at[slot, :, pl.ds(u * tn, tn)], wsem.at[slot, u])

    def wd_load(z, i):
        slot, n = lax.rem(z, 2), lax.rem(z, nz)
        aa, p, cc = i // 4, i % 4 // 2, i % 2
        src = wd.at[pl.ds(cc * nloc + aa * hc + p_src[p], pc[p]), lanes(n, zn)]
        return pltpu.make_async_copy(src, wdbuf.at[slot, pl.ds(aa * hq + p_dst[p] + cc * pc[p], pc[p])], wdsem.at[slot, i])

    def zin_load(z):
        return pltpu.make_async_copy(zin.at[z // nz - 1, lax.rem(z, nz)], zinb.at[lax.rem(z, 2)], zinsem.at[lax.rem(z, 2)])

    def h_write(g):
        slot = lax.rem(g, H_SLOTS)
        return pltpu.make_async_copy(hout.at[slot], hg.at[dest(g // nt), a, lax.rem(g, nt)], hws.at[slot])

    def h_long(g):
        slot = lax.rem(g, H_SLOTS)
        return rc(hout.at[slot], hg.at[dest(g // nt), a, lax.rem(g, nt)], ols.at[slot], olr.at[g], xl)

    def h_short(g):
        slot = lax.rem(g, H_SLOTS)
        return rc(hout.at[slot], hg.at[dest(g // nt), a, lax.rem(g, nt)], oss.at[slot], osr.at[g], xs_)

    def h_fwd(g):
        blk = hg.at[dest(g // nt), ash, lax.rem(g, nt)]
        return rc(blk, blk, fs.at[g], fr.at[g], xl)

    def z_send(z):
        slot = lax.rem(z, Z_SLOTS)
        return rc(zout.at[slot], zin.at[z // nz, lax.rem(z, nz)], zs.at[slot], zr.at[z], yl)

    def o_write(z):
        slot = lax.rem(z, 2)
        return pltpu.make_async_copy(ofin.at[slot], out.at[:, lanes(lax.rem(z, nz), zn)], osem.at[slot])

    def start_w(g):
        w_load(g, 0).start()
        w_load(g, 1).start()

    for k in range(RING):
        x_load(0, k).start()
    got(*(SW + 4 * j + u for j in range(RING) for u in range(2)))
    start_w(0)

    def z_tile(z, carry):
        s, slot = z // nz, lax.rem(z, 2)

        @pl.when(z + 1 < RING * nz)
        def _():
            for i in range(16):
                wd_load(z + 1, i).start()

        with jax.named_scope("zinrecv"):
            @pl.when((z + 1 >= nz) & (z + 1 < RING * nz))
            def _():
                z_send(z + 1 - nz).wait_recv()
                zin_load(z + 1).start()

        with jax.named_scope("wdwait"):
            for i in range(16):
                wd_load(z, i).wait()

        with jax.named_scope("zinwait"):
            @pl.when(s > 0)
            def _():
                zin_load(z).wait()

        with jax.named_scope("zslot"):
            @pl.when((z >= Z_SLOTS) & (s < RING - 1))
            def _():
                z_send(z - Z_SLOTS).wait_send()

        @pl.when(z - 2 >= (RING - 1) * nz)
        def _():
            o_write(z - 2).wait()

        zslot = jnp.where(s < RING - 1, lax.rem(z, Z_SLOTS), Z_SLOTS)

        def part(m, carry):
            r = pl.ds(pl.multiple_of(m * zb, zb), zb)
            acc = jnp.dot(hz[r, :], wdbuf[slot], preferred_element_type=jnp.float32) + zinb[slot, r, :]
            zout[zslot, r, :] = acc
            ofin[slot, r, :] = acc.astype(jnp.bfloat16)
            return carry

        with jax.named_scope("zmm"):
            lax.fori_loop(0, rows // zb, part, 0)

        @pl.when(s < RING - 1)
        def _():
            z_send(z).start()

        @pl.when(s == RING - 1)
        def _():
            o_write(z).start()

        return carry

    def body(g, carry):
        s, t = g // nt, lax.rem(g, nt)

        @pl.when(g == early - 1)
        def _():
            got(WN + 2, WN + 3)
            go(SW + 10, SW + 11)
            got(WL + 2)
            go(SW + 6)
            got(WF + 2)
            go(SW + 14)

        @pl.when(g == early)
        def _():
            got(WF + 3)
            go(SW + 15)
            got(WL + 3)
            go(SW + 7, YS + 2, YS + 3)

            def first(j, carry):
                h_long(j).wait_recv()
                h_fwd(j).start()
                return carry

            lax.fori_loop(0, early, first, 0)
            got(*(SW + 4 * j + 2 + u for j in range(RING) for u in range(2)), SD)
            start_w(g)
            for i in range(16):
                wd_load(0, i).start()

        @pl.when(g < ng)
        def _():
            @pl.when((g + 1 < ng) & (g + 1 != early))
            def _():
                start_w(g + 1)

            @pl.when((t == nt - 1) & (g + 1 < ng))
            def _():
                @pl.when(s + 1 == 1)
                def _():
                    got(*range(YF, WN))

                @pl.when(s + 1 == 2)
                def _():
                    got(*range(YS, YF))

                for k in range(RING):
                    x_load(s + 1, k).start()

            with jax.named_scope("xwait"):
                @pl.when(t == 0)
                def _():
                    for k in range(RING):
                        x_load(s, k).wait()

            with jax.named_scope("wwait"):
                w_load(g, 0).wait()
                w_load(g, 1).wait()

            with jax.named_scope("hslot"):
                @pl.when(g >= H_SLOTS)
                def _():
                    h_long(g - H_SLOTS).wait_send()
                    h_short(g - H_SLOTS).wait_send()

            xslot, wslot, hslot = lax.rem(s, 2), lax.rem(g, 2), lax.rem(g, H_SLOTS)

            def part(m, carry):
                r = pl.ds(pl.multiple_of(m * mb, mb), mb)
                gu = jnp.dot(xbuf[xslot, r, :], wbuf[wslot], preferred_element_type=jnp.float32)
                gate = gu[:, :tn].astype(jnp.bfloat16).astype(jnp.float32)
                up = gu[:, tn:].astype(jnp.bfloat16).astype(jnp.float32)
                hout[hslot, r, :] = (jax.nn.silu(gate) * up).astype(jnp.bfloat16)
                return carry

            with jax.named_scope("gumm"):
                lax.fori_loop(0, rows // mb, part, 0)
            h_long(g).start()
            h_short(g).start()
            h_write(g).start()

        @pl.when((g >= 1) & (g <= ng))
        def _():
            h_write(g - 1).wait()

        last = g == ng + 1
        q = jnp.maximum(g - zstart, 0)
        zs_ = jnp.where(last, RING - 1, q // nt)
        r_ = jnp.where(last, 0, lax.rem(q, nt))
        live = (g >= zstart) & ((zs_ < RING - 1) | last)
        lo = jnp.where(live, nz * zs_ + jnp.minimum(zpi * r_, nz), 0)
        hi = jnp.where(live, jnp.where(last, RING * nz, nz * zs_ + jnp.minimum(zpi * (r_ + 1), nz)), 0)

        @pl.when(live & (r_ == 0))
        def _():
            def piece(j, k):
                return pltpu.make_async_copy(hg.at[dest(zs_), k, j], hz.at[:, lanes(k * nt + j, tn)], hzsem.at[k, j])

            def fetch(j, carry):
                h_short(zs_ * nt + j).wait_recv()
                h_fwd(zs_ * nt + j).wait_recv()
                for k in range(RING):
                    piece(j, k).start()
                return carry

            def fetched(j, carry):
                for k in range(RING):
                    piece(j, k).wait()
                return carry

            with jax.named_scope("harr"):
                lax.fori_loop(0, nt, fetch, 0)
            with jax.named_scope("hzload"):
                lax.fori_loop(0, nt, fetched, 0)

        lax.fori_loop(lo, hi, z_tile, 0)

        with jax.named_scope("fwd"):
            @pl.when((g > early) & (g <= ng))
            def _():
                h_long(g - 1).wait_recv()
                h_fwd(g - 1).start()

        return carry

    lax.fori_loop(0, ng + 2, body, 0)

    with jax.named_scope("owait"):
        for z in range(RING * nz - 2, RING * nz):
            o_write(z).wait()
    for i in range(P1):
        p1(i).wait_send()
    for g in range(ng - H_SLOTS, ng):
        h_long(g).wait_send()
        h_short(g).wait_send()

    def drain(g, carry):
        h_fwd(g).wait_send()
        return carry

    lax.fori_loop(0, ng, drain, 0)
    for z in range(max(0, (RING - 1) * nz - Z_SLOTS), (RING - 1) * nz):
        z_send(z).wait_send()


def _local(x_blk, wg_blk, wu_blk, wd_blk):
    rows, kb = x_blk.shape
    hc = wg_blk.shape[1] // RING
    mc = wd_blk.shape[1]
    tn, zn = _tile(2 * hc, 256), _tile(2 * mc, 256)
    nt, nz = 2 * hc // tn, 2 * mc // zn
    n_moves = 1 + 4 * -(-kb // rows) + -(-wd_blk.shape[0] // rows)
    bf16, f32 = jnp.bfloat16, jnp.float32
    hbm = pl.BlockSpec(memory_space=pl.ANY)
    mb = rows // 2 if rows % 256 == 0 else rows
    zb = mb
    dma = pltpu.SemaphoreType.DMA
    flops = 2 * RING * rows * (RING * kb * 4 * hc + wd_blk.shape[0] * 2 * mc)
    res = pl.pallas_call(
        functools.partial(_kernel, mb, zb),
        name="ring_mlp",
        out_shape=(
            jax.ShapeDtypeStruct((rows, 2 * mc), bf16),
            jax.ShapeDtypeStruct((RING, RING, rows, kb), bf16),
            jax.ShapeDtypeStruct((2, RING * kb, 2 * hc), bf16),
            jax.ShapeDtypeStruct((2, kb, hc), bf16),
            jax.ShapeDtypeStruct((RING, RING, nt, rows, tn), bf16),
            jax.ShapeDtypeStruct((wd_blk.shape[0], 2 * mc), bf16),
            jax.ShapeDtypeStruct((RING - 1, nz, rows, zn), f32),
        ),
        in_specs=[hbm] * 4,
        out_specs=(hbm,) * 7,
        scratch_shapes=[
            pltpu.VMEM((2, rows, RING * kb), bf16),
            pltpu.VMEM((2, RING * kb, 2 * tn), bf16),
            pltpu.VMEM((rows, wd_blk.shape[0]), bf16),
            pltpu.VMEM((2, wd_blk.shape[0], zn), bf16),
            pltpu.VMEM((2, rows, zn), f32),
            pltpu.VMEM((Z_SLOTS + 1, rows, zn), f32),
            pltpu.VMEM((2, rows, zn), bf16),
            pltpu.VMEM((H_SLOTS, rows, tn), bf16),
            dma((P1,)), dma((P1,)), dma((n_moves,)), dma((n_moves,)),
            dma((2, RING)), dma((2, 2)), dma((RING, nt)), dma((2, 16)), dma((2,)), dma((2,)),
            dma((H_SLOTS,)), dma((RING * nt,)), dma((H_SLOTS,)), dma((RING * nt,)),
            dma((RING * nt,)), dma((RING * nt,)), dma((H_SLOTS,)),
            dma((Z_SLOTS,)), dma(((RING - 1) * nz,)),
        ],
        compiler_params=pltpu.CompilerParams(collective_id=0, has_side_effects=True, vmem_limit_bytes=67043328),
        cost_estimate=pl.CostEstimate(flops=flops, bytes_accessed=flops // 500, transcendentals=0),
    )(x_blk, wg_blk, wu_blk, wd_blk)
    return res[0]


def solution(mesh):
    assert mesh.shape["dz"] == RING and mesh.shape["dy"] == RING and mesh.shape["dx"] == 2
    x_spec = P(("grp", "dx", "dz"), "dy")
    w_in_spec = P("dy", ("dz", "dx"))
    w_out_spec = P("dz", ("dy", "dx"))
    return jax.shard_map(_local, mesh=mesh, in_specs=(x_spec, w_in_spec, w_in_spec, w_out_spec), out_specs=x_spec, check_vma=False)
```

```python
import jax
import jax.numpy as jnp
from jax import lax
from jax.experimental import pallas as pl
from jax.experimental.pallas import tpu as pltpu
from jax.sharding import PartitionSpec as P

MESH = pl.DeviceIdType.MESH
RING = 4
H_SLOTS = 10
Z_SLOTS = 8
AHEAD = 4
XL, XS, XF, YL, YS, YF, WN, W2, WF, WL, SW, SD, P1 = 0, 2, 3, 5, 9, 13, 17, 21, 25, 29, 33, 49, 50


def _tile(extent, most):
    return next(t for t in range(most, 0, -128) if extent % t == 0)


def _kernel(x_in, wg_in, wu_in, wd_in, out, xg, wgu, ws, hg, wd, zin,
            xbuf, wbuf, hz, wdbuf, zinb, zout, ofin, hout,
            p1s, p1r, bin_s, bout_s, xsem, wsem, hzsem, wdsem, zinsem, osem,
            ols, olr, oss, osr, fs, fr, hws, zs, zr):
    rows, kb = x_in.shape
    hc = wg_in.shape[1] // RING
    nloc = wg_in.shape[1]
    hq = 2 * hc
    mc = wd_in.shape[1]
    part_rows, tn = hout.shape[2:]
    zn = zout.shape[2]
    nt = hq // tn
    nz = 2 * mc // zn
    ng = RING * nt
    ni = 2 * ng
    zstart = nt + 2
    early = (nt + 1) // 2
    pc = (early * tn // 2, hc - early * tn // 2)
    p_src, p_dst = (0, pc[0]), (0, 2 * pc[0])

    b = lax.axis_index("dz")
    a = lax.axis_index("dy")
    c = lax.axis_index("dx")
    step = 1 - 2 * c
    al = lax.rem(a + step + RING, RING)
    ash = lax.rem(a - step + RING, RING)
    a2 = lax.rem(a + 2, RING)
    bl = lax.rem(b + step + RING, RING)
    bsh = lax.rem(b - step + RING, RING)
    xl, xs_ = {"dy": al}, {"dy": ash}
    yl, ys_ = {"dz": bl}, {"dz": bsh}
    sib = {"dx": 1 - c}
    kbs = (a, ash, al, a2)
    w_in = (wg_in, wu_in)

    def dest(s):
        return lax.rem(b - step * (1 + s) + 2 * RING, RING)

    def rc(src, dst, ss, rs, dev):
        return pltpu.make_async_remote_copy(src_ref=src, dst_ref=dst, send_sem=ss, recv_sem=rs, device_id=dev, device_id_type=MESH)

    def lanes(i, n):
        return pl.ds(pl.multiple_of(i * n, 128), n)

    def krows(k):
        return pl.ds(pl.multiple_of(k * kb, 16), kb)

    half = rows // 2

    def w_piece(u, p, q):
        return w_in[u].at[:, pl.ds(pl.multiple_of(q * hc + p_src[p], 128), pc[p])]

    def w_place(u, p, k):
        return wgu.at[u, krows(k), pl.ds(pl.multiple_of(p_dst[p] + c * pc[p], 128), pc[p])]

    def p1(i):
        sem = (p1s.at[i], p1r.at[i])
        if i < XS:
            r = pl.ds((i - XL) * half, half)
            return rc(x_in.at[r], xg.at[b, a, r], *sem, xl)
        if i < XF:
            return rc(x_in, xg.at[b, a], *sem, xs_)
        if i < YL:
            r = pl.ds((i - XF) * half, half)
            return rc(xg.at[b, ash, r], xg.at[b, ash, r], *sem, xl)
        if i < YF:
            j = (i - YL) % RING
            src = x_in if j == 0 else xg.at[b, kbs[j]]
            return rc(src, xg.at[b, kbs[j]], *sem, yl if i < YS else ys_)
        if i < WN:
            j = i - YF
            return rc(xg.at[bsh, kbs[j]], xg.at[bsh, kbs[j]], *sem, yl)
        if i < WF:
            u, p = (i - WN) % 2, (i - WN) % 4 // 2
            if i < W2:
                return rc(w_piece(u, p, ash), w_place(u, p, a), *sem, xs_)
            return rc(w_piece(u, p, a2), ws.at[u, :, pl.ds(p_src[p], pc[p])], *sem, xl)
        if i < WL:
            u, p = (i - WF) % 2, (i - WF) // 2
            return rc(ws.at[u, :, pl.ds(p_src[p], pc[p])], w_place(u, p, ash), *sem, xl)
        if i < SW:
            u, p = (i - WL) % 2, (i - WL) // 2
            return rc(w_piece(u, p, al), w_place(u, p, a), *sem, xl)
        if i < SD:
            j, p, u = (i - SW) // 4, (i - SW) % 4 // 2, (i - SW) % 2
            dst = w_place(u, p, kbs[j])
            return rc(w_piece(u, p, a) if j == 0 else dst, dst, *sem, sib)
        return rc(wd_in, wd.at[:, lanes(c, mc)], *sem, sib)

    def go(*idx):
        for i in idx:
            p1(i).start()

    def got(*idx):
        for i in idx:
            with jax.named_scope(f"got{i}"):
                p1(i).wait_recv()

    barrier = pltpu.get_barrier_semaphore()
    for dev in (xl, xs_, yl, ys_, sib):
        pl.semaphore_signal(barrier, inc=1, device_id=dev, device_id_type=MESH)
    with jax.named_scope("barrier"):
        pl.semaphore_wait(barrier, 5)

    go(XL, XL + 1, XS, YL, YS, SD, SW, SW + 1, SW + 2, SW + 3, WN, WN + 1)

    moves = [(x_in, xg.at[b, a], xbuf.at[0, :, pl.ds(0, kb)])]
    col = kb
    for u in range(2):
        for r0 in range(0, kb, rows):
            n = min(rows, kb - r0)
            for p in range(2):
                src = w_in[u].at[pl.ds(r0, n), pl.ds(pl.multiple_of(a * hc + p_src[p], 128), pc[p])]
                dst = wgu.at[u, pl.ds(pl.multiple_of(a * kb + r0, 16), n), pl.ds(pl.multiple_of(p_dst[p] + c * pc[p], 128), pc[p])]
                moves.append((src, dst, xbuf.at[0, pl.ds(0, n), pl.ds(col, pc[p])]))
                col += pc[p]
    per = max(1, min(rows, wd_in.shape[0]))
    col = 0
    for r0 in range(0, wd_in.shape[0], per):
        n = min(per, wd_in.shape[0] - r0)
        moves.append((wd_in.at[pl.ds(r0, n)], wd.at[pl.ds(r0, n), lanes(c, mc)], xbuf.at[1, pl.ds(0, n), pl.ds(col, mc)]))
        col += mc
    for i, (src, _, mid) in enumerate(moves):
        pltpu.make_async_copy(src, mid, bin_s.at[i]).start()
    with jax.named_scope("bounce"):
        for i, (src, dst, mid) in enumerate(moves):
            pltpu.make_async_copy(src, mid, bin_s.at[i]).wait()
            pltpu.make_async_copy(mid, dst, bout_s.at[i]).start()
        zinb[...] = jnp.zeros_like(zinb)
        for i, (_, dst, mid) in enumerate(moves):
            pltpu.make_async_copy(mid, dst, bout_s.at[i]).wait()

    got(XL)
    go(XF)
    got(XL + 1)
    go(XF + 1, W2, W2 + 1, YL + 1)
    got(XS)
    go(YL + 2, WN + 2, WN + 3)
    got(YL)
    go(YF)
    got(XF, XF + 1)
    go(YL + 3, WL)
    got(YL + 1)
    go(YF + 1)
    got(W2)
    go(WF)
    got(W2 + 1)
    go(WF + 1, WL + 1, W2 + 2, W2 + 3)
    got(YL + 2)
    go(YF + 2)
    got(WN, WN + 1)
    go(SW + 8, SW + 9)
    got(YL + 3)
    go(YF + 3)
    got(WL)
    go(SW + 4)
    got(WF, WF + 1)
    go(SW + 12, SW + 13)
    got(WL + 1)
    go(SW + 5, WL + 2, YS + 1)
    got(W2 + 2)
    go(WF + 2)
    got(W2 + 3)
    go(WF + 3, WL + 3)

    def x_load(s, k):
        return pltpu.make_async_copy(xg.at[dest(s), k], xbuf.at[lax.rem(s, 2), :, pl.ds(k * kb, kb)], xsem.at[lax.rem(s, 2), k])

    def w_load(g, u):
        slot = lax.rem(g, 2)
        return pltpu.make_async_copy(wgu.at[u, :, lanes(lax.rem(g, nt), tn)], wbuf.at[slot, :, pl.ds(u * tn, tn)], wsem.at[slot, u])

    def wd_load(z, i):
        slot, n = lax.rem(z, 2), lax.rem(z, nz)
        aa, p, cc = i // 4, i % 4 // 2, i % 2
        src = wd.at[pl.ds(cc * nloc + aa * hc + p_src[p], pc[p]), lanes(n, zn)]
        return pltpu.make_async_copy(src, wdbuf.at[slot, pl.ds(aa * hq + p_dst[p] + cc * pc[p], pc[p])], wdsem.at[slot, i])

    def zin_load(z):
        return pltpu.make_async_copy(zin.at[z // nz - 2, lax.rem(z, nz)], zinb.at[lax.rem(z, 2)], zinsem.at[lax.rem(z, 2)])

    def pairs(s):
        return jnp.maximum(early - s, 0)

    def item_of(s, h, t):
        m = pairs(s)
        return 2 * nt * s + jnp.where(t < m, 2 * t + h, 2 * m + h * (nt - m) + t - m)

    def place_of(i):
        s, v = i // (2 * nt), lax.rem(i, 2 * nt)
        m = pairs(s)
        w = jnp.maximum(v - 2 * m, 0)
        late = jnp.where(w >= nt - m, 1, 0)
        h = jnp.where(v < 2 * m, lax.rem(v, 2), late)
        t = jnp.where(v < 2 * m, v // 2, m + w - late * (nt - m))
        return s, h, t

    def h_write(g, h):
        slot = lax.rem(g, H_SLOTS)
        return pltpu.make_async_copy(hout.at[slot, h], hg.at[dest(g // nt), a, h, lax.rem(g, nt)], hws.at[slot, h])

    def h_own(i, dev, ss, rs):
        s, h, t = place_of(i)
        slot = lax.rem(s * nt + t, H_SLOTS)
        return rc(hout.at[slot, h], hg.at[dest(s), a, h, t], ss.at[slot, h], rs.at[i], dev)

    def h_long(i):
        return h_own(i, xl, ols, olr)

    def h_short(i):
        return h_own(i, xs_, oss, osr)

    def h_fwd(i):
        s, h, t = place_of(i)
        blk = hg.at[dest(s), ash, h, t]
        return rc(blk, blk, fs.at[i], fr.at[i], xl)

    def ready(tiles):
        s, r = tiles // nt, lax.rem(tiles, nt)
        m = pairs(s)
        return 2 * nt * s + jnp.where(r <= m, 2 * r, m + r)

    def issued(forwards, tiles):
        return jnp.minimum(forwards + AHEAD, ready(tiles))

    def send(lo, hi):
        def one(i, carry):
            h_long(i).start()
            h_short(i).start()
            return carry

        lax.fori_loop(lo, hi, one, 0)

    def forwards(g):
        return jnp.where(g < early, 0, jnp.minimum(jnp.maximum(early, 2 * (g - early) + 2), ni))

    def serve(j, tiles):
        h_long(j).wait_recv()
        h_fwd(j).start()
        send(issued(j, tiles), issued(j + 1, tiles))

    def z_send(z):
        slot = lax.rem(z, Z_SLOTS)
        return rc(zout.at[slot], zin.at[z // nz, lax.rem(z, nz)], zs.at[slot], zr.at[z], yl)

    def o_write(z):
        slot = lax.rem(z, 2)
        r = pl.ds(pl.multiple_of(lax.rem(z // nz, 2) * part_rows, part_rows), part_rows)
        return pltpu.make_async_copy(ofin.at[slot], out.at[r, lanes(lax.rem(z, nz), zn)], osem.at[slot])

    def start_w(g):
        w_load(g, 0).start()
        w_load(g, 1).start()

    for k in range(RING):
        x_load(0, k).start()
    got(*(SW + 4 * j + u for j in range(RING) for u in range(2)))
    start_w(0)

    nzt, nsum = 2 * RING * nz, 2 * (RING - 1) * nz

    def z_tile(z, carry):
        q, slot = z // nz, lax.rem(z, 2)

        @pl.when(lax.rem(z, nz) == 0)
        def _():
            s, h = q // 2, lax.rem(q, 2)

            def piece(t, k):
                return pltpu.make_async_copy(hg.at[dest(s), k, h, t], hz.at[lax.rem(q, 2), :, lanes(k * nt + t, tn)], hzsem.at[k, t])

            def fetch(t, carry):
                i = item_of(s, h, t)
                h_short(i).wait_recv()
                h_fwd(i).wait_recv()
                for k in range(RING):
                    piece(t, k).start()
                return carry

            def fetched(t, carry):
                for k in range(RING):
                    piece(t, k).wait()
                return carry

            with jax.named_scope("harr"):
                lax.fori_loop(0, nt, fetch, 0)
            with jax.named_scope("hzload"):
                lax.fori_loop(0, nt, fetched, 0)

        @pl.when(z + 1 < nzt)
        def _():
            for i in range(16):
                wd_load(z + 1, i).start()

        with jax.named_scope("zinrecv"):
            @pl.when((z + 1 >= 2 * nz) & (z + 1 < nzt))
            def _():
                z_send(z + 1 - 2 * nz).wait_recv()
                zin_load(z + 1).start()

        with jax.named_scope("wdwait"):
            for i in range(16):
                wd_load(z, i).wait()

        with jax.named_scope("zinwait"):
            @pl.when(z >= 2 * nz)
            def _():
                zin_load(z).wait()

        with jax.named_scope("zslot"):
            @pl.when((z >= Z_SLOTS) & (z < nsum))
            def _():
                z_send(z - Z_SLOTS).wait_send()

        @pl.when(z - 2 >= nsum)
        def _():
            o_write(z - 2).wait()

        zslot = jnp.where(z < nsum, lax.rem(z, Z_SLOTS), Z_SLOTS)
        with jax.named_scope("zmm"):
            acc = jnp.dot(hz[lax.rem(q, 2)], wdbuf[slot], preferred_element_type=jnp.float32) + zinb[slot]
            zout[zslot] = acc
            ofin[slot] = acc.astype(jnp.bfloat16)

        @pl.when(z < nsum)
        def _():
            z_send(z).start()

        @pl.when(z >= nsum)
        def _():
            o_write(z).start()

        return carry

    def z_done(g):
        q = jnp.maximum(g - zstart, 0)
        return jnp.where(g < zstart, 0, 2 * nz * (q // nt) + 2 * nz * (lax.rem(q, nt) + 1) // nt)

    def body(g, carry):
        s, t = g // nt, lax.rem(g, nt)

        @pl.when(g == early - 1)
        def _():
            got(WN + 2, WN + 3)
            go(SW + 10, SW + 11)
            got(WL + 2)
            go(SW + 6)
            got(WF + 2)
            go(SW + 14)

        @pl.when(g == early)
        def _():
            got(WF + 3)
            go(SW + 15)
            got(WL + 3)
            go(SW + 7, YS + 2, YS + 3)

            def first(j, carry):
                serve(j, early)
                return carry

            lax.fori_loop(0, early, first, 0)
            got(*(SW + 4 * j + 2 + u for j in range(RING) for u in range(2)), SD)
            start_w(g)
            for i in range(16):
                wd_load(0, i).start()

        @pl.when(g < ng)
        def _():
            @pl.when((g + 1 < ng) & (g + 1 != early))
            def _():
                start_w(g + 1)

            @pl.when((t == nt - 1) & (g + 1 < ng))
            def _():
                @pl.when(s + 1 == 1)
                def _():
                    got(*range(YF, WN))

                @pl.when(s + 1 == 2)
                def _():
                    got(*range(YS, YF))

                for k in range(RING):
                    x_load(s + 1, k).start()

            with jax.named_scope("xwait"):
                @pl.when(t == 0)
                def _():
                    for k in range(RING):
                        x_load(s, k).wait()

            with jax.named_scope("wwait"):
                w_load(g, 0).wait()
                w_load(g, 1).wait()

            with jax.named_scope("hslot"):
                @pl.when(g >= H_SLOTS)
                def _():
                    for h in range(2):
                        i = item_of((g - H_SLOTS) // nt, h, lax.rem(g - H_SLOTS, nt))
                        h_long(i).wait_send()
                        h_short(i).wait_send()

            xslot, wslot, hslot = lax.rem(s, 2), lax.rem(g, 2), lax.rem(g, H_SLOTS)

            def part(h, carry):
                r = pl.ds(pl.multiple_of(h * part_rows, part_rows), part_rows)
                gu = jnp.dot(xbuf[xslot, r, :], wbuf[wslot], preferred_element_type=jnp.float32)
                gate = gu[:, :tn].astype(jnp.bfloat16).astype(jnp.float32)
                up = gu[:, tn:].astype(jnp.bfloat16).astype(jnp.float32)
                hout[hslot, h] = (jax.nn.silu(gate) * up).astype(jnp.bfloat16)
                return carry

            with jax.named_scope("gumm"):
                lax.fori_loop(0, 2, part, 0)
            for h in range(2):
                h_write(g, h).start()

        done, tiles = jnp.where(g == early, early, forwards(g - 1)), jnp.minimum(g + 1, ng)
        send(issued(done, jnp.minimum(g, ng)), issued(done, tiles))

        with jax.named_scope("fwd"):
            @pl.when(forwards(g) > done)
            def _():
                serve(done, tiles)

        @pl.when((g >= 1) & (g <= ng))
        def _():
            for h in range(2):
                h_write(g - 1, h).wait()

        lax.fori_loop(z_done(g - 1), z_done(g), z_tile, 0)

        with jax.named_scope("fwd"):
            @pl.when(forwards(g) > done + 1)
            def _():
                serve(done + 1, tiles)

        return carry

    last = early + ng
    lax.fori_loop(0, last, body, 0)
    lax.fori_loop(z_done(jnp.int32(last - 1)), nzt, z_tile, 0)

    with jax.named_scope("owait"):
        for z in range(nzt - 2, nzt):
            o_write(z).wait()
    for i in range(P1):
        p1(i).wait_send()

    def sent(g, carry):
        for h in range(2):
            i = item_of(g // nt, h, lax.rem(g, nt))
            h_long(i).wait_send()
            h_short(i).wait_send()
        return carry

    lax.fori_loop(ng - H_SLOTS, ng, sent, 0)

    def drain(i, carry):
        h_fwd(i).wait_send()
        return carry

    lax.fori_loop(0, ni, drain, 0)
    for z in range(max(0, nsum - Z_SLOTS), nsum):
        z_send(z).wait_send()


def _local(x_blk, wg_blk, wu_blk, wd_blk):
    rows, kb = x_blk.shape
    hc = wg_blk.shape[1] // RING
    mc = wd_blk.shape[1]
    tn, zn = _tile(2 * hc, 256), _tile(2 * mc, 256)
    nt, nz = 2 * hc // tn, 2 * mc // zn
    n_moves = 1 + 4 * -(-kb // rows) + -(-wd_blk.shape[0] // rows)
    bf16, f32 = jnp.bfloat16, jnp.float32
    hbm = pl.BlockSpec(memory_space=pl.ANY)
    half = rows // 2
    dma = pltpu.SemaphoreType.DMA
    flops = 2 * RING * rows * (RING * kb * 4 * hc + wd_blk.shape[0] * 2 * mc)
    res = pl.pallas_call(
        _kernel,
        name="ring_mlp",
        out_shape=(
            jax.ShapeDtypeStruct((rows, 2 * mc), bf16),
            jax.ShapeDtypeStruct((RING, RING, rows, kb), bf16),
            jax.ShapeDtypeStruct((2, RING * kb, 2 * hc), bf16),
            jax.ShapeDtypeStruct((2, kb, hc), bf16),
            jax.ShapeDtypeStruct((RING, RING, 2, nt, half, tn), bf16),
            jax.ShapeDtypeStruct((wd_blk.shape[0], 2 * mc), bf16),
            jax.ShapeDtypeStruct((2 * (RING - 1), nz, half, zn), f32),
        ),
        in_specs=[hbm] * 4,
        out_specs=(hbm,) * 7,
        scratch_shapes=[
            pltpu.VMEM((2, rows, RING * kb), bf16),
            pltpu.VMEM((2, RING * kb, 2 * tn), bf16),
            pltpu.VMEM((2, half, wd_blk.shape[0]), bf16),
            pltpu.VMEM((2, wd_blk.shape[0], zn), bf16),
            pltpu.VMEM((2, half, zn), f32),
            pltpu.VMEM((Z_SLOTS + 1, half, zn), f32),
            pltpu.VMEM((2, half, zn), bf16),
            pltpu.VMEM((H_SLOTS, 2, half, tn), bf16),
            dma((P1,)), dma((P1,)), dma((n_moves,)), dma((n_moves,)),
            dma((2, RING)), dma((2, 2)), dma((RING, nt)), dma((2, 16)), dma((2,)), dma((2,)),
            dma((H_SLOTS, 2)), dma((2 * RING * nt,)), dma((H_SLOTS, 2)), dma((2 * RING * nt,)),
            dma((2 * RING * nt,)), dma((2 * RING * nt,)), dma((H_SLOTS, 2)),
            dma((Z_SLOTS,)), dma((2 * (RING - 1) * nz,)),
        ],
        compiler_params=pltpu.CompilerParams(collective_id=0, has_side_effects=True, vmem_limit_bytes=67043328),
        cost_estimate=pl.CostEstimate(flops=flops, bytes_accessed=flops // 500, transcendentals=0),
    )(x_blk, wg_blk, wu_blk, wd_blk)
    return res[0]


def solution(mesh):
    assert mesh.shape["dz"] == RING and mesh.shape["dy"] == RING and mesh.shape["dx"] == 2
    x_spec = P(("grp", "dx", "dz"), "dy")
    w_in_spec = P("dy", ("dz", "dx"))
    w_out_spec = P("dz", ("dy", "dx"))
    return jax.shard_map(_local, mesh=mesh, in_specs=(x_spec, w_in_spec, w_in_spec, w_out_spec), out_specs=x_spec, check_vma=False)
```

```python
import jax
import jax.numpy as jnp
from jax import lax
from jax.experimental import pallas as pl
from jax.experimental.pallas import tpu as pltpu
from jax.sharding import PartitionSpec as P

MESH = pl.DeviceIdType.MESH
RING = 4
H_SLOTS = 8
Z_SLOTS = 8
AHEAD = 3
WD_SLOTS = 3
XL, XS, XF, YL, YS, YF, WN, W2, WF, WL, SW, SD, P1 = 0, 2, 3, 5, 9, 13, 17, 21, 25, 29, 33, 49, 50


def _tile(extent, most):
    return next(t for t in range(most, 0, -128) if extent % t == 0)


def _kernel(x_in, wg_in, wu_in, wd_in, out, xg, wgu, ws, hg, wds, wd, zin,
            xbuf, wbuf, hz, wdbuf, zinb, zout, zacc, ofin, hout,
            p1s, p1r, bin_s, bout_s, xsem, wsem, hzsem, wdsem, zinsem, osem,
            ols, olr, oss, osr, fs, fr, hws, zs, zr):
    rows, kb = x_in.shape
    hc = wg_in.shape[1] // RING
    nloc = wg_in.shape[1]
    hq = 2 * hc
    mc = wd_in.shape[1]
    part_rows, tn = hout.shape[2:]
    zn = zout.shape[2]
    nt = hq // tn
    nz = 2 * mc // zn
    ng = RING * nt
    ni = 2 * ng
    zstart = nt + 2
    early = (nt + 1) // 2
    pc = (early * tn // 2, hc - early * tn // 2)
    p_src, p_dst = (0, pc[0]), (0, 2 * pc[0])

    b = lax.axis_index("dz")
    a = lax.axis_index("dy")
    c = lax.axis_index("dx")
    step = 1 - 2 * c
    al = lax.rem(a + step + RING, RING)
    ash = lax.rem(a - step + RING, RING)
    a2 = lax.rem(a + 2, RING)
    bl = lax.rem(b + step + RING, RING)
    bsh = lax.rem(b - step + RING, RING)
    xl, xs_ = {"dy": al}, {"dy": ash}
    yl, ys_ = {"dz": bl}, {"dz": bsh}
    sib = {"dx": 1 - c}
    kbs = (a, ash, al, a2)
    w_in = (wg_in, wu_in)

    def dest(s):
        return lax.rem(b - step * (1 + s) + 2 * RING, RING)

    def rc(src, dst, ss, rs, dev):
        return pltpu.make_async_remote_copy(src_ref=src, dst_ref=dst, send_sem=ss, recv_sem=rs, device_id=dev, device_id_type=MESH)

    def lanes(i, n):
        return pl.ds(pl.multiple_of(i * n, 128), n)

    def krows(k):
        return pl.ds(pl.multiple_of(k * kb, 16), kb)

    half = rows // 2

    def w_piece(u, p, q):
        return w_in[u].at[:, pl.ds(pl.multiple_of(q * hc + p_src[p], 128), pc[p])]

    def w_place(u, p, k):
        return wgu.at[u, krows(k), pl.ds(pl.multiple_of(p_dst[p] + c * pc[p], 128), pc[p])]

    def p1(i):
        sem = (p1s.at[i], p1r.at[i])
        if i < XS:
            r = pl.ds((i - XL) * half, half)
            return rc(x_in.at[r], xg.at[b, a, r], *sem, xl)
        if i < XF:
            return rc(x_in, xg.at[b, a], *sem, xs_)
        if i < YL:
            r = pl.ds((i - XF) * half, half)
            return rc(xg.at[b, ash, r], xg.at[b, ash, r], *sem, xl)
        if i < YF:
            j = (i - YL) % RING
            src = x_in if j == 0 else xg.at[b, kbs[j]]
            return rc(src, xg.at[b, kbs[j]], *sem, yl if i < YS else ys_)
        if i < WN:
            j = i - YF
            return rc(xg.at[bsh, kbs[j]], xg.at[bsh, kbs[j]], *sem, yl)
        if i < WF:
            u, p = (i - WN) % 2, (i - WN) % 4 // 2
            if i < W2:
                return rc(w_piece(u, p, ash), w_place(u, p, a), *sem, xs_)
            return rc(w_piece(u, p, a2), ws.at[u, :, pl.ds(p_src[p], pc[p])], *sem, xl)
        if i < WL:
            u, p = (i - WF) % 2, (i - WF) // 2
            return rc(ws.at[u, :, pl.ds(p_src[p], pc[p])], w_place(u, p, ash), *sem, xl)
        if i < SW:
            u, p = (i - WL) % 2, (i - WL) // 2
            return rc(w_piece(u, p, al), w_place(u, p, a), *sem, xl)
        if i < SD:
            j, p, u = (i - SW) // 4, (i - SW) % 4 // 2, (i - SW) % 2
            dst = w_place(u, p, kbs[j])
            return rc(w_piece(u, p, a) if j == 0 else dst, dst, *sem, sib)
        return rc(wd_in, wds, *sem, sib)

    def go(*idx):
        for i in idx:
            p1(i).start()

    def got(*idx):
        for i in idx:
            with jax.named_scope(f"got{i}"):
                p1(i).wait_recv()

    barrier = pltpu.get_barrier_semaphore()
    for dev in (xl, xs_, yl, ys_, sib):
        pl.semaphore_signal(barrier, inc=1, device_id=dev, device_id_type=MESH)
    with jax.named_scope("barrier"):
        pl.semaphore_wait(barrier, 5)

    go(XL, XL + 1, XS, YL, YS, SD, SW, SW + 1, SW + 2, SW + 3, WN, WN + 1)

    def bounce(moves):
        outs = 0
        for i, (src, mid, _) in enumerate(moves):
            pltpu.make_async_copy(src, mid, bin_s.at[i]).start()
        for i, (src, mid, parts) in enumerate(moves):
            pltpu.make_async_copy(src, mid, bin_s.at[i]).wait()
            for piece, dst in parts:
                pltpu.make_async_copy(piece, dst, bout_s.at[outs]).start()
                outs += 1
        outs = 0
        for _, _, parts in moves:
            for piece, dst in parts:
                pltpu.make_async_copy(piece, dst, bout_s.at[outs]).wait()
                outs += 1

    def w_down_moves(src, core):
        moves = []
        for cc in range(2):
            for k in range(RING):
                cols = pl.ds((cc * RING + k) * mc, mc)
                parts = []
                for p in range(2):
                    at, end = p_dst[p] + cc * pc[p], p_dst[p] + (cc + 1) * pc[p]
                    while at < end:
                        n = min(end, (at // tn + 1) * tn) - at
                        row = p_src[p] + at - p_dst[p] - cc * pc[p]
                        dst = wd.at[pl.ds((at // tn * RING + k) * tn + at % tn, n), lanes(core, mc)]
                        parts.append((xbuf.at[1, pl.ds(row, n), cols], dst))
                        at += n
                moves.append((src.at[pl.ds(cc * nloc + k * hc, hc)], xbuf.at[1, pl.ds(0, hc), cols], parts))
        return moves

    moves = [(x_in, xbuf.at[0, :, pl.ds(0, kb)], [(xbuf.at[0, :, pl.ds(0, kb)], xg.at[b, a])])]
    col = kb
    for u in range(2):
        for r0 in range(0, kb, rows):
            n = min(rows, kb - r0)
            parts = []
            for p in range(2):
                dst = wgu.at[u, pl.ds(pl.multiple_of(a * kb + r0, 16), n), pl.ds(pl.multiple_of(p_dst[p] + c * pc[p], 128), pc[p])]
                parts.append((xbuf.at[0, pl.ds(0, n), pl.ds(col + p_src[p], pc[p])], dst))
            moves.append((w_in[u].at[pl.ds(r0, n), lanes(a, hc)], xbuf.at[0, pl.ds(0, n), pl.ds(col, hc)], parts))
            col += hc
    with jax.named_scope("bounce"):
        bounce(moves + w_down_moves(wd_in, c))
        zinb[...] = jnp.zeros_like(zinb)

    got(XL)
    go(XF)
    got(XL + 1)
    go(XF + 1, W2, W2 + 1, YL + 1)
    got(XS)
    go(YL + 2, WN + 2, WN + 3)
    got(YL)
    go(YF)
    got(XF, XF + 1)
    go(YL + 3, WL)
    got(YL + 1)
    go(YF + 1)
    got(SD)
    with jax.named_scope("bounce"):
        bounce(w_down_moves(wds, 1 - c))
    got(W2)
    go(WF)
    got(W2 + 1)
    go(WF + 1, WL + 1, W2 + 2, W2 + 3)
    got(YL + 2)
    go(YF + 2)
    got(WN, WN + 1)
    go(SW + 8, SW + 9)
    got(YL + 3)
    go(YF + 3)
    got(WL)
    go(SW + 4)
    got(WF, WF + 1)
    go(SW + 12, SW + 13)
    got(WL + 1)
    go(SW + 5, WL + 2, YS + 1)
    got(W2 + 2)
    go(WF + 2)
    got(W2 + 3)
    go(WF + 3, WL + 3)

    def x_load(s, k):
        return pltpu.make_async_copy(xg.at[dest(s), k], xbuf.at[lax.rem(s, 2), :, pl.ds(k * kb, kb)], xsem.at[lax.rem(s, 2), k])

    def w_load(g, u):
        slot = lax.rem(g, 2)
        return pltpu.make_async_copy(wgu.at[u, :, lanes(lax.rem(g, nt), tn)], wbuf.at[slot, :, pl.ds(u * tn, tn)], wsem.at[slot, u])

    ka = RING * tn * (nt - 2)
    whole, nzt = (2 * RING - 1) * nz, 2 * RING * nz
    wd_rows = (pl.ds(0, RING * hq), pl.ds(0, ka), pl.ds(ka, RING * hq - ka))

    def wd_load(w, kind):
        slot = lax.rem(w, WD_SLOTS)
        return pltpu.make_async_copy(wd.at[wd_rows[kind], lanes(lax.rem(w, nz), zn)], wdbuf.at[slot, wd_rows[kind]], wdsem.at[slot])

    def wd_fetch(w):
        for kind, (lo, hi) in enumerate(((0, whole), (whole, nzt), (nzt, nzt + nz))):
            @pl.when((w >= lo) & (w < hi))
            def _():
                wd_load(w, kind).start()

    def zin_load(z, slot):
        return pltpu.make_async_copy(zin.at[z // nz - 2, lax.rem(z, nz)], zinb.at[slot], zinsem.at[slot])

    def pairs(s):
        return jnp.maximum(early - s, 0)

    def item_of(s, h, t):
        m = pairs(s)
        return 2 * nt * s + jnp.where(t < m, 2 * t + h, 2 * m + h * (nt - m) + t - m)

    def place_of(i):
        s, v = i // (2 * nt), lax.rem(i, 2 * nt)
        m = pairs(s)
        w = jnp.maximum(v - 2 * m, 0)
        late = jnp.where(w >= nt - m, 1, 0)
        h = jnp.where(v < 2 * m, lax.rem(v, 2), late)
        t = jnp.where(v < 2 * m, v // 2, m + w - late * (nt - m))
        return s, h, t

    def h_write(g, h):
        slot = lax.rem(g, H_SLOTS)
        return pltpu.make_async_copy(hout.at[slot, h], hg.at[dest(g // nt), a, h, lax.rem(g, nt)], hws.at[slot, h])

    def h_own(i, dev, ss, rs):
        s, h, t = place_of(i)
        slot = lax.rem(s * nt + t, H_SLOTS)
        return rc(hout.at[slot, h], hg.at[dest(s), a, h, t], ss.at[slot, h], rs.at[i], dev)

    def h_long(i):
        return h_own(i, xl, ols, olr)

    def h_short(i):
        return h_own(i, xs_, oss, osr)

    def h_fwd(i):
        s, h, t = place_of(i)
        blk = hg.at[dest(s), ash, h, t]
        return rc(blk, blk, fs.at[i], fr.at[i], xl)

    def ready(tiles):
        s, r = tiles // nt, lax.rem(tiles, nt)
        m = pairs(s)
        return 2 * nt * s + jnp.where(r <= m, 2 * r, m + r)

    def issued(forwards, tiles):
        return jnp.minimum(forwards + AHEAD, ready(tiles))

    def send(lo, hi):
        def one(i, carry):
            h_long(i).start()
            h_short(i).start()
            return carry

        lax.fori_loop(lo, hi, one, 0)

    def forwards(g):
        return jnp.where(g < early, 0, jnp.minimum(jnp.maximum(early, 2 * (g - early) + 2), ni))

    def serve(j, tiles):
        h_long(j).wait_recv()
        h_fwd(j).start()
        send(issued(j, tiles), issued(j + 1, tiles))

        @pl.when(j >= 2)
        def _():
            h_long(j - 2).wait_send()
            h_short(j - 2).wait_send()

        @pl.when(j >= 4)
        def _():
            h_fwd(j - 4).wait_send()

    def pieces(q, t):
        s, h = q // 2, lax.rem(q, 2)
        return [pltpu.make_async_copy(hg.at[dest(s), k, h, t], hz.at[lax.rem(q, 2), :, lanes(t * RING + k, tn)], hzsem.at[k, t]) for k in range(RING)]

    def pull(q, lo, hi):
        def one(t, carry):
            i = item_of(q // 2, lax.rem(q, 2), t)
            h_short(i).wait_recv()
            h_fwd(i).wait_recv()
            for copy in pieces(q, t):
                copy.start()
            return carry

        lax.fori_loop(lo, hi, one, 0)

    def pulled(q, lo, hi):
        def one(t, carry):
            for copy in pieces(q, t):
                copy.wait()
            return carry

        lax.fori_loop(lo, hi, one, 0)

    def z_send(z):
        slot = lax.rem(z, Z_SLOTS)
        return rc(zout.at[slot], zin.at[z // nz, lax.rem(z, nz)], zs.at[slot], zr.at[z], yl)

    def o_write(z, slot):
        r = pl.ds(pl.multiple_of(lax.rem(z // nz, 2) * part_rows, part_rows), part_rows)
        return pltpu.make_async_copy(ofin.at[slot], out.at[r, lanes(lax.rem(z, nz), zn)], osem.at[slot])

    def start_w(g):
        w_load(g, 0).start()
        w_load(g, 1).start()

    for k in range(RING):
        x_load(0, k).start()
    got(*(SW + 4 * j + u for j in range(RING) for u in range(2)))
    start_w(0)

    nsum = 2 * (RING - 1) * nz

    def z_tile(z, carry):
        q, slot, wslot = z // nz, lax.rem(z, 2), lax.rem(z, WD_SLOTS)
        wd_fetch(z + 2)

        @pl.when(lax.rem(z, nz) == 0)
        def _():
            with jax.named_scope("harr"):
                pull(q, 0, nt)
            with jax.named_scope("hzload"):
                pulled(q, 0, nt)

        with jax.named_scope("zinrecv"):
            @pl.when((z + 1 >= 2 * nz) & (z + 1 < whole))
            def _():
                z_send(z + 1 - 2 * nz).wait_recv()
                zin_load(z + 1, 1 - slot).start()

        with jax.named_scope("wdwait"):
            wd_load(z, 0).wait()

        with jax.named_scope("zinwait"):
            @pl.when(z >= 2 * nz)
            def _():
                zin_load(z, slot).wait()

        with jax.named_scope("zslot"):
            @pl.when((z >= Z_SLOTS) & (z - Z_SLOTS < nsum))
            def _():
                z_send(z - Z_SLOTS).wait_send()

        @pl.when(z - 2 >= nsum)
        def _():
            o_write(z - 2, slot).wait()

        zslot = jnp.where(z < nsum, lax.rem(z, Z_SLOTS), Z_SLOTS)
        with jax.named_scope("zmm"):
            acc = jnp.dot(hz[lax.rem(q, 2)], wdbuf[wslot], preferred_element_type=jnp.float32) + zinb[slot]
            zout[zslot] = acc
            ofin[slot] = acc.astype(jnp.bfloat16)

        @pl.when(z < nsum)
        def _():
            z_send(z).start()

        @pl.when(z >= nsum)
        def _():
            o_write(z, slot).start()

        return carry

    last_q = 2 * RING - 1

    def tail_first(n, carry):
        w = whole + n
        wd_fetch(w + 2)
        wd_load(w, 1).wait()

        @pl.when(n == nz - 1)
        def _():
            z_send(whole - 2 * nz).wait_recv()
            zin_load(jnp.int32(whole), lax.rem(nzt, 2)).start()

        with jax.named_scope("za"):
            zacc[n] = jnp.dot(hz[1, :, wd_rows[1]], wdbuf[lax.rem(w, WD_SLOTS), wd_rows[1]], preferred_element_type=jnp.float32)
        return carry

    def tail_second(n, carry):
        w, z = nzt + n, whole + n
        slot = lax.rem(w, 2)
        wd_fetch(w + 2)

        @pl.when(n + 1 < nz)
        def _():
            z_send(z + 1 - 2 * nz).wait_recv()
            zin_load(z + 1, 1 - slot).start()

        wd_load(w, 2).wait()
        zin_load(z, slot).wait()
        o_write(z, slot).wait()
        with jax.named_scope("zb"):
            acc = jnp.dot(hz[1, :, wd_rows[2]], wdbuf[lax.rem(w, WD_SLOTS), wd_rows[2]], preferred_element_type=jnp.float32)
            ofin[slot] = (acc + zacc[n] + zinb[slot]).astype(jnp.bfloat16)
        o_write(z, slot).start()
        return carry

    def z_done(g):
        q, k = jnp.maximum(g - zstart, 0), g - zstart - 2 * nt + 1
        steady = 2 * nz * (q // nt) + 2 * nz * (lax.rem(q, nt) + 1) // nt
        ending = 4 * nz + 3 * nz * k // (early + ng - zstart - 2 * nt)
        return jnp.where(g < zstart, 0, jnp.where(k > 0, ending, steady))

    def body(g, carry):
        s, t = g // nt, lax.rem(g, nt)

        @pl.when(g == early - 1)
        def _():
            got(WN + 2, WN + 3)
            go(SW + 10, SW + 11)
            got(WL + 2)
            go(SW + 6)
            got(WF + 2)
            go(SW + 14)

        @pl.when(g == early)
        def _():
            got(WF + 3)
            go(SW + 15)
            got(WL + 3)
            go(SW + 7, YS + 2, YS + 3)

            def first(j, carry):
                serve(j, early)
                return carry

            lax.fori_loop(0, early, first, 0)
            got(*(SW + 4 * j + 2 + u for j in range(RING) for u in range(2)))
            start_w(g)
            wd_load(0, 0).start()
            wd_load(1, 0).start()

        @pl.when(g < ng)
        def _():
            @pl.when((g + 1 < ng) & (g + 1 != early))
            def _():
                start_w(g + 1)

            @pl.when((t == nt - 1) & (g + 1 < ng))
            def _():
                @pl.when(s + 1 == 1)
                def _():
                    got(*range(YF, WN))

                @pl.when(s + 1 == 2)
                def _():
                    got(*range(YS, YF))

                for k in range(RING):
                    x_load(s + 1, k).start()

            with jax.named_scope("xwait"):
                @pl.when(t == 0)
                def _():
                    for k in range(RING):
                        x_load(s, k).wait()

            with jax.named_scope("wwait"):
                w_load(g, 0).wait()
                w_load(g, 1).wait()

            xslot, wslot, hslot = lax.rem(s, 2), lax.rem(g, 2), lax.rem(g, H_SLOTS)

            def part(h, carry):
                r = pl.ds(pl.multiple_of(h * part_rows, part_rows), part_rows)
                gu = jnp.dot(xbuf[xslot, r, :], wbuf[wslot], preferred_element_type=jnp.float32)
                gate = gu[:, :tn].astype(jnp.bfloat16).astype(jnp.float32)
                up = gu[:, tn:].astype(jnp.bfloat16).astype(jnp.float32)
                hout[hslot, h] = (jax.nn.silu(gate) * up).astype(jnp.bfloat16)
                return carry

            with jax.named_scope("gumm"):
                lax.fori_loop(0, 2, part, 0)
            for h in range(2):
                h_write(g, h).start()

        @pl.when(g == 2 * nt)
        def _():
            for i in range(P1):
                p1(i).wait_send()

        done, tiles = jnp.where(g == early, early, forwards(g - 1)), jnp.minimum(g + 1, ng)
        send(issued(done, jnp.minimum(g, ng)), issued(done, tiles))

        with jax.named_scope("fwd"):
            @pl.when(forwards(g) > done)
            def _():
                serve(done, tiles)

        @pl.when((g >= 1) & (g <= ng))
        def _():
            for h in range(2):
                h_write(g - 1, h).wait()

        lax.fori_loop(z_done(g - 1), z_done(g), z_tile, 0)

        with jax.named_scope("fwd"):
            @pl.when(forwards(g) > done + 1)
            def _():
                serve(done + 1, tiles)

        return carry

    lax.fori_loop(0, early + ng, body, 0)

    with jax.named_scope("harr"):
        pull(last_q, 0, nt - 2)
        pulled(last_q, 0, nt - 2)
    lax.fori_loop(0, nz, tail_first, 0)
    with jax.named_scope("harr"):
        pull(last_q, nt - 2, nt)
        pulled(last_q, nt - 2, nt)
    lax.fori_loop(0, nz, tail_second, 0)

    with jax.named_scope("owait"):
        for slot in range(2):
            o_write(jnp.int32(nzt - 1), slot).wait()

    for i in range(ni - 2, ni):
        h_long(jnp.int32(i)).wait_send()
        h_short(jnp.int32(i)).wait_send()
    for i in range(ni - 4, ni):
        h_fwd(jnp.int32(i)).wait_send()
    for z in range(max(0, whole - Z_SLOTS), nsum):
        z_send(z).wait_send()


def _local(x_blk, wg_blk, wu_blk, wd_blk):
    rows, kb = x_blk.shape
    hc = wg_blk.shape[1] // RING
    mc = wd_blk.shape[1]
    tn, zn = _tile(2 * hc, 256), _tile(2 * mc, 256)
    nt, nz = 2 * hc // tn, 2 * mc // zn
    n_loads = 1 + 2 * -(-kb // rows) + 2 * RING
    n_outs = 1 + 4 * -(-kb // rows) + 8 * RING
    bf16, f32 = jnp.bfloat16, jnp.float32
    hbm = pl.BlockSpec(memory_space=pl.ANY)
    half = rows // 2
    dma = pltpu.SemaphoreType.DMA
    flops = 2 * RING * rows * (RING * kb * 4 * hc + wd_blk.shape[0] * 2 * mc)
    res = pl.pallas_call(
        _kernel,
        name="ring_mlp",
        out_shape=(
            jax.ShapeDtypeStruct((rows, 2 * mc), bf16),
            jax.ShapeDtypeStruct((RING, RING, rows, kb), bf16),
            jax.ShapeDtypeStruct((2, RING * kb, 2 * hc), bf16),
            jax.ShapeDtypeStruct((2, kb, hc), bf16),
            jax.ShapeDtypeStruct((RING, RING, 2, nt, half, tn), bf16),
            jax.ShapeDtypeStruct(wd_blk.shape, bf16),
            jax.ShapeDtypeStruct((wd_blk.shape[0], 2 * mc), bf16),
            jax.ShapeDtypeStruct((2 * (RING - 1), nz, half, zn), f32),
        ),
        in_specs=[hbm] * 4,
        out_specs=(hbm,) * 8,
        scratch_shapes=[
            pltpu.VMEM((2, rows, RING * kb), bf16),
            pltpu.VMEM((2, RING * kb, 2 * tn), bf16),
            pltpu.VMEM((2, half, wd_blk.shape[0]), bf16),
            pltpu.VMEM((WD_SLOTS, wd_blk.shape[0], zn), bf16),
            pltpu.VMEM((2, half, zn), f32),
            pltpu.VMEM((Z_SLOTS + 1, half, zn), f32),
            pltpu.VMEM((nz, half, zn), f32),
            pltpu.VMEM((2, half, zn), bf16),
            pltpu.VMEM((H_SLOTS, 2, half, tn), bf16),
            dma((P1,)), dma((P1,)), dma((n_loads,)), dma((n_outs,)),
            dma((2, RING)), dma((2, 2)), dma((RING, nt)), dma((WD_SLOTS,)), dma((2,)), dma((2,)),
            dma((H_SLOTS, 2)), dma((2 * RING * nt,)), dma((H_SLOTS, 2)), dma((2 * RING * nt,)),
            dma((2 * RING * nt,)), dma((2 * RING * nt,)), dma((H_SLOTS, 2)),
            dma((Z_SLOTS,)), dma((2 * (RING - 1) * nz,)),
        ],
        compiler_params=pltpu.CompilerParams(collective_id=0, has_side_effects=True, vmem_limit_bytes=67043328),
        cost_estimate=pl.CostEstimate(flops=flops, bytes_accessed=flops // 500, transcendentals=0),
    )(x_blk, wg_blk, wu_blk, wd_blk)
    return res[0]


def solution(mesh):
    assert mesh.shape["dz"] == RING and mesh.shape["dy"] == RING and mesh.shape["dx"] == 2
    x_spec = P(("grp", "dx", "dz"), "dy")
    w_in_spec = P("dy", ("dz", "dx"))
    w_out_spec = P("dz", ("dy", "dx"))
    return jax.shard_map(_local, mesh=mesh, in_specs=(x_spec, w_in_spec, w_in_spec, w_out_spec), out_specs=x_spec, check_vma=False)
```

```python
import jax
import jax.numpy as jnp
from jax import lax
from jax.experimental import pallas as pl
from jax.experimental.pallas import tpu as pltpu
from jax.sharding import PartitionSpec as P

MESH = pl.DeviceIdType.MESH
RING = 4
H_SLOTS = 7
Z_SLOTS = 6
AHEAD = 3
WD_SLOTS = 3
XL, XS, XF, YL, YS, YF, WN, W2, WF, WL, SW, SD, P1 = 0, 2, 3, 5, 9, 13, 17, 21, 25, 29, 33, 49, 50
JOINT = (
    (XF, XF + 1), tuple(range(YS, YF)), tuple(range(YF, WN)), (WN, WN + 1), (WN + 2, WN + 3), (WF, WF + 1),
    tuple(SW + 4 * j + u for j in range(RING) for u in range(2)), tuple(SW + 4 * j + 2 + u for j in range(RING) for u in range(2)),
)
RECV = {}
for _i in range(P1):
    _group = next((g for g in JOINT if _i in g), (_i,))
    RECV[_i] = RECV[_group[0]] if _i != _group[0] else len(set(RECV.values()))
N_RECV = len(set(RECV.values()))


def _tile(extent, most):
    return next(t for t in range(most, 0, -128) if extent % t == 0)


def _kernel(x_in, wg_in, wu_in, wd_in, out, xg, wgu, ws, hg, wds, wd, zin,
            xbuf, wbuf, hz, wdbuf, zinb, zout, zacc, ofin, hout,
            p1s, p1r, bin_s, bout_s, xsem, wsem, hzsem, wdsem, zinsem, osem,
            ols, olr, oss, osr, fs, fr, hws, zs, zr):
    rows, kb = x_in.shape
    hc = wg_in.shape[1] // RING
    nloc = wg_in.shape[1]
    hq = 2 * hc
    mc = wd_in.shape[1]
    part_rows, tn = hout.shape[2:]
    zn = zout.shape[2]
    nt = hq // tn
    nz = 2 * mc // zn
    ng = RING * nt
    ni = 2 * ng
    zstart = nt + 2
    early = (nt + 1) // 2
    pc = (early * tn // 2, hc - early * tn // 2)
    p_src, p_dst = (0, pc[0]), (0, 2 * pc[0])

    b = lax.axis_index("dz")
    a = lax.axis_index("dy")
    c = lax.axis_index("dx")
    step = 1 - 2 * c
    al = lax.rem(a + step + RING, RING)
    ash = lax.rem(a - step + RING, RING)
    a2 = lax.rem(a + 2, RING)
    bl = lax.rem(b + step + RING, RING)
    bsh = lax.rem(b - step + RING, RING)
    xl, xs_ = {"dy": al}, {"dy": ash}
    yl, ys_ = {"dz": bl}, {"dz": bsh}
    sib = {"dx": 1 - c}
    kbs = (a, ash, al, a2)
    w_in = (wg_in, wu_in)

    def dest(s):
        return lax.rem(b - step * (1 + s) + 2 * RING, RING)

    def rc(src, dst, ss, rs, dev):
        return pltpu.make_async_remote_copy(src_ref=src, dst_ref=dst, send_sem=ss, recv_sem=rs, device_id=dev, device_id_type=MESH)

    def lanes(i, n):
        return pl.ds(pl.multiple_of(i * n, 128), n)

    def krows(k):
        return pl.ds(pl.multiple_of(k * kb, 16), kb)

    half = rows // 2

    def w_piece(u, p, q):
        return w_in[u].at[:, pl.ds(pl.multiple_of(q * hc + p_src[p], 128), pc[p])]

    def w_place(u, p, k):
        return wgu.at[u, krows(k), pl.ds(pl.multiple_of(p_dst[p] + c * pc[p], 128), pc[p])]

    def p1(i):
        kind = 0 if i < YL else 1 if i < WN else 2 if i < SW else 3 if i < SD else 4
        sem = (p1s.at[kind], p1r.at[RECV[i]])
        if i < XS:
            r = pl.ds((i - XL) * half, half)
            return rc(x_in.at[r], xg.at[b, a, r], *sem, xl)
        if i < XF:
            return rc(x_in, xg.at[b, a], *sem, xs_)
        if i < YL:
            r = pl.ds((i - XF) * half, half)
            return rc(xg.at[b, ash, r], xg.at[b, ash, r], *sem, xl)
        if i < YF:
            j = (i - YL) % RING
            src = x_in if j == 0 else xg.at[b, kbs[j]]
            return rc(src, xg.at[b, kbs[j]], *sem, yl if i < YS else ys_)
        if i < WN:
            j = i - YF
            return rc(xg.at[bsh, kbs[j]], xg.at[bsh, kbs[j]], *sem, yl)
        if i < WF:
            u, p = (i - WN) % 2, (i - WN) % 4 // 2
            if i < W2:
                return rc(w_piece(u, p, ash), w_place(u, p, a), *sem, xs_)
            return rc(w_piece(u, p, a2), ws.at[u, :, pl.ds(p_src[p], pc[p])], *sem, xl)
        if i < WL:
            u, p = (i - WF) % 2, (i - WF) // 2
            return rc(ws.at[u, :, pl.ds(p_src[p], pc[p])], w_place(u, p, ash), *sem, xl)
        if i < SW:
            u, p = (i - WL) % 2, (i - WL) // 2
            return rc(w_piece(u, p, al), w_place(u, p, a), *sem, xl)
        if i < SD:
            j, p, u = (i - SW) // 4, (i - SW) % 4 // 2, (i - SW) % 2
            dst = w_place(u, p, kbs[j])
            return rc(w_piece(u, p, a) if j == 0 else dst, dst, *sem, sib)
        return rc(wd_in, wds, *sem, sib)

    def go(*idx):
        for i in idx:
            p1(i).start()

    def got(*idx):
        for i in idx:
            with jax.named_scope(f"got{i}"):
                p1(i).wait_recv()

    def total(ref, sem):
        pltpu.make_async_copy(ref, ref, sem).wait()

    def got_all(first, ref):
        with jax.named_scope(f"got{first}"):
            total(ref, p1r.at[RECV[first]])

    def part_of(u_refs, p):
        return u_refs.at[:, :, pl.ds(p_src[p], pc[p])]

    def all_sent():
        quarter = wgu.at[:, :, pl.ds(0, hc)]
        for kind, ref in enumerate((xg.at[0, pl.ds(0, 3)], xg.at[pl.ds(0, 3)], quarter, quarter, wds)):
            total(ref, p1s.at[kind])

    barrier = pltpu.get_barrier_semaphore()
    for dev in (xl, xs_, yl, ys_, sib):
        pl.semaphore_signal(barrier, inc=1, device_id=dev, device_id_type=MESH)
    with jax.named_scope("barrier"):
        pl.semaphore_wait(barrier, 5)

    go(XL, XL + 1, XS, YL, YS, SD, SW, SW + 1, SW + 2, SW + 3, WN, WN + 1)

    def bounce(*classes):
        for i, (size, moves) in enumerate(classes):
            for src, mid, _ in moves:
                pltpu.make_async_copy(src, mid, bin_s.at[i]).start()
        for i, (size, moves) in enumerate(classes):
            total(size, bin_s.at[i])
            for _, _, parts in moves:
                for piece, dst in parts:
                    pltpu.make_async_copy(piece, dst, bout_s.at[i]).start()
        for i, (size, moves) in enumerate(classes):
            total(size, bout_s.at[i])

    def w_down_moves(src, core):
        moves = []
        for cc in range(2):
            for k in range(RING):
                cols = pl.ds((cc * RING + k) * mc, mc)
                parts = []
                for p in range(2):
                    at, end = p_dst[p] + cc * pc[p], p_dst[p] + (cc + 1) * pc[p]
                    while at < end:
                        n = min(end, (at // tn + 1) * tn) - at
                        row = p_src[p] + at - p_dst[p] - cc * pc[p]
                        dst = wd.at[pl.ds((at // tn * RING + k) * tn + at % tn, n), lanes(core, mc)]
                        parts.append((xbuf.at[1, pl.ds(row, n), cols], dst))
                        at += n
                moves.append((src.at[pl.ds(cc * nloc + k * hc, hc)], xbuf.at[1, pl.ds(0, hc), cols], parts))
        return moves

    x_moves = [(x_in, xbuf.at[0, :, pl.ds(0, kb)], [(xbuf.at[0, :, pl.ds(0, kb)], xg.at[b, a])])]
    w_moves, col = [], kb
    for u in range(2):
        for r0 in range(0, kb, rows):
            n = min(rows, kb - r0)
            parts = []
            for p in range(2):
                dst = wgu.at[u, pl.ds(pl.multiple_of(a * kb + r0, 16), n), pl.ds(pl.multiple_of(p_dst[p] + c * pc[p], 128), pc[p])]
                parts.append((xbuf.at[0, pl.ds(0, n), pl.ds(col + p_src[p], pc[p])], dst))
            w_moves.append((w_in[u].at[pl.ds(r0, n), lanes(a, hc)], xbuf.at[0, pl.ds(0, n), pl.ds(col, hc)], parts))
            col += hc
    with jax.named_scope("bounce"):
        bounce((x_in, x_moves), (ws, w_moves), (wd_in, w_down_moves(wd_in, c)))
        zinb[...] = jnp.zeros_like(zinb)

    got(XL)
    go(XF)
    got(XL + 1)
    go(XF + 1, W2, W2 + 1, YL + 1)
    got(XS)
    go(YL + 2, WN + 2, WN + 3)
    got(YL)
    go(YF)
    got_all(XF, xg.at[0, 0])
    go(YL + 3, WL)
    got(YL + 1)
    go(YF + 1)
    got(SD)
    with jax.named_scope("bounce"):
        bounce((wds, w_down_moves(wds, 1 - c)))
    got(W2)
    go(WF)
    got(W2 + 1)
    go(WF + 1, WL + 1, W2 + 2, W2 + 3)
    got(YL + 2)
    go(YF + 2)
    got_all(WN, part_of(ws, 0))
    go(SW + 8, SW + 9)
    got(YL + 3)
    go(YF + 3)
    got(WL)
    go(SW + 4)
    got_all(WF, part_of(ws, 0))
    go(SW + 12, SW + 13)
    got(WL + 1)
    go(SW + 5, WL + 2, YS + 1)
    got(W2 + 2)
    go(WF + 2)
    got(W2 + 3)
    go(WF + 3, WL + 3)

    def x_load(s, k):
        return pltpu.make_async_copy(xg.at[dest(s), k], xbuf.at[lax.rem(s, 2), :, pl.ds(k * kb, kb)], xsem.at[lax.rem(s, 2)])

    def w_load(g, u):
        slot = lax.rem(g, 2)
        return pltpu.make_async_copy(wgu.at[u, :, lanes(lax.rem(g, nt), tn)], wbuf.at[slot, :, pl.ds(u * tn, tn)], wsem.at[slot])

    ka = RING * tn * (nt - 2)
    whole, nzt = (2 * RING - 1) * nz, 2 * RING * nz
    wd_rows = (pl.ds(0, RING * hq), pl.ds(0, ka), pl.ds(ka, RING * hq - ka))

    n_seg = RING * kb // (RING * hq - ka)

    def late_place(n):
        rows_b = RING * hq - ka
        seg = pl.ds(pl.multiple_of(lax.rem(n // 2, n_seg) * rows_b, 16), rows_b)
        return wbuf.at[n // (2 * n_seg), seg, lanes(lax.rem(n, 2), tn)]

    def late_load(n):
        return pltpu.make_async_copy(wd.at[wd_rows[2], lanes(n, zn)], late_place(n), wdsem.at[WD_SLOTS])

    def wd_load(w, kind):
        slot = lax.rem(w, WD_SLOTS)
        return pltpu.make_async_copy(wd.at[wd_rows[kind], lanes(lax.rem(w, nz), zn)], wdbuf.at[slot, wd_rows[kind]], wdsem.at[slot])

    def wd_fetch(w):
        for kind, (lo, hi) in enumerate(((0, whole), (whole, nzt))):
            @pl.when((w >= lo) & (w < hi))
            def _():
                wd_load(w, kind).start()

    def zin_load(z, slot, sem):
        return pltpu.make_async_copy(zin.at[z // nz - 2, lax.rem(z, nz)], zinb.at[slot], zinsem.at[sem])

    def pairs(s):
        return jnp.maximum(early - s, 0)

    def item_of(s, h, t):
        m = pairs(s)
        return 2 * nt * s + jnp.where(t < m, 2 * t + h, 2 * m + h * (nt - m) + t - m)

    def place_of(i):
        s, v = i // (2 * nt), lax.rem(i, 2 * nt)
        m = pairs(s)
        w = jnp.maximum(v - 2 * m, 0)
        late = jnp.where(w >= nt - m, 1, 0)
        h = jnp.where(v < 2 * m, lax.rem(v, 2), late)
        t = jnp.where(v < 2 * m, v // 2, m + w - late * (nt - m))
        return s, h, t

    def h_write(g):
        slot = lax.rem(g, H_SLOTS)
        return pltpu.make_async_copy(hout.at[slot], hg.at[dest(g // nt), a, :, lax.rem(g, nt)], hws.at[lax.rem(g, 2)])

    def half_of(s, h, t):
        q = 2 * s + h
        return q + jnp.where((q == 2 * RING - 1) & (t >= nt - 2), 1, 0)

    def h_long(i):
        s, h, t = place_of(i)
        return rc(hout.at[lax.rem(s * nt + t, H_SLOTS), h], hg.at[dest(s), a, h, t], ols.at[lax.rem(i, 8)], olr.at[i], xl)

    def h_short(i):
        s, h, t = place_of(i)
        return rc(hout.at[lax.rem(s * nt + t, H_SLOTS), h], hg.at[dest(s), a, h, t], oss.at[lax.rem(i, 8)], osr.at[half_of(s, h, t)], xs_)

    def h_fwd(i):
        s, h, t = place_of(i)
        blk = hg.at[dest(s), ash, h, t]
        return rc(blk, blk, fs.at[lax.rem(i, 8)], fr.at[half_of(s, h, t)], xl)

    def ready(tiles):
        s, r = tiles // nt, lax.rem(tiles, nt)
        m = pairs(s)
        return 2 * nt * s + jnp.where(r <= m, 2 * r, m + r)

    def issued(forwards, tiles):
        return jnp.minimum(forwards + AHEAD, ready(tiles))

    def send(lo, hi):
        def one(i, carry):
            h_long(i).start()
            h_short(i).start()
            return carry

        lax.fori_loop(lo, hi, one, 0)

    def forwards(g):
        return jnp.where(g < early, 0, jnp.minimum(jnp.maximum(early, 2 * (g - early) + 2), ni))

    def serve(j, tiles):
        h_long(j).wait_recv()
        h_fwd(j).start()
        send(issued(j, tiles), issued(j + 1, tiles))

        @pl.when(j >= 2)
        def _():
            h_long(j - 2).wait_send()
            h_short(j - 2).wait_send()

        @pl.when(j >= 4)
        def _():
            h_fwd(j - 4).wait_send()

    def pull(q, sem, lo, hi):
        s, h = q // 2, lax.rem(q, 2)
        arrived = hg.at[0, 0, 0, pl.ds(lo, hi - lo)]
        total(arrived, osr.at[sem])
        total(arrived, fr.at[sem])

        def one(t, carry):
            for k in range(RING):
                pltpu.make_async_copy(hg.at[dest(s), k, h, t], hz.at[lax.rem(q, 2), :, lanes(t * RING + k, tn)], hzsem.at[0]).start()
            return carry

        lax.fori_loop(lo, hi, one, 0)

    def pulled(q, lo, hi):
        total(hz.at[lax.rem(q, 2), :, pl.ds(lo * RING * tn, (hi - lo) * RING * tn)], hzsem.at[0])

    def z_send(z):
        slot = lax.rem(z, Z_SLOTS)
        return rc(zout.at[slot], zin.at[z // nz, lax.rem(z, nz)], zs.at[slot], zr.at[z // nz], yl)

    def o_write(z, slot, sem):
        r = pl.ds(pl.multiple_of(lax.rem(z // nz, 2) * part_rows, part_rows), part_rows)
        return pltpu.make_async_copy(ofin.at[slot], out.at[r, lanes(lax.rem(z, nz), zn)], osem.at[sem])

    def start_w(g):
        w_load(g, 0).start()
        w_load(g, 1).start()

    for k in range(RING):
        x_load(0, k).start()
    got_all(SW, wgu.at[:, :, pl.ds(p_dst[0], pc[0])])
    start_w(0)

    nsum = 2 * (RING - 1) * nz

    def z_tile(z, carry):
        q, slot, wslot = z // nz, lax.rem(z, 2), lax.rem(z, WD_SLOTS)
        wd_fetch(z + 2)

        @pl.when(lax.rem(z, nz) == 0)
        def _():
            with jax.named_scope("harr"):
                pull(q, q, 0, nt)
            with jax.named_scope("hzload"):
                pulled(q, 0, nt)

        with jax.named_scope("zinrecv"):
            @pl.when((z + 2 >= 2 * nz) & (z + 2 < whole))
            def _():
                @pl.when(lax.rem(z + 2, nz) == 0)
                def _():
                    total(zin.at[0], zr.at[(z + 2) // nz - 2])

                zin_load(z + 2, lax.rem(z + 2, 3), lax.rem(z + 2, 3)).start()

        with jax.named_scope("wdwait"):
            wd_load(z, 0).wait()

        with jax.named_scope("zinwait"):
            @pl.when(z >= 2 * nz)
            def _():
                zin_load(z, lax.rem(z, 3), lax.rem(z, 3)).wait()

        with jax.named_scope("zslot"):
            @pl.when((z >= Z_SLOTS) & (z - Z_SLOTS < nsum))
            def _():
                z_send(z - Z_SLOTS).wait_send()

        @pl.when(z - 2 >= nsum)
        def _():
            o_write(z - 2, slot, slot).wait()

        zslot = jnp.where(z < nsum, lax.rem(z, Z_SLOTS), Z_SLOTS)
        with jax.named_scope("zmm"):
            acc = jnp.dot(hz[lax.rem(q, 2)], wdbuf[wslot], preferred_element_type=jnp.float32) + zinb[lax.rem(z, 3)]
            zout[zslot] = acc
            ofin[slot] = acc.astype(jnp.bfloat16)

        @pl.when(z < nsum)
        def _():
            z_send(z).start()

        @pl.when(z >= nsum)
        def _():
            o_write(z, slot, slot).start()

        return carry

    last_q = 2 * RING - 1

    def tail_first(n, carry):
        w = whole + n
        wd_fetch(w + 2)
        wd_load(w, 1).wait()
        with jax.named_scope("za"):
            zacc[n] = jnp.dot(hz[1, :, wd_rows[1]], wdbuf[lax.rem(w, WD_SLOTS), wd_rows[1]], preferred_element_type=jnp.float32)
        return carry

    def tail_second(n, carry):
        with jax.named_scope("zb"):
            acc = jnp.dot(hz[1, :, wd_rows[2]], late_place(n)[...], preferred_element_type=jnp.float32)
            ofin[n] = (acc + zacc[n] + zinb[n]).astype(jnp.bfloat16)
        o_write(whole + n, n, 2).start()
        return carry

    def z_done(g):
        q, k = jnp.maximum(g - zstart, 0), g - zstart - 2 * nt + 1
        steady = 2 * nz * (q // nt) + 2 * nz * (lax.rem(q, nt) + 1) // nt
        ending = 4 * nz + 3 * nz * k // (early + ng - zstart - 2 * nt)
        return jnp.where(g < zstart, 0, jnp.where(k > 0, ending, steady))

    def body(g, carry):
        s, t = g // nt, lax.rem(g, nt)

        @pl.when(g == early - 1)
        def _():
            got_all(WN + 2, part_of(ws, 1))
            go(SW + 10, SW + 11)
            got(WL + 2)
            go(SW + 6)
            got(WF + 2)
            go(SW + 14)

        @pl.when(g == early)
        def _():
            got(WF + 3)
            go(SW + 15)
            got(WL + 3)
            go(SW + 7, YS + 2, YS + 3)

            def first(j, carry):
                serve(j, early)
                return carry

            lax.fori_loop(0, early, first, 0)
            got_all(SW + 2, wgu.at[:, :, pl.ds(p_dst[1], pc[1])])
            start_w(g)
            wd_load(0, 0).start()
            wd_load(1, 0).start()

        @pl.when(g < ng)
        def _():
            @pl.when((g + 1 < ng) & (g + 1 != early))
            def _():
                start_w(g + 1)

            @pl.when((t == nt - 1) & (g + 1 < ng))
            def _():
                @pl.when(s + 1 == 1)
                def _():
                    got_all(YF, xg.at[0])

                @pl.when(s + 1 == 2)
                def _():
                    got_all(YS, xg.at[0])

                for k in range(RING):
                    x_load(s + 1, k).start()

            with jax.named_scope("xwait"):
                @pl.when(t == 0)
                def _():
                    total(xbuf.at[lax.rem(s, 2)], xsem.at[lax.rem(s, 2)])

            with jax.named_scope("wwait"):
                total(wbuf.at[lax.rem(g, 2)], wsem.at[lax.rem(g, 2)])

            xslot, wslot, hslot = lax.rem(s, 2), lax.rem(g, 2), lax.rem(g, H_SLOTS)

            def part(h, carry):
                r = pl.ds(pl.multiple_of(h * part_rows, part_rows), part_rows)
                gu = jnp.dot(xbuf[xslot, r, :], wbuf[wslot], preferred_element_type=jnp.float32)
                gate = gu[:, :tn].astype(jnp.bfloat16).astype(jnp.float32)
                up = gu[:, tn:].astype(jnp.bfloat16).astype(jnp.float32)
                hout[hslot, h] = (jax.nn.silu(gate) * up).astype(jnp.bfloat16)
                return carry

            with jax.named_scope("gumm"):
                lax.fori_loop(0, 2, part, 0)
            h_write(g).start()

        @pl.when(g == 2 * nt)
        def _():
            all_sent()

        @pl.when(g == ng)
        def _():
            for n in range(nz):
                late_load(jnp.int32(n)).start()


        done, tiles = jnp.where(g == early, early, forwards(g - 1)), jnp.minimum(g + 1, ng)
        send(issued(done, jnp.minimum(g, ng)), issued(done, tiles))

        with jax.named_scope("fwd"):
            @pl.when(forwards(g) > done)
            def _():
                serve(done, tiles)

        @pl.when((g >= 1) & (g <= ng))
        def _():
            h_write(g - 1).wait()

        lax.fori_loop(z_done(g - 1), z_done(g), z_tile, 0)

        with jax.named_scope("fwd"):
            @pl.when(forwards(g) > done + 1)
            def _():
                serve(done + 1, tiles)

        return carry

    lax.fori_loop(0, early + ng, body, 0)

    for slot in range(2):
        o_write(jnp.int32(whole - 1), slot, slot).wait()
    with jax.named_scope("harr"):
        pull(last_q, last_q, 0, nt - 2)
    total(zin.at[0], zr.at[2 * RING - 3])
    for n in range(nz):
        zin_load(jnp.int32(whole + n), n, 3).start()
    with jax.named_scope("hzload"):
        pulled(last_q, 0, nt - 2)
    lax.fori_loop(0, nz, tail_first, 0)
    with jax.named_scope("harr"):
        pull(last_q, last_q + 1, nt - 2, nt)
    with jax.named_scope("hzload"):
        total(wd.at[wd_rows[2]], wdsem.at[WD_SLOTS])
        total(zinb, zinsem.at[3])
        pulled(last_q, nt - 2, nt)
    lax.fori_loop(0, nz, tail_second, 0)

    for i in range(ni - 2, ni):
        h_long(jnp.int32(i)).wait_send()
        h_short(jnp.int32(i)).wait_send()
    for i in range(ni - 4, ni):
        h_fwd(jnp.int32(i)).wait_send()
    for z in range(max(0, whole - Z_SLOTS), nsum):
        z_send(z).wait_send()
    with jax.named_scope("owait"):
        total(out.at[pl.ds(0, part_rows)], osem.at[2])


def _local(x_blk, wg_blk, wu_blk, wd_blk):
    rows, kb = x_blk.shape
    hc = wg_blk.shape[1] // RING
    mc = wd_blk.shape[1]
    tn, zn = _tile(2 * hc, 256), _tile(2 * mc, 256)
    nt, nz = 2 * hc // tn, 2 * mc // zn
    bf16, f32 = jnp.bfloat16, jnp.float32
    hbm = pl.BlockSpec(memory_space=pl.ANY)
    half = rows // 2
    dma = pltpu.SemaphoreType.DMA
    flops = 2 * RING * rows * (RING * kb * 4 * hc + wd_blk.shape[0] * 2 * mc)
    res = pl.pallas_call(
        _kernel,
        name="ring_mlp",
        out_shape=(
            jax.ShapeDtypeStruct((rows, 2 * mc), bf16),
            jax.ShapeDtypeStruct((RING, RING, rows, kb), bf16),
            jax.ShapeDtypeStruct((2, RING * kb, 2 * hc), bf16),
            jax.ShapeDtypeStruct((2, kb, hc), bf16),
            jax.ShapeDtypeStruct((RING, RING, 2, nt, half, tn), bf16),
            jax.ShapeDtypeStruct(wd_blk.shape, bf16),
            jax.ShapeDtypeStruct((wd_blk.shape[0], 2 * mc), bf16),
            jax.ShapeDtypeStruct((2 * (RING - 1), nz, half, zn), f32),
        ),
        in_specs=[hbm] * 4,
        out_specs=(hbm,) * 8,
        scratch_shapes=[
            pltpu.VMEM((2, rows, RING * kb), bf16),
            pltpu.VMEM((2, RING * kb, 2 * tn), bf16),
            pltpu.VMEM((2, half, wd_blk.shape[0]), bf16),
            pltpu.VMEM((WD_SLOTS, wd_blk.shape[0], zn), bf16),
            pltpu.VMEM((nz, half, zn), f32),
            pltpu.VMEM((Z_SLOTS + 1, half, zn), f32),
            pltpu.VMEM((nz, half, zn), f32),
            pltpu.VMEM((nz, half, zn), bf16),
            pltpu.VMEM((H_SLOTS, 2, half, tn), bf16),
            dma((5,)), dma((N_RECV,)), dma((3,)), dma((3,)),
            dma((2,)), dma((2,)), dma((1,)), dma((WD_SLOTS + 1,)), dma((4,)), dma((3,)),
            dma((8,)), dma((2 * RING * nt,)), dma((8,)), dma((2 * RING + 1,)),
            dma((8,)), dma((2 * RING + 1,)), dma((2,)),
            dma((Z_SLOTS,)), dma((2 * (RING - 1),)),
        ],
        compiler_params=pltpu.CompilerParams(collective_id=0, has_side_effects=True, vmem_limit_bytes=67043328),
        cost_estimate=pl.CostEstimate(flops=flops, bytes_accessed=flops // 500, transcendentals=0),
    )(x_blk, wg_blk, wu_blk, wd_blk)
    return res[0]


def solution(mesh):
    assert mesh.shape["dz"] == RING and mesh.shape["dy"] == RING and mesh.shape["dx"] == 2
    x_spec = P(("grp", "dx", "dz"), "dy")
    w_in_spec = P("dy", ("dz", "dx"))
    w_out_spec = P("dz", ("dy", "dx"))
    return jax.shard_map(_local, mesh=mesh, in_specs=(x_spec, w_in_spec, w_in_spec, w_out_spec), out_specs=x_spec, check_vma=False)
```

```python
import jax
import jax.numpy as jnp
from jax import lax
from jax.experimental import pallas as pl
from jax.experimental.pallas import tpu as pltpu
from jax.sharding import PartitionSpec as P

MESH = pl.DeviceIdType.MESH
RING = 4
H_SLOTS = 7
Z_SLOTS = 6
AHEAD = 3
WD_SLOTS = 3
XL, XS, XF, YL, YS, YF, WN, W2, WF, WL, SW, SD, P1 = 0, 2, 3, 5, 9, 13, 17, 21, 25, 29, 33, 49, 50
JOINT = (
    (XF, XF + 1), tuple(range(YS, YF)), tuple(range(YF, WN)), (WN, WN + 1), (WN + 2, WN + 3), (WF, WF + 1),
    tuple(SW + 4 * j + u for j in range(RING) for u in range(2)), tuple(SW + 4 * j + 2 + u for j in range(RING) for u in range(2)),
)
RECV = {}
for _i in range(P1):
    _group = next((g for g in JOINT if _i in g), (_i,))
    RECV[_i] = RECV[_group[0]] if _i != _group[0] else len(set(RECV.values()))
N_RECV = len(set(RECV.values()))


def _tile(extent, most):
    return next(t for t in range(most, 0, -128) if extent % t == 0)


def _kernel(x_in, wg_in, wu_in, wd_in, z_half, z_part, xg, wgu, ws, hg, wds, wd, zin,
            xbuf, wbuf, hz, wdbuf, zinb, zout, zacc, ofin, hout,
            p1s, p1r, bin_s, bout_s, xsem, wsem, hzsem, wdsem, zinsem, osem,
            ols, olr, oss, osr, fs, fr, hws, zs, zr):
    rows, kb = x_in.shape
    hc = wg_in.shape[1] // RING
    nloc = wg_in.shape[1]
    hq = 2 * hc
    mc = wd_in.shape[1]
    part_rows, tn = hout.shape[2:]
    zn = zout.shape[2]
    nt = hq // tn
    nz = 2 * mc // zn
    ng = RING * nt
    ni = 2 * ng
    zstart = nt + 2
    early = (nt + 1) // 2
    pc = (early * tn // 2, hc - early * tn // 2)
    p_src, p_dst = (0, pc[0]), (0, 2 * pc[0])

    b = lax.axis_index("dz")
    a = lax.axis_index("dy")
    c = lax.axis_index("dx")
    step = 1 - 2 * c
    al = lax.rem(a + step + RING, RING)
    ash = lax.rem(a - step + RING, RING)
    a2 = lax.rem(a + 2, RING)
    bl = lax.rem(b + step + RING, RING)
    bsh = lax.rem(b - step + RING, RING)
    xl, xs_ = {"dy": al}, {"dy": ash}
    yl, ys_ = {"dz": bl}, {"dz": bsh}
    sib = {"dx": 1 - c}
    kbs = (a, ash, al, a2)
    w_in = (wg_in, wu_in)

    def dest(s):
        return lax.rem(b - step * (1 + s) + 2 * RING, RING)

    def rc(src, dst, ss, rs, dev):
        return pltpu.make_async_remote_copy(src_ref=src, dst_ref=dst, send_sem=ss, recv_sem=rs, device_id=dev, device_id_type=MESH)

    def lanes(i, n):
        return pl.ds(pl.multiple_of(i * n, 128), n)

    def krows(k):
        return pl.ds(pl.multiple_of(k * kb, 16), kb)

    half = rows // 2

    def w_piece(u, p, q):
        return w_in[u].at[:, pl.ds(pl.multiple_of(q * hc + p_src[p], 128), pc[p])]

    def w_place(u, p, k):
        return wgu.at[u, krows(k), pl.ds(pl.multiple_of(p_dst[p] + c * pc[p], 128), pc[p])]

    def p1(i):
        kind = 0 if i < YL else 1 if i < WN else 2 if i < SW else 3 if i < SD else 4
        sem = (p1s.at[kind], p1r.at[RECV[i]])
        if i < XS:
            r = pl.ds((i - XL) * half, half)
            return rc(x_in.at[r], xg.at[b, a, r], *sem, xl)
        if i < XF:
            return rc(x_in, xg.at[b, a], *sem, xs_)
        if i < YL:
            r = pl.ds((i - XF) * half, half)
            return rc(xg.at[b, ash, r], xg.at[b, ash, r], *sem, xl)
        if i < YF:
            j = (i - YL) % RING
            src = x_in if j == 0 else xg.at[b, kbs[j]]
            return rc(src, xg.at[b, kbs[j]], *sem, yl if i < YS else ys_)
        if i < WN:
            j = i - YF
            return rc(xg.at[bsh, kbs[j]], xg.at[bsh, kbs[j]], *sem, yl)
        if i < WF:
            u, p = (i - WN) % 2, (i - WN) % 4 // 2
            if i < W2:
                return rc(w_piece(u, p, ash), w_place(u, p, a), *sem, xs_)
            return rc(w_piece(u, p, a2), ws.at[u, :, pl.ds(p_src[p], pc[p])], *sem, xl)
        if i < WL:
            u, p = (i - WF) % 2, (i - WF) // 2
            return rc(ws.at[u, :, pl.ds(p_src[p], pc[p])], w_place(u, p, ash), *sem, xl)
        if i < SW:
            u, p = (i - WL) % 2, (i - WL) // 2
            return rc(w_piece(u, p, al), w_place(u, p, a), *sem, xl)
        if i < SD:
            j, p, u = (i - SW) // 4, (i - SW) % 4 // 2, (i - SW) % 2
            dst = w_place(u, p, kbs[j])
            return rc(w_piece(u, p, a) if j == 0 else dst, dst, *sem, sib)
        return rc(wd_in, wds, *sem, sib)

    def go(*idx):
        for i in idx:
            p1(i).start()

    def got(*idx):
        for i in idx:
            with jax.named_scope(f"got{i}"):
                p1(i).wait_recv()

    def total(ref, sem):
        pltpu.make_async_copy(ref, ref, sem).wait()

    def got_all(first, ref):
        with jax.named_scope(f"got{first}"):
            total(ref, p1r.at[RECV[first]])

    def part_of(u_refs, p):
        return u_refs.at[:, :, pl.ds(p_src[p], pc[p])]

    def all_sent():
        quarter = wgu.at[:, :, pl.ds(0, hc)]
        for kind, ref in enumerate((xg.at[0, pl.ds(0, 3)], xg.at[pl.ds(0, 3)], quarter, quarter, wds)):
            total(ref, p1s.at[kind])

    barrier = pltpu.get_barrier_semaphore()
    for dev in (xl, xs_, yl, ys_, sib):
        pl.semaphore_signal(barrier, inc=1, device_id=dev, device_id_type=MESH)
    with jax.named_scope("barrier"):
        pl.semaphore_wait(barrier, 5)

    go(XL, XL + 1, XS, YL, YS, SD, SW, SW + 1, SW + 2, SW + 3, WN, WN + 1)

    def bounce(*classes):
        for i, (size, moves) in enumerate(classes):
            for src, mid, _ in moves:
                pltpu.make_async_copy(src, mid, bin_s.at[i]).start()
        for i, (size, moves) in enumerate(classes):
            total(size, bin_s.at[i])
            for _, _, parts in moves:
                for piece, dst in parts:
                    pltpu.make_async_copy(piece, dst, bout_s.at[i]).start()
        for i, (size, moves) in enumerate(classes):
            total(size, bout_s.at[i])

    def w_down_moves(src, core):
        moves = []
        for cc in range(2):
            for k in range(RING):
                cols = pl.ds((cc * RING + k) * mc, mc)
                parts = []
                for p in range(2):
                    at, end = p_dst[p] + cc * pc[p], p_dst[p] + (cc + 1) * pc[p]
                    while at < end:
                        n = min(end, (at // tn + 1) * tn) - at
                        row = p_src[p] + at - p_dst[p] - cc * pc[p]
                        dst = wd.at[pl.ds((at // tn * RING + k) * tn + at % tn, n), lanes(core, mc)]
                        parts.append((xbuf.at[1, pl.ds(row, n), cols], dst))
                        at += n
                moves.append((src.at[pl.ds(cc * nloc + k * hc, hc)], xbuf.at[1, pl.ds(0, hc), cols], parts))
        return moves

    x_moves = [(x_in, xbuf.at[0, :, pl.ds(0, kb)], [(xbuf.at[0, :, pl.ds(0, kb)], xg.at[b, a])])]
    w_moves, col = [], kb
    for u in range(2):
        for r0 in range(0, kb, rows):
            n = min(rows, kb - r0)
            parts = []
            for p in range(2):
                dst = wgu.at[u, pl.ds(pl.multiple_of(a * kb + r0, 16), n), pl.ds(pl.multiple_of(p_dst[p] + c * pc[p], 128), pc[p])]
                parts.append((xbuf.at[0, pl.ds(0, n), pl.ds(col + p_src[p], pc[p])], dst))
            w_moves.append((w_in[u].at[pl.ds(r0, n), lanes(a, hc)], xbuf.at[0, pl.ds(0, n), pl.ds(col, hc)], parts))
            col += hc
    with jax.named_scope("bounce"):
        bounce((x_in, x_moves), (ws, w_moves), (wd_in, w_down_moves(wd_in, c)))
        zinb[...] = jnp.zeros_like(zinb)

    got(XL)
    go(XF)
    got(XL + 1)
    go(XF + 1, W2, W2 + 1, YL + 1)
    got(XS)
    go(YL + 2, WN + 2, WN + 3)
    got(YL)
    go(YF)
    got_all(XF, xg.at[0, 0])
    go(YL + 3, WL)
    got(YL + 1)
    go(YF + 1)
    got(SD)
    with jax.named_scope("bounce"):
        bounce((wds, w_down_moves(wds, 1 - c)))
    got(W2)
    go(WF)
    got(W2 + 1)
    go(WF + 1, WL + 1, W2 + 2, W2 + 3)
    got(YL + 2)
    go(YF + 2)
    got_all(WN, part_of(ws, 0))
    go(SW + 8, SW + 9)
    got(YL + 3)
    go(YF + 3)
    got(WL)
    go(SW + 4)
    got_all(WF, part_of(ws, 0))
    go(SW + 12, SW + 13)
    got(WL + 1)
    go(SW + 5, WL + 2, YS + 1)
    got(W2 + 2)
    go(WF + 2)
    got(W2 + 3)
    go(WF + 3, WL + 3)

    def x_load(s, k):
        return pltpu.make_async_copy(xg.at[dest(s), k], xbuf.at[lax.rem(s, 2), :, pl.ds(k * kb, kb)], xsem.at[lax.rem(s, 2)])

    def w_load(g, u):
        slot = lax.rem(g, 2)
        return pltpu.make_async_copy(wgu.at[u, :, lanes(lax.rem(g, nt), tn)], wbuf.at[slot, :, pl.ds(u * tn, tn)], wsem.at[slot])

    ka = RING * tn * (nt - 2)
    whole, nzt = (2 * RING - 1) * nz, 2 * RING * nz
    wd_rows = (pl.ds(0, RING * hq), pl.ds(0, ka))


    def wd_load(w, kind):
        slot = lax.rem(w, WD_SLOTS)
        return pltpu.make_async_copy(wd.at[wd_rows[kind], lanes(lax.rem(w, nz), zn)], wdbuf.at[slot, wd_rows[kind]], wdsem.at[slot])

    def wd_fetch(w):
        for kind, (lo, hi) in enumerate(((0, whole), (whole, nzt))):
            @pl.when((w >= lo) & (w < hi))
            def _():
                wd_load(w, kind).start()

    def zin_load(z, slot, sem):
        return pltpu.make_async_copy(zin.at[z // nz - 2, lax.rem(z, nz)], zinb.at[slot], zinsem.at[sem])

    def pairs(s):
        return jnp.maximum(early - s, 0)

    def item_of(s, h, t):
        m = pairs(s)
        return 2 * nt * s + jnp.where(t < m, 2 * t + h, 2 * m + h * (nt - m) + t - m)

    def place_of(i):
        s, v = i // (2 * nt), lax.rem(i, 2 * nt)
        m = pairs(s)
        w = jnp.maximum(v - 2 * m, 0)
        late = jnp.where(w >= nt - m, 1, 0)
        h = jnp.where(v < 2 * m, lax.rem(v, 2), late)
        t = jnp.where(v < 2 * m, v // 2, m + w - late * (nt - m))
        return s, h, t

    def h_write(g):
        slot = lax.rem(g, H_SLOTS)
        return pltpu.make_async_copy(hout.at[slot], hg.at[dest(g // nt), a, :, lax.rem(g, nt)], hws.at[lax.rem(g, 2)])

    def half_of(s, h, t):
        q = 2 * s + h
        return q + jnp.where((q == 2 * RING - 1) & (t >= nt - 2), 1, 0)

    def h_long(i):
        s, h, t = place_of(i)
        return rc(hout.at[lax.rem(s * nt + t, H_SLOTS), h], hg.at[dest(s), a, h, t], ols.at[lax.rem(i, 8)], olr.at[i], xl)

    def h_short(i):
        s, h, t = place_of(i)
        return rc(hout.at[lax.rem(s * nt + t, H_SLOTS), h], hg.at[dest(s), a, h, t], oss.at[lax.rem(i, 8)], osr.at[half_of(s, h, t)], xs_)

    def h_fwd(i):
        s, h, t = place_of(i)
        blk = hg.at[dest(s), ash, h, t]
        return rc(blk, blk, fs.at[lax.rem(i, 8)], fr.at[half_of(s, h, t)], xl)

    def ready(tiles):
        s, r = tiles // nt, lax.rem(tiles, nt)
        m = pairs(s)
        return 2 * nt * s + jnp.where(r <= m, 2 * r, m + r)

    def issued(forwards, tiles):
        return jnp.minimum(forwards + AHEAD, ready(tiles))

    def send(lo, hi):
        def one(i, carry):
            h_long(i).start()
            h_short(i).start()
            return carry

        lax.fori_loop(lo, hi, one, 0)

    def forwards(g):
        return jnp.where(g < early, 0, jnp.minimum(jnp.maximum(early, 2 * (g - early) + 2), ni))

    def serve(j, tiles):
        h_long(j).wait_recv()
        h_fwd(j).start()
        send(issued(j, tiles), issued(j + 1, tiles))

        @pl.when(j >= 2)
        def _():
            h_long(j - 2).wait_send()
            h_short(j - 2).wait_send()

        @pl.when(j >= 4)
        def _():
            h_fwd(j - 4).wait_send()

    def pull(q, sem, lo, hi):
        s, h = q // 2, lax.rem(q, 2)
        arrived = hg.at[0, 0, 0, pl.ds(lo, hi - lo)]
        total(arrived, osr.at[sem])
        total(arrived, fr.at[sem])

        def one(t, carry):
            for k in range(RING):
                pltpu.make_async_copy(hg.at[dest(s), k, h, t], hz.at[lax.rem(q, 2), :, lanes(t * RING + k, tn)], hzsem.at[0]).start()
            return carry

        lax.fori_loop(lo, hi, one, 0)

    def pulled(q, lo, hi):
        total(hz.at[lax.rem(q, 2), :, pl.ds(lo * RING * tn, (hi - lo) * RING * tn)], hzsem.at[0])

    def z_send(z):
        slot = lax.rem(z, Z_SLOTS)
        return rc(zout.at[slot], zin.at[z // nz, lax.rem(z, nz)], zs.at[slot], zr.at[z // nz], yl)

    def o_write(z, slot):
        return pltpu.make_async_copy(ofin.at[slot], z_half.at[:, lanes(lax.rem(z, nz), zn)], osem.at[slot])

    def start_w(g):
        w_load(g, 0).start()
        w_load(g, 1).start()

    for k in range(RING):
        x_load(0, k).start()
    got_all(SW, wgu.at[:, :, pl.ds(p_dst[0], pc[0])])
    start_w(0)

    nsum = 2 * (RING - 1) * nz

    def z_tile(z, carry):
        q, slot, wslot = z // nz, lax.rem(z, 2), lax.rem(z, WD_SLOTS)
        wd_fetch(z + 2)

        @pl.when(lax.rem(z, nz) == 0)
        def _():
            with jax.named_scope("harr"):
                pull(q, q, 0, nt)
            with jax.named_scope("hzload"):
                pulled(q, 0, nt)

        with jax.named_scope("zinrecv"):
            @pl.when((z + 2 >= 2 * nz) & (z + 2 < whole))
            def _():
                @pl.when(lax.rem(z + 2, nz) == 0)
                def _():
                    total(zin.at[0], zr.at[(z + 2) // nz - 2])

                zin_load(z + 2, lax.rem(z + 2, 3), lax.rem(z + 2, 3)).start()

        with jax.named_scope("wdwait"):
            wd_load(z, 0).wait()

        with jax.named_scope("zinwait"):
            @pl.when(z >= 2 * nz)
            def _():
                zin_load(z, lax.rem(z, 3), lax.rem(z, 3)).wait()

        with jax.named_scope("zslot"):
            @pl.when((z >= Z_SLOTS) & (z - Z_SLOTS < nsum))
            def _():
                z_send(z - Z_SLOTS).wait_send()

        @pl.when(z - 2 >= nsum)
        def _():
            o_write(z - 2, slot).wait()

        zslot = jnp.where(z < nsum, lax.rem(z, Z_SLOTS), Z_SLOTS)
        with jax.named_scope("zmm"):
            acc = jnp.dot(hz[lax.rem(q, 2)], wdbuf[wslot], preferred_element_type=jnp.float32) + zinb[lax.rem(z, 3)]
            zout[zslot] = acc
            ofin[slot] = acc.astype(jnp.bfloat16)

        @pl.when(z < nsum)
        def _():
            z_send(z).start()

        @pl.when(z >= nsum)
        def _():
            o_write(z, slot).start()

        return carry

    last_q = 2 * RING - 1

    def tail_first(n, carry):
        w = whole + n
        wd_fetch(w + 2)
        wd_load(w, 1).wait()
        with jax.named_scope("za"):
            zacc[n] = jnp.dot(hz[1, :, wd_rows[1]], wdbuf[lax.rem(w, WD_SLOTS), wd_rows[1]], preferred_element_type=jnp.float32)
        pltpu.make_async_copy(zacc.at[n], z_part.at[n], osem.at[2]).start()
        return carry

    def z_done(g):
        q, k = jnp.maximum(g - zstart, 0), g - zstart - 2 * nt + 1
        steady = 2 * nz * (q // nt) + 2 * nz * (lax.rem(q, nt) + 1) // nt
        ending = 4 * nz + 3 * nz * k // (early + ng - zstart - 2 * nt)
        return jnp.where(g < zstart, 0, jnp.where(k > 0, ending, steady))

    def body(g, carry):
        s, t = g // nt, lax.rem(g, nt)

        @pl.when(g == early - 1)
        def _():
            got_all(WN + 2, part_of(ws, 1))
            go(SW + 10, SW + 11)
            got(WL + 2)
            go(SW + 6)
            got(WF + 2)
            go(SW + 14)

        @pl.when(g == early)
        def _():
            got(WF + 3)
            go(SW + 15)
            got(WL + 3)
            go(SW + 7, YS + 2, YS + 3)

            def first(j, carry):
                serve(j, early)
                return carry

            lax.fori_loop(0, early, first, 0)
            got_all(SW + 2, wgu.at[:, :, pl.ds(p_dst[1], pc[1])])
            start_w(g)
            wd_load(0, 0).start()
            wd_load(1, 0).start()

        @pl.when(g < ng)
        def _():
            @pl.when((g + 1 < ng) & (g + 1 != early))
            def _():
                start_w(g + 1)

            @pl.when((t == nt - 1) & (g + 1 < ng))
            def _():
                @pl.when(s + 1 == 1)
                def _():
                    got_all(YF, xg.at[0])

                @pl.when(s + 1 == 2)
                def _():
                    got_all(YS, xg.at[0])

                for k in range(RING):
                    x_load(s + 1, k).start()

            with jax.named_scope("xwait"):
                @pl.when(t == 0)
                def _():
                    total(xbuf.at[lax.rem(s, 2)], xsem.at[lax.rem(s, 2)])

            with jax.named_scope("wwait"):
                total(wbuf.at[lax.rem(g, 2)], wsem.at[lax.rem(g, 2)])

            xslot, wslot, hslot = lax.rem(s, 2), lax.rem(g, 2), lax.rem(g, H_SLOTS)

            def part(h, carry):
                r = pl.ds(pl.multiple_of(h * part_rows, part_rows), part_rows)
                gu = jnp.dot(xbuf[xslot, r, :], wbuf[wslot], preferred_element_type=jnp.float32)
                gate = gu[:, :tn].astype(jnp.bfloat16).astype(jnp.float32)
                up = gu[:, tn:].astype(jnp.bfloat16).astype(jnp.float32)
                hout[hslot, h] = (jax.nn.silu(gate) * up).astype(jnp.bfloat16)
                return carry

            with jax.named_scope("gumm"):
                lax.fori_loop(0, 2, part, 0)
            h_write(g).start()

        @pl.when(g == 2 * nt)
        def _():
            all_sent()

        done, tiles = jnp.where(g == early, early, forwards(g - 1)), jnp.minimum(g + 1, ng)
        send(issued(done, jnp.minimum(g, ng)), issued(done, tiles))

        with jax.named_scope("fwd"):
            @pl.when(forwards(g) > done)
            def _():
                serve(done, tiles)

        @pl.when((g >= 1) & (g <= ng))
        def _():
            h_write(g - 1).wait()

        lax.fori_loop(z_done(g - 1), z_done(g), z_tile, 0)

        with jax.named_scope("fwd"):
            @pl.when(forwards(g) > done + 1)
            def _():
                serve(done + 1, tiles)

        return carry

    lax.fori_loop(0, early + ng, body, 0)

    with jax.named_scope("harr"):
        pull(last_q, last_q, 0, nt - 2)
    with jax.named_scope("hzload"):
        pulled(last_q, 0, nt - 2)
    lax.fori_loop(0, nz, tail_first, 0)
    with jax.named_scope("harr"):
        arrived = hg.at[0, 0, 0, pl.ds(0, 2)]
        total(arrived, osr.at[last_q + 1])
        total(arrived, fr.at[last_q + 1])
        total(zin.at[0], zr.at[2 * RING - 3])

    with jax.named_scope("drain"):
        for i in range(ni - 2, ni):
            h_long(jnp.int32(i)).wait_send()
            h_short(jnp.int32(i)).wait_send()
        for i in range(ni - 4, ni):
            h_fwd(jnp.int32(i)).wait_send()
        for z in range(max(0, whole - Z_SLOTS), nsum):
            z_send(z).wait_send()
        for slot in range(2):
            o_write(jnp.int32(whole - 1), slot).wait()
        total(z_part, osem.at[2])


def _finish(hg, wd, zin, z_part, z_half, out, hz, wdb, zinb, accb, keep, res, hsem, wsem, zsem, asem, ksem, osem):
    rows, tn = hg.shape[4:]
    nz, _, zn = z_part.shape
    nt = hg.shape[3]
    ka = RING * tn * (nt - 2)
    b = lax.axis_index("dz")
    top, low = pl.ds(0, rows), pl.ds(rows, rows)

    for t in range(2):
        for k in range(RING):
            pltpu.make_async_copy(hg.at[b, k, 1, nt - 2 + t], hz.at[:, pl.ds((t * RING + k) * tn, tn)], hsem.at[0]).start()
    loads = [
        (
            pltpu.make_async_copy(wd.at[pl.ds(ka, 2 * RING * tn), pl.ds(n * zn, zn)], wdb.at[n], wsem.at[n]),
            pltpu.make_async_copy(z_part.at[n], accb.at[n], asem.at[n]),
            pltpu.make_async_copy(zin.at[zin.shape[0] - 1, n], zinb.at[n], zsem.at[n]),
        )
        for n in range(nz)
    ]
    for group in loads:
        for copy in group:
            copy.start()
    first = pltpu.make_async_copy(z_half, keep, ksem.at[0])
    first.start()
    pltpu.make_async_copy(hz, hz, hsem.at[0]).wait()

    writes = [pltpu.make_async_copy(res.at[n], out.at[low, pl.ds(n * zn, zn)], osem.at[n]) for n in range(nz)]
    for n in range(nz):
        for copy in loads[n]:
            copy.wait()
        acc = jnp.dot(hz[...], wdb[n], preferred_element_type=jnp.float32)
        res[n] = (acc + accb[n] + zinb[n]).astype(jnp.bfloat16)
        writes[n].start()
        if n == nz // 2:
            first.wait()
            second = pltpu.make_async_copy(keep, out.at[top], ksem.at[1])
            second.start()
    for copy in writes:
        copy.wait()
    second.wait()


def _local(x_blk, wg_blk, wu_blk, wd_blk):
    rows, kb = x_blk.shape
    hc = wg_blk.shape[1] // RING
    mc = wd_blk.shape[1]
    tn, zn = _tile(2 * hc, 256), _tile(2 * mc, 256)
    nt, nz = 2 * hc // tn, 2 * mc // zn
    bf16, f32 = jnp.bfloat16, jnp.float32
    hbm = pl.BlockSpec(memory_space=pl.ANY)
    half = rows // 2
    dma = pltpu.SemaphoreType.DMA
    flops = 2 * RING * rows * (RING * kb * 4 * hc + wd_blk.shape[0] * 2 * mc)
    res = pl.pallas_call(
        _kernel,
        name="ring_mlp",
        out_shape=(
            jax.ShapeDtypeStruct((half, 2 * mc), bf16),
            jax.ShapeDtypeStruct((nz, half, zn), f32),
            jax.ShapeDtypeStruct((RING, RING, rows, kb), bf16),
            jax.ShapeDtypeStruct((2, RING * kb, 2 * hc), bf16),
            jax.ShapeDtypeStruct((2, kb, hc), bf16),
            jax.ShapeDtypeStruct((RING, RING, 2, nt, half, tn), bf16),
            jax.ShapeDtypeStruct(wd_blk.shape, bf16),
            jax.ShapeDtypeStruct((wd_blk.shape[0], 2 * mc), bf16),
            jax.ShapeDtypeStruct((2 * (RING - 1), nz, half, zn), f32),
        ),
        in_specs=[hbm] * 4,
        out_specs=(hbm,) * 9,
        scratch_shapes=[
            pltpu.VMEM((2, rows, RING * kb), bf16),
            pltpu.VMEM((2, RING * kb, 2 * tn), bf16),
            pltpu.VMEM((2, half, wd_blk.shape[0]), bf16),
            pltpu.VMEM((WD_SLOTS, wd_blk.shape[0], zn), bf16),
            pltpu.VMEM((3, half, zn), f32),
            pltpu.VMEM((Z_SLOTS + 1, half, zn), f32),
            pltpu.VMEM((nz, half, zn), f32),
            pltpu.VMEM((2, half, zn), bf16),
            pltpu.VMEM((H_SLOTS, 2, half, tn), bf16),
            dma((5,)), dma((N_RECV,)), dma((3,)), dma((3,)),
            dma((2,)), dma((2,)), dma((1,)), dma((WD_SLOTS,)), dma((3,)), dma((3,)),
            dma((8,)), dma((2 * RING * nt,)), dma((8,)), dma((2 * RING + 1,)),
            dma((8,)), dma((2 * RING + 1,)), dma((2,)),
            dma((Z_SLOTS,)), dma((2 * (RING - 1),)),
        ],
        compiler_params=pltpu.CompilerParams(collective_id=0, has_side_effects=True, vmem_limit_bytes=67043328),
        cost_estimate=pl.CostEstimate(flops=flops, bytes_accessed=flops // 500, transcendentals=0),
    )(x_blk, wg_blk, wu_blk, wd_blk)
    z_half, z_part, hg, wd, zin = res[0], res[1], res[5], res[7], res[8]
    flops = 2 * half * 2 * RING * tn * 2 * mc
    return pl.pallas_call(
        _finish,
        name="last_part",
        out_shape=jax.ShapeDtypeStruct((rows, 2 * mc), bf16),
        in_specs=[hbm] * 5,
        out_specs=hbm,
        scratch_shapes=[
            pltpu.VMEM((half, 2 * RING * tn), bf16),
            pltpu.VMEM((nz, 2 * RING * tn, zn), bf16),
            pltpu.VMEM((nz, half, zn), f32),
            pltpu.VMEM((nz, half, zn), f32),
            pltpu.VMEM((half, 2 * mc), bf16),
            pltpu.VMEM((nz, half, zn), bf16),
            dma((1,)), dma((nz,)), dma((nz,)), dma((nz,)), dma((2,)), dma((nz,)),
        ],
        compiler_params=pltpu.CompilerParams(vmem_limit_bytes=67043328),
        cost_estimate=pl.CostEstimate(flops=flops, bytes_accessed=flops // 500, transcendentals=0),
    )(hg, wd, zin, z_part, z_half)


def solution(mesh):
    assert mesh.shape["dz"] == RING and mesh.shape["dy"] == RING and mesh.shape["dx"] == 2
    x_spec = P(("grp", "dx", "dz"), "dy")
    w_in_spec = P("dy", ("dz", "dx"))
    w_out_spec = P("dz", ("dy", "dx"))
    return jax.shard_map(_local, mesh=mesh, in_specs=(x_spec, w_in_spec, w_in_spec, w_out_spec), out_specs=x_spec, check_vma=False)
```

```python
import jax
import jax.numpy as jnp
from jax import lax
from jax.experimental import pallas as pl
from jax.experimental.pallas import tpu as pltpu
from jax.sharding import PartitionSpec as P

MESH = pl.DeviceIdType.MESH
RING = 4
H_SLOTS = 7
Z_SLOTS = 6
AHEAD = 3
WD_SLOTS = 3
XL, XS, XF, YL, YS, YF, WN, W2, WF, WL, SW, SD, P1 = 0, 2, 3, 5, 9, 13, 17, 21, 25, 29, 33, 49, 50
JOINT = (
    (XF, XF + 1), tuple(range(YS, YF)), tuple(range(YF, WN)), (WN, WN + 1), (WN + 2, WN + 3), (WF, WF + 1),
    tuple(SW + 4 * j + u for j in range(RING) for u in range(2)), tuple(SW + 4 * j + 2 + u for j in range(RING) for u in range(2)),
)
RECV = {}
for _i in range(P1):
    _group = next((g for g in JOINT if _i in g), (_i,))
    RECV[_i] = RECV[_group[0]] if _i != _group[0] else len(set(RECV.values()))
N_RECV = len(set(RECV.values()))


def _tile(extent, most):
    return next(t for t in range(most, 0, -128) if extent % t == 0)


def _kernel(x_in, wg_in, wu_in, wd_in, z_half, z_part, xg, wgu, ws, hg, wds, wd, zin,
            xbuf, wbuf, hz, wdbuf, zinb, zout, zacc, ofin, hout,
            p1s, p1r, bin_s, bout_s, xsem, wsem, hzsem, wdsem, zinsem, osem,
            ols, olr, oss, osr, fs, fr, hws, zs, zr):
    rows, kb = x_in.shape
    hc = wg_in.shape[1] // RING
    nloc = wg_in.shape[1]
    hq = 2 * hc
    mc = wd_in.shape[1]
    part_rows, tn = hout.shape[2:]
    zn = zout.shape[2]
    nt = hq // tn
    nz = 2 * mc // zn
    ng = RING * nt
    ni = 2 * ng
    zstart = nt + 2
    early = (nt + 1) // 2
    pc = (early * tn // 2, hc - early * tn // 2)
    p_src, p_dst = (0, pc[0]), (0, 2 * pc[0])

    b = lax.axis_index("dz")
    a = lax.axis_index("dy")
    c = lax.axis_index("dx")
    step = 1 - 2 * c
    al = lax.rem(a + step + RING, RING)
    ash = lax.rem(a - step + RING, RING)
    a2 = lax.rem(a + 2, RING)
    bl = lax.rem(b + step + RING, RING)
    bsh = lax.rem(b - step + RING, RING)
    xl, xs_ = {"dy": al}, {"dy": ash}
    yl, ys_ = {"dz": bl}, {"dz": bsh}
    sib = {"dx": 1 - c}
    kbs = (a, ash, al, a2)
    w_in = (wg_in, wu_in)

    def dest(s):
        return lax.rem(b - step * (1 + s) + 2 * RING, RING)

    def rc(src, dst, ss, rs, dev):
        return pltpu.make_async_remote_copy(src_ref=src, dst_ref=dst, send_sem=ss, recv_sem=rs, device_id=dev, device_id_type=MESH)

    def lanes(i, n):
        return pl.ds(pl.multiple_of(i * n, 128), n)

    def krows(k):
        return pl.ds(pl.multiple_of(k * kb, 16), kb)

    half = rows // 2

    def w_piece(u, p, q):
        return w_in[u].at[:, pl.ds(pl.multiple_of(q * hc + p_src[p], 128), pc[p])]

    def w_place(u, p, k):
        return wgu.at[u, krows(k), pl.ds(pl.multiple_of(p_dst[p] + c * pc[p], 128), pc[p])]

    def p1(i):
        kind = 0 if i < YL else 1 if i < WN else 2 if i < SW else 3 if i < SD else 4
        sem = (p1s.at[kind], p1r.at[RECV[i]])
        if i < XS:
            r = pl.ds((i - XL) * half, half)
            return rc(x_in.at[r], xg.at[b, a, r], *sem, xl)
        if i < XF:
            return rc(x_in, xg.at[b, a], *sem, xs_)
        if i < YL:
            r = pl.ds((i - XF) * half, half)
            return rc(xg.at[b, ash, r], xg.at[b, ash, r], *sem, xl)
        if i < YF:
            j = (i - YL) % RING
            src = x_in if j == 0 else xg.at[b, kbs[j]]
            return rc(src, xg.at[b, kbs[j]], *sem, yl if i < YS else ys_)
        if i < WN:
            j = i - YF
            return rc(xg.at[bsh, kbs[j]], xg.at[bsh, kbs[j]], *sem, yl)
        if i < WF:
            u, p = (i - WN) % 2, (i - WN) % 4 // 2
            if i < W2:
                return rc(w_piece(u, p, ash), w_place(u, p, a), *sem, xs_)
            return rc(w_piece(u, p, a2), ws.at[u, :, pl.ds(p_src[p], pc[p])], *sem, xl)
        if i < WL:
            u, p = (i - WF) % 2, (i - WF) // 2
            return rc(ws.at[u, :, pl.ds(p_src[p], pc[p])], w_place(u, p, ash), *sem, xl)
        if i < SW:
            u, p = (i - WL) % 2, (i - WL) // 2
            return rc(w_piece(u, p, al), w_place(u, p, a), *sem, xl)
        if i < SD:
            j, p, u = (i - SW) // 4, (i - SW) % 4 // 2, (i - SW) % 2
            dst = w_place(u, p, kbs[j])
            return rc(w_piece(u, p, a) if j == 0 else dst, dst, *sem, sib)
        return rc(wd_in, wds, *sem, sib)

    def go(*idx):
        for i in idx:
            p1(i).start()

    def got(*idx):
        for i in idx:
            with jax.named_scope(f"got{i}"):
                p1(i).wait_recv()

    def total(ref, sem):
        pltpu.make_async_copy(ref, ref, sem).wait()

    def got_all(first, ref):
        with jax.named_scope(f"got{first}"):
            total(ref, p1r.at[RECV[first]])

    def part_of(u_refs, p):
        return u_refs.at[:, :, pl.ds(p_src[p], pc[p])]

    def all_sent():
        quarter = wgu.at[:, :, pl.ds(0, hc)]
        for kind, ref in enumerate((xg.at[0, pl.ds(0, 3)], xg.at[pl.ds(0, 3)], quarter, quarter, wds)):
            total(ref, p1s.at[kind])

    barrier = pltpu.get_barrier_semaphore()
    for dev in (xl, xs_, yl, ys_, sib):
        pl.semaphore_signal(barrier, inc=1, device_id=dev, device_id_type=MESH)
    with jax.named_scope("barrier"):
        pl.semaphore_wait(barrier, 5)

    go(XL, XL + 1, XS, YL, YS, SD, SW, SW + 1, SW + 2, SW + 3, WN, WN + 1)

    def bounce(*classes):
        for i, (size, moves) in enumerate(classes):
            for src, mid, _ in moves:
                pltpu.make_async_copy(src, mid, bin_s.at[i]).start()
        for i, (size, moves) in enumerate(classes):
            total(size, bin_s.at[i])
            for _, _, parts in moves:
                for piece, dst in parts:
                    pltpu.make_async_copy(piece, dst, bout_s.at[i]).start()
        for i, (size, moves) in enumerate(classes):
            total(size, bout_s.at[i])

    def w_down_moves(src, core):
        moves = []
        for cc in range(2):
            for k in range(RING):
                cols = pl.ds((cc * RING + k) * mc, mc)
                parts = []
                for p in range(2):
                    at, end = p_dst[p] + cc * pc[p], p_dst[p] + (cc + 1) * pc[p]
                    while at < end:
                        n = min(end, (at // tn + 1) * tn) - at
                        row = p_src[p] + at - p_dst[p] - cc * pc[p]
                        dst = wd.at[pl.ds((at // tn * RING + k) * tn + at % tn, n), lanes(core, mc)]
                        parts.append((xbuf.at[1, pl.ds(row, n), cols], dst))
                        at += n
                moves.append((src.at[pl.ds(cc * nloc + k * hc, hc)], xbuf.at[1, pl.ds(0, hc), cols], parts))
        return moves

    x_moves = [(x_in, xbuf.at[0, :, pl.ds(0, kb)], [(xbuf.at[0, :, pl.ds(0, kb)], xg.at[b, a])])]
    w_moves, col = [], kb
    for u in range(2):
        for r0 in range(0, kb, rows):
            n = min(rows, kb - r0)
            parts = []
            for p in range(2):
                dst = wgu.at[u, pl.ds(pl.multiple_of(a * kb + r0, 16), n), pl.ds(pl.multiple_of(p_dst[p] + c * pc[p], 128), pc[p])]
                parts.append((xbuf.at[0, pl.ds(0, n), pl.ds(col + p_src[p], pc[p])], dst))
            w_moves.append((w_in[u].at[pl.ds(r0, n), lanes(a, hc)], xbuf.at[0, pl.ds(0, n), pl.ds(col, hc)], parts))
            col += hc
    with jax.named_scope("bounce"):
        bounce((x_in, x_moves), (ws, w_moves), (wd_in, w_down_moves(wd_in, c)))
        zinb[...] = jnp.zeros_like(zinb)

    got(XL)
    go(XF)
    got(XL + 1)
    go(XF + 1, W2, W2 + 1, YL + 1)
    got(XS)
    go(YL + 2, WN + 2, WN + 3)
    got(YL)
    go(YF)
    got_all(XF, xg.at[0, 0])
    go(YL + 3, WL)
    got(YL + 1)
    go(YF + 1)
    got(SD)
    with jax.named_scope("bounce"):
        bounce((wds, w_down_moves(wds, 1 - c)))
    got(W2)
    go(WF)
    got(W2 + 1)
    go(WF + 1, WL + 1, W2 + 2, W2 + 3)
    got(YL + 2)
    go(YF + 2)
    got_all(WN, part_of(ws, 0))
    go(SW + 8, SW + 9)
    got(YL + 3)
    go(YF + 3)
    got(WL)
    go(SW + 4)
    got_all(WF, part_of(ws, 0))
    go(SW + 12, SW + 13)
    got(WL + 1)
    go(SW + 5, WL + 2, YS + 1)
    got(W2 + 2)
    go(WF + 2)
    got(W2 + 3)
    go(WF + 3, WL + 3)

    def x_load(s, k):
        return pltpu.make_async_copy(xg.at[dest(s), k], xbuf.at[lax.rem(s, 2), :, pl.ds(k * kb, kb)], xsem.at[lax.rem(s, 2)])

    def w_load(g, u):
        slot = lax.rem(g, 2)
        return pltpu.make_async_copy(wgu.at[u, :, lanes(lax.rem(g, nt), tn)], wbuf.at[slot, :, pl.ds(u * tn, tn)], wsem.at[slot])

    ka = RING * tn * (nt - 2)
    whole, nzt = (2 * RING - 1) * nz, 2 * RING * nz
    wd_rows = (pl.ds(0, RING * hq), pl.ds(0, ka))


    def wd_load(w, kind):
        slot = lax.rem(w, WD_SLOTS)
        return pltpu.make_async_copy(wd.at[wd_rows[kind], lanes(lax.rem(w, nz), zn)], wdbuf.at[slot, wd_rows[kind]], wdsem.at[slot])

    def wd_fetch(w):
        for kind, (lo, hi) in enumerate(((0, whole), (whole, nzt))):
            @pl.when((w >= lo) & (w < hi))
            def _():
                wd_load(w, kind).start()

    def zin_load(z, slot, sem):
        return pltpu.make_async_copy(zin.at[z // nz - 2, lax.rem(z, nz)], zinb.at[slot], zinsem.at[sem])

    def pairs(s):
        return jnp.maximum(early - s, 0)

    def item_of(s, h, t):
        m = pairs(s)
        return 2 * nt * s + jnp.where(t < m, 2 * t + h, 2 * m + h * (nt - m) + t - m)

    def place_of(i):
        s, v = i // (2 * nt), lax.rem(i, 2 * nt)
        m = pairs(s)
        w = jnp.maximum(v - 2 * m, 0)
        late = jnp.where(w >= nt - m, 1, 0)
        h = jnp.where(v < 2 * m, lax.rem(v, 2), late)
        t = jnp.where(v < 2 * m, v // 2, m + w - late * (nt - m))
        return s, h, t

    def h_write(g):
        slot = lax.rem(g, H_SLOTS)
        return pltpu.make_async_copy(hout.at[slot], hg.at[dest(g // nt), a, :, lax.rem(g, nt)], hws.at[lax.rem(g, 2)])

    def half_of(s, h, t):
        q = 2 * s + h
        return q + jnp.where((q == 2 * RING - 1) & (t >= nt - 2), 1, 0)

    def h_long(i):
        s, h, t = place_of(i)
        return rc(hout.at[lax.rem(s * nt + t, H_SLOTS), h], hg.at[dest(s), a, h, t], ols.at[lax.rem(i, 8)], olr.at[i], xl)

    def h_short(i):
        s, h, t = place_of(i)
        return rc(hout.at[lax.rem(s * nt + t, H_SLOTS), h], hg.at[dest(s), a, h, t], oss.at[lax.rem(i, 8)], osr.at[half_of(s, h, t)], xs_)

    def h_fwd(i):
        s, h, t = place_of(i)
        blk = hg.at[dest(s), ash, h, t]
        return rc(blk, blk, fs.at[lax.rem(i, 8)], fr.at[half_of(s, h, t)], xl)

    def ready(tiles):
        s, r = tiles // nt, lax.rem(tiles, nt)
        m = pairs(s)
        return 2 * nt * s + jnp.where(r <= m, 2 * r, m + r)

    def issued(forwards, tiles):
        return jnp.minimum(forwards + AHEAD, ready(tiles))

    def send(lo, hi):
        def one(i, carry):
            h_long(i).start()
            h_short(i).start()
            return carry

        lax.fori_loop(lo, hi, one, 0)

    def forwards(g):
        return jnp.where(g < early, 0, jnp.minimum(jnp.maximum(early, 2 * (g - early) + 2), ni))

    def serve(j, tiles):
        h_long(j).wait_recv()
        h_fwd(j).start()
        send(issued(j, tiles), issued(j + 1, tiles))

        @pl.when(j >= 2)
        def _():
            h_long(j - 2).wait_send()
            h_short(j - 2).wait_send()

        @pl.when(j >= 4)
        def _():
            h_fwd(j - 4).wait_send()

    def pull(q, sem, lo, hi):
        s, h = q // 2, lax.rem(q, 2)
        arrived = hg.at[0, 0, 0, pl.ds(lo, hi - lo)]
        total(arrived, osr.at[sem])
        total(arrived, fr.at[sem])

        def one(t, carry):
            for k in range(RING):
                pltpu.make_async_copy(hg.at[dest(s), k, h, t], hz.at[lax.rem(q, 2), :, lanes(t * RING + k, tn)], hzsem.at[0]).start()
            return carry

        lax.fori_loop(lo, hi, one, 0)

    def pulled(q, lo, hi):
        total(hz.at[lax.rem(q, 2), :, pl.ds(lo * RING * tn, (hi - lo) * RING * tn)], hzsem.at[0])

    def z_send(z):
        slot = lax.rem(z, Z_SLOTS)
        return rc(zout.at[slot], zin.at[z // nz, lax.rem(z, nz)], zs.at[slot], zr.at[z // nz], yl)

    def o_write(z, slot):
        return pltpu.make_async_copy(ofin.at[slot], z_half.at[:, lanes(lax.rem(z, nz), zn)], osem.at[slot])

    def start_w(g):
        w_load(g, 0).start()
        w_load(g, 1).start()

    for k in range(RING):
        x_load(0, k).start()
    got_all(SW, wgu.at[:, :, pl.ds(p_dst[0], pc[0])])
    start_w(0)

    nsum = 2 * (RING - 1) * nz

    def z_tile(z, carry):
        q, slot, wslot = z // nz, lax.rem(z, 2), lax.rem(z, WD_SLOTS)
        wd_fetch(z + 2)

        @pl.when(lax.rem(z, nz) == 0)
        def _():
            with jax.named_scope("harr"):
                pull(q, q, 0, nt)
            with jax.named_scope("hzload"):
                pulled(q, 0, nt)

        with jax.named_scope("zinrecv"):
            @pl.when((z + 2 >= 2 * nz) & (z + 2 < whole))
            def _():
                @pl.when(lax.rem(z + 2, nz) == 0)
                def _():
                    total(zin.at[0], zr.at[(z + 2) // nz - 2])

                zin_load(z + 2, lax.rem(z + 2, 3), lax.rem(z + 2, 3)).start()

        with jax.named_scope("wdwait"):
            wd_load(z, 0).wait()

        with jax.named_scope("zinwait"):
            @pl.when(z >= 2 * nz)
            def _():
                zin_load(z, lax.rem(z, 3), lax.rem(z, 3)).wait()

        with jax.named_scope("zslot"):
            @pl.when((z >= Z_SLOTS) & (z - Z_SLOTS < nsum))
            def _():
                z_send(z - Z_SLOTS).wait_send()

        @pl.when(z - 2 >= nsum)
        def _():
            o_write(z - 2, slot).wait()

        zslot = jnp.where(z < nsum, lax.rem(z, Z_SLOTS), Z_SLOTS)
        with jax.named_scope("zmm"):
            acc = jnp.dot(hz[lax.rem(q, 2)], wdbuf[wslot], preferred_element_type=jnp.float32) + zinb[lax.rem(z, 3)]
            zout[zslot] = acc
            ofin[slot] = acc.astype(jnp.bfloat16)

        @pl.when(z < nsum)
        def _():
            z_send(z).start()

        @pl.when(z >= nsum)
        def _():
            o_write(z, slot).start()

        return carry

    last_q = 2 * RING - 1

    def tail_first(n, carry):
        w = whole + n
        wd_fetch(w + 2)
        wd_load(w, 1).wait()
        with jax.named_scope("za"):
            zacc[n] = jnp.dot(hz[1, :, wd_rows[1]], wdbuf[lax.rem(w, WD_SLOTS), wd_rows[1]], preferred_element_type=jnp.float32)
        pltpu.make_async_copy(zacc.at[n], z_part.at[n], osem.at[2]).start()
        return carry

    def z_done(g):
        q, k = jnp.maximum(g - zstart, 0), g - zstart - 2 * nt + 1
        steady = 2 * nz * (q // nt) + 2 * nz * (lax.rem(q, nt) + 1) // nt
        ending = 4 * nz + 3 * nz * k // (early + ng - zstart - 2 * nt)
        return jnp.where(g < zstart, 0, jnp.where(k > 0, ending, steady))

    def body(g, carry):
        s, t = g // nt, lax.rem(g, nt)

        @pl.when(g == early - 1)
        def _():
            got_all(WN + 2, part_of(ws, 1))
            go(SW + 10, SW + 11)
            got(WL + 2)
            go(SW + 6)
            got(WF + 2)
            go(SW + 14)

        @pl.when(g == early)
        def _():
            got(WF + 3)
            go(SW + 15)
            got(WL + 3)
            go(SW + 7, YS + 2, YS + 3)

            def first(j, carry):
                serve(j, early)
                return carry

            lax.fori_loop(0, early, first, 0)
            got_all(SW + 2, wgu.at[:, :, pl.ds(p_dst[1], pc[1])])
            start_w(g)
            wd_load(0, 0).start()
            wd_load(1, 0).start()

        @pl.when(g < ng)
        def _():
            @pl.when((g + 1 < ng) & (g + 1 != early))
            def _():
                start_w(g + 1)

            @pl.when((t == nt - 1) & (g + 1 < ng))
            def _():
                @pl.when(s + 1 == 1)
                def _():
                    got_all(YF, xg.at[0])

                @pl.when(s + 1 == 2)
                def _():
                    got_all(YS, xg.at[0])

                for k in range(RING):
                    x_load(s + 1, k).start()

            with jax.named_scope("xwait"):
                @pl.when(t == 0)
                def _():
                    total(xbuf.at[lax.rem(s, 2)], xsem.at[lax.rem(s, 2)])

            with jax.named_scope("wwait"):
                total(wbuf.at[lax.rem(g, 2)], wsem.at[lax.rem(g, 2)])

            xslot, wslot, hslot = lax.rem(s, 2), lax.rem(g, 2), lax.rem(g, H_SLOTS)

            def part(h, carry):
                r = pl.ds(pl.multiple_of(h * part_rows, part_rows), part_rows)
                gu = jnp.dot(xbuf[xslot, r, :], wbuf[wslot], preferred_element_type=jnp.float32)
                gate = gu[:, :tn].astype(jnp.bfloat16).astype(jnp.float32)
                up = gu[:, tn:].astype(jnp.bfloat16).astype(jnp.float32)
                hout[hslot, h] = (jax.nn.silu(gate) * up).astype(jnp.bfloat16)
                return carry

            with jax.named_scope("gumm"):
                lax.fori_loop(0, 2, part, 0)
            h_write(g).start()

        @pl.when(g == 2 * nt)
        def _():
            all_sent()

        done, tiles = jnp.where(g == early, early, forwards(g - 1)), jnp.minimum(g + 1, ng)
        send(issued(done, jnp.minimum(g, ng)), issued(done, tiles))

        with jax.named_scope("fwd"):
            @pl.when(forwards(g) > done)
            def _():
                serve(done, tiles)

        @pl.when((g >= 1) & (g <= ng))
        def _():
            h_write(g - 1).wait()

        lax.fori_loop(z_done(g - 1), z_done(g), z_tile, 0)

        with jax.named_scope("fwd"):
            @pl.when(forwards(g) > done + 1)
            def _():
                serve(done + 1, tiles)

        return carry

    lax.fori_loop(0, early + ng, body, 0)

    with jax.named_scope("harr"):
        pull(last_q, last_q, 0, nt - 2)
    with jax.named_scope("hzload"):
        pulled(last_q, 0, nt - 2)
    lax.fori_loop(0, nz, tail_first, 0)
    with jax.named_scope("harr"):
        arrived = hg.at[0, 0, 0, pl.ds(0, 2)]
        total(arrived, osr.at[last_q + 1])
        total(arrived, fr.at[last_q + 1])
        total(zin.at[0], zr.at[2 * RING - 3])

    with jax.named_scope("drain"):
        for i in range(ni - 2, ni):
            h_long(jnp.int32(i)).wait_send()
            h_short(jnp.int32(i)).wait_send()
        for i in range(ni - 4, ni):
            h_fwd(jnp.int32(i)).wait_send()
        for z in range(max(0, whole - Z_SLOTS), nsum):
            z_send(z).wait_send()
        for slot in range(2):
            o_write(jnp.int32(whole - 1), slot).wait()
        total(z_part, osem.at[2])


def _finish(hg, wd, zin, z_part, z_half, out, hz, wdb, zinb, accb, keep, res, hsem, wsem, zsem, asem, ksem, osem):
    rows, tn = hg.shape[4:]
    nz, _, zn = z_part.shape
    nt = hg.shape[3]
    ka = RING * tn * (nt - 2)
    b = lax.axis_index("dz")
    top, low = pl.ds(0, rows), pl.ds(rows, rows)

    for t in range(2):
        for k in range(RING):
            pltpu.make_async_copy(hg.at[b, k, 1, nt - 2 + t], hz.at[:, pl.ds((t * RING + k) * tn, tn)], hsem.at[0]).start()
    def cols(n):
        return pl.ds(pl.multiple_of(n * zn, 128), zn)

    def loads(n):
        return (
            pltpu.make_async_copy(wd.at[pl.ds(ka, 2 * RING * tn), cols(n)], wdb.at[n], wsem.at[n]),
            pltpu.make_async_copy(z_part.at[n], accb.at[n], asem.at[n]),
            pltpu.make_async_copy(zin.at[zin.shape[0] - 1, n], zinb.at[n], zsem.at[n]),
        )

    def fetch(n, carry):
        for copy in loads(n):
            copy.start()
        return carry

    lax.fori_loop(0, nz, fetch, 0)
    first = pltpu.make_async_copy(z_half, keep, ksem.at[0])
    first.start()
    pltpu.make_async_copy(hz, hz, hsem.at[0]).wait()

    def tile(n, carry):
        for copy in loads(n):
            copy.wait()
        acc = jnp.dot(hz[...], wdb[n], preferred_element_type=jnp.float32)
        res[n] = (acc + accb[n] + zinb[n]).astype(jnp.bfloat16)
        pltpu.make_async_copy(res.at[n], out.at[low, cols(n)], osem.at[0]).start()
        return carry

    lax.fori_loop(0, nz - 1, tile, 0)
    first.wait()
    second = pltpu.make_async_copy(keep, out.at[top], ksem.at[1])
    second.start()
    lax.fori_loop(nz - 1, nz, tile, 0)
    pltpu.make_async_copy(out.at[low], out.at[low], osem.at[0]).wait()
    second.wait()


def _local(x_blk, wg_blk, wu_blk, wd_blk):
    rows, kb = x_blk.shape
    hc = wg_blk.shape[1] // RING
    mc = wd_blk.shape[1]
    tn, zn = _tile(2 * hc, 256), _tile(2 * mc, 256)
    nt, nz = 2 * hc // tn, 2 * mc // zn
    bf16, f32 = jnp.bfloat16, jnp.float32
    hbm = pl.BlockSpec(memory_space=pl.ANY)
    half = rows // 2
    dma = pltpu.SemaphoreType.DMA
    flops = 2 * RING * rows * (RING * kb * 4 * hc + wd_blk.shape[0] * 2 * mc)
    res = pl.pallas_call(
        _kernel,
        name="ring_mlp",
        out_shape=(
            jax.ShapeDtypeStruct((half, 2 * mc), bf16),
            jax.ShapeDtypeStruct((nz, half, zn), f32),
            jax.ShapeDtypeStruct((RING, RING, rows, kb), bf16),
            jax.ShapeDtypeStruct((2, RING * kb, 2 * hc), bf16),
            jax.ShapeDtypeStruct((2, kb, hc), bf16),
            jax.ShapeDtypeStruct((RING, RING, 2, nt, half, tn), bf16),
            jax.ShapeDtypeStruct(wd_blk.shape, bf16),
            jax.ShapeDtypeStruct((wd_blk.shape[0], 2 * mc), bf16),
            jax.ShapeDtypeStruct((2 * (RING - 1), nz, half, zn), f32),
        ),
        in_specs=[hbm] * 4,
        out_specs=(hbm,) * 9,
        scratch_shapes=[
            pltpu.VMEM((2, rows, RING * kb), bf16),
            pltpu.VMEM((2, RING * kb, 2 * tn), bf16),
            pltpu.VMEM((2, half, wd_blk.shape[0]), bf16),
            pltpu.VMEM((WD_SLOTS, wd_blk.shape[0], zn), bf16),
            pltpu.VMEM((3, half, zn), f32),
            pltpu.VMEM((Z_SLOTS + 1, half, zn), f32),
            pltpu.VMEM((nz, half, zn), f32),
            pltpu.VMEM((2, half, zn), bf16),
            pltpu.VMEM((H_SLOTS, 2, half, tn), bf16),
            dma((5,)), dma((N_RECV,)), dma((3,)), dma((3,)),
            dma((2,)), dma((2,)), dma((1,)), dma((WD_SLOTS,)), dma((3,)), dma((3,)),
            dma((8,)), dma((2 * RING * nt,)), dma((8,)), dma((2 * RING + 1,)),
            dma((8,)), dma((2 * RING + 1,)), dma((2,)),
            dma((Z_SLOTS,)), dma((2 * (RING - 1),)),
        ],
        compiler_params=pltpu.CompilerParams(collective_id=0, has_side_effects=True, vmem_limit_bytes=67043328),
        cost_estimate=pl.CostEstimate(flops=flops, bytes_accessed=flops // 500, transcendentals=0),
    )(x_blk, wg_blk, wu_blk, wd_blk)
    z_half, z_part, hg, wd, zin = res[0], res[1], res[5], res[7], res[8]
    flops = 2 * half * 2 * RING * tn * 2 * mc
    return pl.pallas_call(
        _finish,
        name="last_part",
        out_shape=jax.ShapeDtypeStruct((rows, 2 * mc), bf16),
        in_specs=[hbm] * 5,
        out_specs=hbm,
        scratch_shapes=[
            pltpu.VMEM((half, 2 * RING * tn), bf16),
            pltpu.VMEM((nz, 2 * RING * tn, zn), bf16),
            pltpu.VMEM((nz, half, zn), f32),
            pltpu.VMEM((nz, half, zn), f32),
            pltpu.VMEM((half, 2 * mc), bf16),
            pltpu.VMEM((nz, half, zn), bf16),
            dma((1,)), dma((nz,)), dma((nz,)), dma((nz,)), dma((2,)), dma((1,)),
        ],
        compiler_params=pltpu.CompilerParams(vmem_limit_bytes=67043328),
        cost_estimate=pl.CostEstimate(flops=flops, bytes_accessed=flops // 500, transcendentals=0),
    )(hg, wd, zin, z_part, z_half)


def solution(mesh):
    assert mesh.shape["dz"] == RING and mesh.shape["dy"] == RING and mesh.shape["dx"] == 2
    x_spec = P(("grp", "dx", "dz"), "dy")
    w_in_spec = P("dy", ("dz", "dx"))
    w_out_spec = P("dz", ("dy", "dx"))
    return jax.shard_map(_local, mesh=mesh, in_specs=(x_spec, w_in_spec, w_in_spec, w_out_spec), out_specs=x_spec, check_vma=False)
```

```python
import jax
import jax.numpy as jnp
from jax import lax
from jax.experimental import pallas as pl
from jax.experimental.pallas import tpu as pltpu
from jax.sharding import PartitionSpec as P

MESH = pl.DeviceIdType.MESH
RING = 4
H_SLOTS = 7
Z_SLOTS = 6
AHEAD, AHEAD_LAST = 4, 2
WD_SLOTS = 3
XL, XS, XF, YL, YS, YF, WN, W2, WF, WL, SW, SD, P1 = 0, 2, 3, 5, 9, 13, 17, 21, 25, 29, 33, 49, 50
JOINT = (
    (XF, XF + 1), tuple(range(YS, YF)), tuple(range(YF, WN)), (WN, WN + 1), (WN + 2, WN + 3), (WF, WF + 1),
    tuple(SW + 4 * j + u for j in range(RING) for u in range(2)), tuple(SW + 4 * j + 2 + u for j in range(RING) for u in range(2)),
)
RECV = {}
for _i in range(P1):
    _group = next((g for g in JOINT if _i in g), (_i,))
    RECV[_i] = RECV[_group[0]] if _i != _group[0] else len(set(RECV.values()))
N_RECV = len(set(RECV.values()))


def _tile(extent, most):
    return next(t for t in range(most, 0, -128) if extent % t == 0)


def _kernel(x_in, wg_in, wu_in, wd_in, z_half, z_part, xg, wgu, ws, hg, wds, wd, zin,
            xbuf, wbuf, hz, wdbuf, zinb, zout, zacc, ofin, hout,
            p1s, p1r, bin_s, bout_s, xsem, wsem, hzsem, wdsem, zinsem, osem,
            ols, olr, oss, osr, fs, fr, hws, zs, zr):
    rows, kb = x_in.shape
    hc = wg_in.shape[1] // RING
    nloc = wg_in.shape[1]
    hq = 2 * hc
    mc = wd_in.shape[1]
    part_rows, tn = hout.shape[2:]
    zn = zout.shape[2]
    nt = hq // tn
    nz = 2 * mc // zn
    ng = RING * nt
    ni = 2 * ng
    zstart = nt + 2
    early = (nt + 1) // 2
    pc = (early * tn // 2, hc - early * tn // 2)
    p_src, p_dst = (0, pc[0]), (0, 2 * pc[0])

    b = lax.axis_index("dz")
    a = lax.axis_index("dy")
    c = lax.axis_index("dx")
    step = 1 - 2 * c
    al = lax.rem(a + step + RING, RING)
    ash = lax.rem(a - step + RING, RING)
    a2 = lax.rem(a + 2, RING)
    bl = lax.rem(b + step + RING, RING)
    bsh = lax.rem(b - step + RING, RING)
    xl, xs_ = {"dy": al}, {"dy": ash}
    yl, ys_ = {"dz": bl}, {"dz": bsh}
    sib = {"dx": 1 - c}
    kbs = (a, ash, al, a2)
    w_in = (wg_in, wu_in)

    def dest(s):
        return lax.rem(b - step * (1 + s) + 2 * RING, RING)

    def rc(src, dst, ss, rs, dev):
        return pltpu.make_async_remote_copy(src_ref=src, dst_ref=dst, send_sem=ss, recv_sem=rs, device_id=dev, device_id_type=MESH)

    def lanes(i, n):
        return pl.ds(pl.multiple_of(i * n, 128), n)

    def krows(k):
        return pl.ds(pl.multiple_of(k * kb, 16), kb)

    half = rows // 2

    def w_piece(u, p, q):
        return w_in[u].at[:, pl.ds(pl.multiple_of(q * hc + p_src[p], 128), pc[p])]

    def w_place(u, p, k):
        return wgu.at[u, krows(k), pl.ds(pl.multiple_of(p_dst[p] + c * pc[p], 128), pc[p])]

    def p1(i):
        kind = 0 if i < YL else 1 if i < WN else 2 if i < SW else 3 if i < SD else 4
        sem = (p1s.at[kind], p1r.at[RECV[i]])
        if i < XS:
            r = pl.ds((i - XL) * half, half)
            return rc(x_in.at[r], xg.at[b, a, r], *sem, xl)
        if i < XF:
            return rc(x_in, xg.at[b, a], *sem, xs_)
        if i < YL:
            r = pl.ds((i - XF) * half, half)
            return rc(xg.at[b, ash, r], xg.at[b, ash, r], *sem, xl)
        if i < YF:
            j = (i - YL) % RING
            src = x_in if j == 0 else xg.at[b, kbs[j]]
            return rc(src, xg.at[b, kbs[j]], *sem, yl if i < YS else ys_)
        if i < WN:
            j = i - YF
            return rc(xg.at[bsh, kbs[j]], xg.at[bsh, kbs[j]], *sem, yl)
        if i < WF:
            u, p = (i - WN) % 2, (i - WN) % 4 // 2
            if i < W2:
                return rc(w_piece(u, p, ash), w_place(u, p, a), *sem, xs_)
            return rc(w_piece(u, p, a2), ws.at[u, :, pl.ds(p_src[p], pc[p])], *sem, xl)
        if i < WL:
            u, p = (i - WF) % 2, (i - WF) // 2
            return rc(ws.at[u, :, pl.ds(p_src[p], pc[p])], w_place(u, p, ash), *sem, xl)
        if i < SW:
            u, p = (i - WL) % 2, (i - WL) // 2
            return rc(w_piece(u, p, al), w_place(u, p, a), *sem, xl)
        if i < SD:
            j, p, u = (i - SW) // 4, (i - SW) % 4 // 2, (i - SW) % 2
            dst = w_place(u, p, kbs[j])
            return rc(w_piece(u, p, a) if j == 0 else dst, dst, *sem, sib)
        return rc(wd_in, wds, *sem, sib)

    def go(*idx):
        for i in idx:
            p1(i).start()

    def got(*idx):
        for i in idx:
            with jax.named_scope(f"got{i}"):
                p1(i).wait_recv()

    def total(ref, sem):
        pltpu.make_async_copy(ref, ref, sem).wait()

    def got_all(first, ref):
        with jax.named_scope(f"got{first}"):
            total(ref, p1r.at[RECV[first]])

    def part_of(u_refs, p):
        return u_refs.at[:, :, pl.ds(p_src[p], pc[p])]

    def all_sent():
        quarter = wgu.at[:, :, pl.ds(0, hc)]
        for kind, ref in enumerate((xg.at[0, pl.ds(0, 3)], xg.at[pl.ds(0, 3)], quarter, quarter, wds)):
            total(ref, p1s.at[kind])

    barrier = pltpu.get_barrier_semaphore()
    for dev in (xl, xs_, yl, ys_, sib):
        pl.semaphore_signal(barrier, inc=1, device_id=dev, device_id_type=MESH)
    with jax.named_scope("barrier"):
        pl.semaphore_wait(barrier, 5)

    go(XL, XL + 1, XS, YL, YS, SD, SW, SW + 1, SW + 2, SW + 3, WN, WN + 1)

    def bounce(*classes):
        for i, (size, moves) in enumerate(classes):
            for src, mid, _ in moves:
                pltpu.make_async_copy(src, mid, bin_s.at[i]).start()
        for i, (size, moves) in enumerate(classes):
            total(size, bin_s.at[i])
            for _, _, parts in moves:
                for piece, dst in parts:
                    pltpu.make_async_copy(piece, dst, bout_s.at[i]).start()
        for i, (size, moves) in enumerate(classes):
            total(size, bout_s.at[i])

    def w_down_moves(src, core):
        moves = []
        for cc in range(2):
            for k in range(RING):
                cols = pl.ds((cc * RING + k) * mc, mc)
                parts = []
                for p in range(2):
                    at, end = p_dst[p] + cc * pc[p], p_dst[p] + (cc + 1) * pc[p]
                    while at < end:
                        n = min(end, (at // tn + 1) * tn) - at
                        row = p_src[p] + at - p_dst[p] - cc * pc[p]
                        dst = wd.at[pl.ds((at // tn * RING + k) * tn + at % tn, n), lanes(core, mc)]
                        parts.append((xbuf.at[1, pl.ds(row, n), cols], dst))
                        at += n
                moves.append((src.at[pl.ds(cc * nloc + k * hc, hc)], xbuf.at[1, pl.ds(0, hc), cols], parts))
        return moves

    x_moves = [(x_in, xbuf.at[0, :, pl.ds(0, kb)], [(xbuf.at[0, :, pl.ds(0, kb)], xg.at[b, a])])]
    w_moves, col = [], kb
    for u in range(2):
        for r0 in range(0, kb, rows):
            n = min(rows, kb - r0)
            parts = []
            for p in range(2):
                dst = wgu.at[u, pl.ds(pl.multiple_of(a * kb + r0, 16), n), pl.ds(pl.multiple_of(p_dst[p] + c * pc[p], 128), pc[p])]
                parts.append((xbuf.at[0, pl.ds(0, n), pl.ds(col + p_src[p], pc[p])], dst))
            w_moves.append((w_in[u].at[pl.ds(r0, n), lanes(a, hc)], xbuf.at[0, pl.ds(0, n), pl.ds(col, hc)], parts))
            col += hc
    with jax.named_scope("bounce"):
        bounce((x_in, x_moves), (ws, w_moves), (wd_in, w_down_moves(wd_in, c)))
        zinb[...] = jnp.zeros_like(zinb)

    got(XL)
    go(XF)
    got(XL + 1)
    go(XF + 1, W2, W2 + 1, YL + 1)
    got(XS)
    go(YL + 2, WN + 2, WN + 3)
    got(YL)
    go(YF)
    got_all(XF, xg.at[0, 0])
    go(YL + 3, WL)
    got(YL + 1)
    go(YF + 1)
    got(SD)
    with jax.named_scope("bounce"):
        bounce((wds, w_down_moves(wds, 1 - c)))
    got(W2)
    go(WF)
    got(W2 + 1)
    go(WF + 1, WL + 1, W2 + 2, W2 + 3)
    got(YL + 2)
    go(YF + 2)
    got_all(WN, part_of(ws, 0))
    go(SW + 8, SW + 9)
    got(YL + 3)
    go(YF + 3)
    got(WL)
    go(SW + 4)
    got_all(WF, part_of(ws, 0))
    go(SW + 12, SW + 13)
    got(WL + 1)
    go(SW + 5, WL + 2, YS + 1)
    got(W2 + 2)
    go(WF + 2)
    got(W2 + 3)
    go(WF + 3, WL + 3)

    def x_load(s, k):
        return pltpu.make_async_copy(xg.at[dest(s), k], xbuf.at[lax.rem(s, 2), :, pl.ds(k * kb, kb)], xsem.at[lax.rem(s, 2)])

    def w_load(g, u):
        slot = lax.rem(g, 2)
        return pltpu.make_async_copy(wgu.at[u, :, lanes(lax.rem(g, nt), tn)], wbuf.at[slot, :, pl.ds(u * tn, tn)], wsem.at[slot])

    ka = RING * tn * (nt - 2)
    whole, nzt = (2 * RING - 1) * nz, 2 * RING * nz
    wd_rows = (pl.ds(0, RING * hq), pl.ds(0, ka))


    def wd_load(w, kind):
        slot = lax.rem(w, WD_SLOTS)
        return pltpu.make_async_copy(wd.at[wd_rows[kind], lanes(lax.rem(w, nz), zn)], wdbuf.at[slot, wd_rows[kind]], wdsem.at[slot])

    def wd_fetch(w):
        for kind, (lo, hi) in enumerate(((0, whole), (whole, nzt))):
            @pl.when((w >= lo) & (w < hi))
            def _():
                wd_load(w, kind).start()

    def zin_load(z, slot, sem):
        return pltpu.make_async_copy(zin.at[z // nz - 2, lax.rem(z, nz)], zinb.at[slot], zinsem.at[sem])

    def pairs(s):
        return jnp.maximum(early - s, 0)

    def item_of(s, h, t):
        m = pairs(s)
        return 2 * nt * s + jnp.where(t < m, 2 * t + h, 2 * m + h * (nt - m) + t - m)

    def place_of(i):
        s, v = i // (2 * nt), lax.rem(i, 2 * nt)
        m = pairs(s)
        w = jnp.maximum(v - 2 * m, 0)
        late = jnp.where(w >= nt - m, 1, 0)
        h = jnp.where(v < 2 * m, lax.rem(v, 2), late)
        t = jnp.where(v < 2 * m, v // 2, m + w - late * (nt - m))
        return s, h, t

    def h_write(g):
        slot = lax.rem(g, H_SLOTS)
        return pltpu.make_async_copy(hout.at[slot], hg.at[dest(g // nt), a, :, lax.rem(g, nt)], hws.at[lax.rem(g, 2)])

    def half_of(s, h, t):
        q = 2 * s + h
        return q + jnp.where((q == 2 * RING - 1) & (t >= nt - 2), 1, 0)

    def h_long(i):
        s, h, t = place_of(i)
        return rc(hout.at[lax.rem(s * nt + t, H_SLOTS), h], hg.at[dest(s), a, h, t], ols.at[lax.rem(i, 8)], olr.at[i], xl)

    def h_short(i):
        s, h, t = place_of(i)
        return rc(hout.at[lax.rem(s * nt + t, H_SLOTS), h], hg.at[dest(s), a, h, t], oss.at[lax.rem(i, 8)], osr.at[half_of(s, h, t)], xs_)

    def h_fwd(i):
        s, h, t = place_of(i)
        blk = hg.at[dest(s), ash, h, t]
        return rc(blk, blk, fs.at[lax.rem(i, 8)], fr.at[half_of(s, h, t)], xl)

    def ready(tiles):
        s, r = tiles // nt, lax.rem(tiles, nt)
        m = pairs(s)
        return 2 * nt * s + jnp.where(r <= m, 2 * r, m + r)

    cut = ni - 12

    def issued(forwards, tiles):
        ahead = jnp.where(forwards < cut, forwards + AHEAD, jnp.maximum(forwards + AHEAD_LAST, cut + AHEAD - 1))
        return jnp.minimum(ahead, ready(tiles))

    def send(lo, hi):
        def one(i, carry):
            h_long(i).start()
            h_short(i).start()
            return carry

        lax.fori_loop(lo, hi, one, 0)

    def forwards(g):
        done = jnp.where(g < ng, jnp.maximum(early, 2 * (g - early) + 2), 2 * (ng - early) + g - ng + 1)
        return jnp.where(g < early, 0, done)

    n_steps = ng + 2 * early

    def serve(j, tiles):
        h_long(j).wait_recv()
        h_fwd(j).start()
        send(issued(j, tiles), issued(j + 1, tiles))

        @pl.when(j >= 2)
        def _():
            h_long(j - 2).wait_send()
            h_short(j - 2).wait_send()

        @pl.when(j >= 4)
        def _():
            h_fwd(j - 4).wait_send()

    def pull(q, sem, lo, hi):
        s, h = q // 2, lax.rem(q, 2)
        arrived = hg.at[0, 0, 0, pl.ds(lo, hi - lo)]
        total(arrived, osr.at[sem])
        total(arrived, fr.at[sem])

        def one(t, carry):
            for k in range(RING):
                pltpu.make_async_copy(hg.at[dest(s), k, h, t], hz.at[lax.rem(q, 2), :, lanes(t * RING + k, tn)], hzsem.at[0]).start()
            return carry

        lax.fori_loop(lo, hi, one, 0)

    def pulled(q, lo, hi):
        total(hz.at[lax.rem(q, 2), :, pl.ds(lo * RING * tn, (hi - lo) * RING * tn)], hzsem.at[0])

    def z_send(z):
        slot = lax.rem(z, Z_SLOTS)
        return rc(zout.at[slot], zin.at[z // nz, lax.rem(z, nz)], zs.at[slot], zr.at[z // nz], yl)

    def o_write(z, slot):
        return pltpu.make_async_copy(ofin.at[slot], z_half.at[:, lanes(lax.rem(z, nz), zn)], osem.at[slot])

    def start_w(g):
        w_load(g, 0).start()
        w_load(g, 1).start()

    for k in range(RING):
        x_load(0, k).start()
    got_all(SW, wgu.at[:, :, pl.ds(p_dst[0], pc[0])])
    start_w(0)

    nsum = 2 * (RING - 1) * nz

    def z_tile(z, carry):
        q, slot, wslot = z // nz, lax.rem(z, 2), lax.rem(z, WD_SLOTS)
        wd_fetch(z + 2)

        @pl.when(lax.rem(z, nz) == 0)
        def _():
            with jax.named_scope("harr"):
                pull(q, q, 0, nt)
            with jax.named_scope("hzload"):
                pulled(q, 0, nt)

        with jax.named_scope("zinrecv"):
            @pl.when((z + 2 >= 2 * nz) & (z + 2 < whole))
            def _():
                @pl.when(lax.rem(z + 2, nz) == 0)
                def _():
                    total(zin.at[0], zr.at[(z + 2) // nz - 2])

                zin_load(z + 2, lax.rem(z + 2, 3), lax.rem(z + 2, 3)).start()

        with jax.named_scope("wdwait"):
            wd_load(z, 0).wait()

        with jax.named_scope("zinwait"):
            @pl.when(z >= 2 * nz)
            def _():
                zin_load(z, lax.rem(z, 3), lax.rem(z, 3)).wait()

        with jax.named_scope("zslot"):
            @pl.when((z >= Z_SLOTS) & (z - Z_SLOTS < nsum))
            def _():
                z_send(z - Z_SLOTS).wait_send()

        @pl.when(z - 2 >= nsum)
        def _():
            o_write(z - 2, slot).wait()

        zslot = jnp.where(z < nsum, lax.rem(z, Z_SLOTS), Z_SLOTS)
        with jax.named_scope("zmm"):
            acc = jnp.dot(hz[lax.rem(q, 2)], wdbuf[wslot], preferred_element_type=jnp.float32) + zinb[lax.rem(z, 3)]
            zout[zslot] = acc
            ofin[slot] = acc.astype(jnp.bfloat16)

        @pl.when(z < nsum)
        def _():
            z_send(z).start()

        @pl.when(z >= nsum)
        def _():
            o_write(z, slot).start()

        return carry

    last_q = 2 * RING - 1

    def tail_first(n, carry):
        w = whole + n
        wd_fetch(w + 2)
        wd_load(w, 1).wait()
        with jax.named_scope("za"):
            zacc[n] = jnp.dot(hz[1, :, wd_rows[1]], wdbuf[lax.rem(w, WD_SLOTS), wd_rows[1]], preferred_element_type=jnp.float32)
        pltpu.make_async_copy(zacc.at[n], z_part.at[n], osem.at[2]).start()
        return carry

    def z_done(g):
        q, k = jnp.maximum(g - zstart, 0), g - zstart - 2 * nt + 1
        steady = 2 * nz * (q // nt) + 2 * nz * (lax.rem(q, nt) + 1) // nt
        ending = 4 * nz + 3 * nz * k // (early + ng - zstart - 2 * nt)
        last = 6 * nz + nz * jnp.maximum(g - n_steps + 4, 0) // 3
        return jnp.where(g < zstart, 0, jnp.where(g >= ng, last, jnp.where(k > 0, ending, steady)))

    def body(g, carry):
        s, t = g // nt, lax.rem(g, nt)

        @pl.when(g == early - 1)
        def _():
            got_all(WN + 2, part_of(ws, 1))
            go(SW + 10, SW + 11)
            got(WL + 2)
            go(SW + 6)
            got(WF + 2)
            go(SW + 14)

        @pl.when(g == early)
        def _():
            got(WF + 3)
            go(SW + 15)
            got(WL + 3)
            go(SW + 7, YS + 2, YS + 3)

            def first(j, carry):
                serve(j, early)
                return carry

            lax.fori_loop(0, early, first, 0)
            got_all(SW + 2, wgu.at[:, :, pl.ds(p_dst[1], pc[1])])
            start_w(g)
            wd_load(0, 0).start()
            wd_load(1, 0).start()

        @pl.when(g < ng)
        def _():
            @pl.when((g + 1 < ng) & (g + 1 != early))
            def _():
                start_w(g + 1)

            @pl.when((t == nt - 1) & (g + 1 < ng))
            def _():
                @pl.when(s + 1 == 1)
                def _():
                    got_all(YF, xg.at[0])

                @pl.when(s + 1 == 2)
                def _():
                    got_all(YS, xg.at[0])

                for k in range(RING):
                    x_load(s + 1, k).start()

            with jax.named_scope("xwait"):
                @pl.when(t == 0)
                def _():
                    total(xbuf.at[lax.rem(s, 2)], xsem.at[lax.rem(s, 2)])

            with jax.named_scope("wwait"):
                total(wbuf.at[lax.rem(g, 2)], wsem.at[lax.rem(g, 2)])

            xslot, wslot, hslot = lax.rem(s, 2), lax.rem(g, 2), lax.rem(g, H_SLOTS)

            def part(h, carry):
                r = pl.ds(pl.multiple_of(h * part_rows, part_rows), part_rows)
                gu = jnp.dot(xbuf[xslot, r, :], wbuf[wslot], preferred_element_type=jnp.float32)
                gate = gu[:, :tn].astype(jnp.bfloat16).astype(jnp.float32)
                up = gu[:, tn:].astype(jnp.bfloat16).astype(jnp.float32)
                hout[hslot, h] = (jax.nn.silu(gate) * up).astype(jnp.bfloat16)
                return carry

            with jax.named_scope("gumm"):
                lax.fori_loop(0, 2, part, 0)
            h_write(g).start()

        @pl.when(g == 2 * nt)
        def _():
            all_sent()

        done, tiles = jnp.where(g == early, early, forwards(g - 1)), jnp.minimum(g + 1, ng)
        send(issued(done, jnp.minimum(g, ng)), issued(done, tiles))

        with jax.named_scope("fwd"):
            @pl.when((g < ng) & (forwards(g) > done))
            def _():
                serve(done, tiles)

        @pl.when((g >= 1) & (g <= ng))
        def _():
            h_write(g - 1).wait()

        lax.fori_loop(z_done(g - 1), z_done(g), z_tile, 0)

        with jax.named_scope("fwd"):
            second = done + jnp.where(g < ng, 1, 0)

            @pl.when(forwards(g) > second)
            def _():
                serve(second, tiles)

        return carry

    lax.fori_loop(0, n_steps, body, 0)

    with jax.named_scope("harr"):
        pull(last_q, last_q, 0, nt - 2)
    with jax.named_scope("hzload"):
        pulled(last_q, 0, nt - 2)
    lax.fori_loop(0, nz, tail_first, 0)
    with jax.named_scope("harr"):
        arrived = hg.at[0, 0, 0, pl.ds(0, 2)]
        total(arrived, osr.at[last_q + 1])
        total(arrived, fr.at[last_q + 1])
        total(zin.at[0], zr.at[2 * RING - 3])

    with jax.named_scope("drain"):
        for i in range(ni - 2, ni):
            h_long(jnp.int32(i)).wait_send()
            h_short(jnp.int32(i)).wait_send()
        for i in range(ni - 4, ni):
            h_fwd(jnp.int32(i)).wait_send()
        for z in range(max(0, whole - Z_SLOTS), nsum):
            z_send(z).wait_send()
        for slot in range(2):
            o_write(jnp.int32(whole - 1), slot).wait()
        total(z_part, osem.at[2])


def _finish(hg, wd, zin, z_part, z_half, out, hz, wdb, zinb, accb, keep, res, hsem, wsem, zsem, asem, ksem, osem):
    rows, tn = hg.shape[4:]
    nz, _, zn = z_part.shape
    nt = hg.shape[3]
    ka = RING * tn * (nt - 2)
    b = lax.axis_index("dz")
    top, low = pl.ds(0, rows), pl.ds(rows, rows)

    for t in range(2):
        for k in range(RING):
            pltpu.make_async_copy(hg.at[b, k, 1, nt - 2 + t], hz.at[:, pl.ds((t * RING + k) * tn, tn)], hsem.at[0]).start()
    def cols(n):
        return pl.ds(pl.multiple_of(n * zn, 128), zn)

    def loads(n):
        return (
            pltpu.make_async_copy(wd.at[pl.ds(ka, 2 * RING * tn), cols(n)], wdb.at[n], wsem.at[n]),
            pltpu.make_async_copy(z_part.at[n], accb.at[n], asem.at[n]),
            pltpu.make_async_copy(zin.at[zin.shape[0] - 1, n], zinb.at[n], zsem.at[n]),
        )

    def fetch(n, carry):
        for copy in loads(n):
            copy.start()
        return carry

    lax.fori_loop(0, nz, fetch, 0)
    first = pltpu.make_async_copy(z_half, keep, ksem.at[0])
    first.start()
    pltpu.make_async_copy(hz, hz, hsem.at[0]).wait()

    def tile(n, carry):
        for copy in loads(n):
            copy.wait()
        acc = jnp.dot(hz[...], wdb[n], preferred_element_type=jnp.float32)
        res[n] = (acc + accb[n] + zinb[n]).astype(jnp.bfloat16)
        pltpu.make_async_copy(res.at[n], out.at[low, cols(n)], osem.at[0]).start()
        return carry

    lax.fori_loop(0, nz - 1, tile, 0)
    first.wait()
    second = pltpu.make_async_copy(keep, out.at[top], ksem.at[1])
    second.start()
    lax.fori_loop(nz - 1, nz, tile, 0)
    pltpu.make_async_copy(out.at[low], out.at[low], osem.at[0]).wait()
    second.wait()


def _local(x_blk, wg_blk, wu_blk, wd_blk):
    rows, kb = x_blk.shape
    hc = wg_blk.shape[1] // RING
    mc = wd_blk.shape[1]
    tn, zn = _tile(2 * hc, 256), _tile(2 * mc, 256)
    nt, nz = 2 * hc // tn, 2 * mc // zn
    bf16, f32 = jnp.bfloat16, jnp.float32
    hbm = pl.BlockSpec(memory_space=pl.ANY)
    half = rows // 2
    dma = pltpu.SemaphoreType.DMA
    flops = 2 * RING * rows * (RING * kb * 4 * hc + wd_blk.shape[0] * 2 * mc)
    res = pl.pallas_call(
        _kernel,
        name="ring_mlp",
        out_shape=(
            jax.ShapeDtypeStruct((half, 2 * mc), bf16),
            jax.ShapeDtypeStruct((nz, half, zn), f32),
            jax.ShapeDtypeStruct((RING, RING, rows, kb), bf16),
            jax.ShapeDtypeStruct((2, RING * kb, 2 * hc), bf16),
            jax.ShapeDtypeStruct((2, kb, hc), bf16),
            jax.ShapeDtypeStruct((RING, RING, 2, nt, half, tn), bf16),
            jax.ShapeDtypeStruct(wd_blk.shape, bf16),
            jax.ShapeDtypeStruct((wd_blk.shape[0], 2 * mc), bf16),
            jax.ShapeDtypeStruct((2 * (RING - 1), nz, half, zn), f32),
        ),
        in_specs=[hbm] * 4,
        out_specs=(hbm,) * 9,
        scratch_shapes=[
            pltpu.VMEM((2, rows, RING * kb), bf16),
            pltpu.VMEM((2, RING * kb, 2 * tn), bf16),
            pltpu.VMEM((2, half, wd_blk.shape[0]), bf16),
            pltpu.VMEM((WD_SLOTS, wd_blk.shape[0], zn), bf16),
            pltpu.VMEM((3, half, zn), f32),
            pltpu.VMEM((Z_SLOTS + 1, half, zn), f32),
            pltpu.VMEM((nz, half, zn), f32),
            pltpu.VMEM((2, half, zn), bf16),
            pltpu.VMEM((H_SLOTS, 2, half, tn), bf16),
            dma((5,)), dma((N_RECV,)), dma((3,)), dma((3,)),
            dma((2,)), dma((2,)), dma((1,)), dma((WD_SLOTS,)), dma((3,)), dma((3,)),
            dma((8,)), dma((2 * RING * nt,)), dma((8,)), dma((2 * RING + 1,)),
            dma((8,)), dma((2 * RING + 1,)), dma((2,)),
            dma((Z_SLOTS,)), dma((2 * (RING - 1),)),
        ],
        compiler_params=pltpu.CompilerParams(collective_id=0, has_side_effects=True, vmem_limit_bytes=67043328),
        cost_estimate=pl.CostEstimate(flops=flops, bytes_accessed=flops // 500, transcendentals=0),
    )(x_blk, wg_blk, wu_blk, wd_blk)
    z_half, z_part, hg, wd, zin = res[0], res[1], res[5], res[7], res[8]
    flops = 2 * half * 2 * RING * tn * 2 * mc
    return pl.pallas_call(
        _finish,
        name="last_part",
        out_shape=jax.ShapeDtypeStruct((rows, 2 * mc), bf16),
        in_specs=[hbm] * 5,
        out_specs=hbm,
        scratch_shapes=[
            pltpu.VMEM((half, 2 * RING * tn), bf16),
            pltpu.VMEM((nz, 2 * RING * tn, zn), bf16),
            pltpu.VMEM((nz, half, zn), f32),
            pltpu.VMEM((nz, half, zn), f32),
            pltpu.VMEM((half, 2 * mc), bf16),
            pltpu.VMEM((nz, half, zn), bf16),
            dma((1,)), dma((nz,)), dma((nz,)), dma((nz,)), dma((2,)), dma((1,)),
        ],
        compiler_params=pltpu.CompilerParams(vmem_limit_bytes=67043328),
        cost_estimate=pl.CostEstimate(flops=flops, bytes_accessed=flops // 500, transcendentals=0),
    )(hg, wd, zin, z_part, z_half)


def solution(mesh):
    assert mesh.shape["dz"] == RING and mesh.shape["dy"] == RING and mesh.shape["dx"] == 2
    x_spec = P(("grp", "dx", "dz"), "dy")
    w_in_spec = P("dy", ("dz", "dx"))
    w_out_spec = P("dz", ("dy", "dx"))
    return jax.shard_map(_local, mesh=mesh, in_specs=(x_spec, w_in_spec, w_in_spec, w_out_spec), out_specs=x_spec, check_vma=False)
```

```python
import jax
import jax.numpy as jnp
from jax import lax
from jax.experimental import pallas as pl
from jax.experimental.pallas import tpu as pltpu
from jax.sharding import PartitionSpec as P

MESH = pl.DeviceIdType.MESH
RING = 4
H_SLOTS = 7
Z_SLOTS = 6
AHEAD = 3
WD_SLOTS = 3
XL, XS, XF, YL, YS, YF, WN, W2, WF, WL, SW, SD, YH, P1 = 0, 2, 3, 5, 9, 13, 17, 21, 25, 29, 33, 49, 50, 52
JOINT = (
    (XF, XF + 1), (YH, YH + 1), tuple(range(YS, YF)), tuple(range(YF, WN)), (WN, WN + 1), (WN + 2, WN + 3), (WF, WF + 1),
    tuple(SW + 4 * j + u for j in range(RING) for u in range(2)), tuple(SW + 4 * j + 2 + u for j in range(RING) for u in range(2)),
)
RECV = {}
for _i in range(P1):
    _group = next((g for g in JOINT if _i in g), (_i,))
    RECV[_i] = RECV[_group[0]] if _i != _group[0] else len(set(RECV.values()))
N_RECV = len(set(RECV.values()))


def _tile(extent, most):
    return next(t for t in range(most, 0, -128) if extent % t == 0)


def _kernel(x_in, wg_in, wu_in, wd_in, z_half, z_part, xg, wgu, ws, hg, wds, wd, zin,
            xbuf, wbuf, hz, wdbuf, zinb, zout, zacc, ofin, hout,
            p1s, p1r, bin_s, bout_s, xsem, wsem, hzsem, wdsem, zinsem, osem,
            ols, olr, oss, osr, fs, fr, hws, zs, zr):
    rows, kb = x_in.shape
    hc = wg_in.shape[1] // RING
    nloc = wg_in.shape[1]
    hq = 2 * hc
    mc = wd_in.shape[1]
    part_rows, tn = hout.shape[2:]
    zn = zout.shape[2]
    nt = hq // tn
    nz = 2 * mc // zn
    ng = RING * nt
    ni = 2 * ng
    zstart = nt + 2
    early = (nt + 1) // 2
    pc = (early * tn // 2, hc - early * tn // 2)
    p_src, p_dst = (0, pc[0]), (0, 2 * pc[0])

    b = lax.axis_index("dz")
    a = lax.axis_index("dy")
    c = lax.axis_index("dx")
    step = 1 - 2 * c
    al = lax.rem(a + step + RING, RING)
    ash = lax.rem(a - step + RING, RING)
    a2 = lax.rem(a + 2, RING)
    bl = lax.rem(b + step + RING, RING)
    bsh = lax.rem(b - step + RING, RING)
    xl, xs_ = {"dy": al}, {"dy": ash}
    yl, ys_ = {"dz": bl}, {"dz": bsh}
    sib = {"dx": 1 - c}
    kbs = (a, ash, al, a2)
    w_in = (wg_in, wu_in)

    def dest(s):
        return lax.rem(b - step * (1 + s) + 2 * RING, RING)

    def rc(src, dst, ss, rs, dev):
        return pltpu.make_async_remote_copy(src_ref=src, dst_ref=dst, send_sem=ss, recv_sem=rs, device_id=dev, device_id_type=MESH)

    def lanes(i, n):
        return pl.ds(pl.multiple_of(i * n, 128), n)

    def krows(k):
        return pl.ds(pl.multiple_of(k * kb, 16), kb)

    half = rows // 2

    def w_piece(u, p, q):
        return w_in[u].at[:, pl.ds(pl.multiple_of(q * hc + p_src[p], 128), pc[p])]

    def w_place(u, p, k):
        return wgu.at[u, krows(k), pl.ds(pl.multiple_of(p_dst[p] + c * pc[p], 128), pc[p])]

    def p1(i):
        kind = 0 if i < YL else 1 if i < WN or i >= YH else 2 if i < SW else 3 if i < SD else 4
        sem = (p1s.at[kind], p1r.at[RECV[i]])
        if i >= YH:
            r = pl.ds((i - YH) * half, half)
            return rc(xg.at[b, ash, r], xg.at[b, ash, r], *sem, yl)
        if i < XS:
            r = pl.ds((i - XL) * half, half)
            return rc(x_in.at[r], xg.at[b, a, r], *sem, xl)
        if i < XF:
            return rc(x_in, xg.at[b, a], *sem, xs_)
        if i < YL:
            r = pl.ds((i - XF) * half, half)
            return rc(xg.at[b, ash, r], xg.at[b, ash, r], *sem, xl)
        if i < YF:
            j = (i - YL) % RING
            src = x_in if j == 0 else xg.at[b, kbs[j]]
            return rc(src, xg.at[b, kbs[j]], *sem, yl if i < YS else ys_)
        if i < WN:
            j = i - YF
            return rc(xg.at[bsh, kbs[j]], xg.at[bsh, kbs[j]], *sem, yl)
        if i < WF:
            u, p = (i - WN) % 2, (i - WN) % 4 // 2
            if i < W2:
                return rc(w_piece(u, p, ash), w_place(u, p, a), *sem, xs_)
            return rc(w_piece(u, p, a2), ws.at[u, :, pl.ds(p_src[p], pc[p])], *sem, xl)
        if i < WL:
            u, p = (i - WF) % 2, (i - WF) // 2
            return rc(ws.at[u, :, pl.ds(p_src[p], pc[p])], w_place(u, p, ash), *sem, xl)
        if i < SW:
            u, p = (i - WL) % 2, (i - WL) // 2
            return rc(w_piece(u, p, al), w_place(u, p, a), *sem, xl)
        if i < SD:
            j, p, u = (i - SW) // 4, (i - SW) % 4 // 2, (i - SW) % 2
            dst = w_place(u, p, kbs[j])
            return rc(w_piece(u, p, a) if j == 0 else dst, dst, *sem, sib)
        return rc(wd_in, wds, *sem, sib)

    def go(*idx):
        for i in idx:
            p1(i).start()

    def got(*idx):
        for i in idx:
            with jax.named_scope(f"got{i}"):
                p1(i).wait_recv()

    def total(ref, sem):
        pltpu.make_async_copy(ref, ref, sem).wait()

    def got_all(first, ref):
        with jax.named_scope(f"got{first}"):
            total(ref, p1r.at[RECV[first]])

    def part_of(u_refs, p):
        return u_refs.at[:, :, pl.ds(p_src[p], pc[p])]

    def all_sent():
        quarter = wgu.at[:, :, pl.ds(0, hc)]
        for kind, ref in enumerate((xg.at[0, pl.ds(0, 3)], xg.at[pl.ds(0, 3)], quarter, quarter, wds)):
            total(ref, p1s.at[kind])

    barrier = pltpu.get_barrier_semaphore()
    for dev in (xl, xs_, yl, ys_, sib):
        pl.semaphore_signal(barrier, inc=1, device_id=dev, device_id_type=MESH)
    with jax.named_scope("barrier"):
        pl.semaphore_wait(barrier, 5)

    go(XL, XL + 1, XS, YL, YS, SD, SW, SW + 1, SW + 2, SW + 3, WN, WN + 1)

    def bounce(*classes):
        for i, (size, moves) in enumerate(classes):
            for src, mid, _ in moves:
                pltpu.make_async_copy(src, mid, bin_s.at[i]).start()
        for i, (size, moves) in enumerate(classes):
            total(size, bin_s.at[i])
            for _, _, parts in moves:
                for piece, dst in parts:
                    pltpu.make_async_copy(piece, dst, bout_s.at[i]).start()
        for i, (size, moves) in enumerate(classes):
            total(size, bout_s.at[i])

    def w_down_moves(src, core):
        moves = []
        for cc in range(2):
            for k in range(RING):
                cols = pl.ds((cc * RING + k) * mc, mc)
                parts = []
                for p in range(2):
                    at, end = p_dst[p] + cc * pc[p], p_dst[p] + (cc + 1) * pc[p]
                    while at < end:
                        n = min(end, (at // tn + 1) * tn) - at
                        row = p_src[p] + at - p_dst[p] - cc * pc[p]
                        dst = wd.at[pl.ds((at // tn * RING + k) * tn + at % tn, n), lanes(core, mc)]
                        parts.append((xbuf.at[1, pl.ds(row, n), cols], dst))
                        at += n
                moves.append((src.at[pl.ds(cc * nloc + k * hc, hc)], xbuf.at[1, pl.ds(0, hc), cols], parts))
        return moves

    x_moves = [(x_in, xbuf.at[0, :, pl.ds(0, kb)], [(xbuf.at[0, :, pl.ds(0, kb)], xg.at[b, a])])]
    w_moves, col = [], kb
    for u in range(2):
        for r0 in range(0, kb, rows):
            n = min(rows, kb - r0)
            parts = []
            for p in range(2):
                dst = wgu.at[u, pl.ds(pl.multiple_of(a * kb + r0, 16), n), pl.ds(pl.multiple_of(p_dst[p] + c * pc[p], 128), pc[p])]
                parts.append((xbuf.at[0, pl.ds(0, n), pl.ds(col + p_src[p], pc[p])], dst))
            w_moves.append((w_in[u].at[pl.ds(r0, n), lanes(a, hc)], xbuf.at[0, pl.ds(0, n), pl.ds(col, hc)], parts))
            col += hc
    with jax.named_scope("bounce"):
        bounce((x_in, x_moves), (ws, w_moves), (wd_in, w_down_moves(wd_in, c)))
        zinb[...] = jnp.zeros_like(zinb)

    got(XL)
    go(XF, YH)
    got(XL + 1)
    go(XF + 1, W2, W2 + 1, YH + 1)
    got(XS)
    go(YL + 2, WN + 2, WN + 3)
    got(YL)
    go(YF)
    got_all(XF, xg.at[0, 0])
    go(YL + 3, WL)
    got_all(YH, xg.at[0, 0])
    go(YF + 1)
    got(SD)
    with jax.named_scope("bounce"):
        bounce((wds, w_down_moves(wds, 1 - c)))
    got(W2)
    go(WF)
    got(W2 + 1)
    go(WF + 1, WL + 1, W2 + 2, W2 + 3)
    got(YL + 2)
    go(YF + 2)
    got_all(WN, part_of(ws, 0))
    go(SW + 8, SW + 9)
    got(YL + 3)
    go(YF + 3)
    got(WL)
    go(SW + 4)
    got_all(WF, part_of(ws, 0))
    go(SW + 12, SW + 13)
    got(WL + 1)
    go(SW + 5, WL + 2, YS + 1)
    got(W2 + 2)
    go(WF + 2)
    got(W2 + 3)
    go(WF + 3, WL + 3)

    def x_load(s, k):
        return pltpu.make_async_copy(xg.at[dest(s), k], xbuf.at[lax.rem(s, 2), :, pl.ds(k * kb, kb)], xsem.at[lax.rem(s, 2)])

    def w_load(g, u):
        slot = lax.rem(g, 2)
        return pltpu.make_async_copy(wgu.at[u, :, lanes(lax.rem(g, nt), tn)], wbuf.at[slot, :, pl.ds(u * tn, tn)], wsem.at[slot])

    assert nt >= 4
    nsum = 2 * (RING - 1) * nz
    ta, first_q, last_q = nt - 2, 2 * RING - 2, 2 * RING - 1
    spans = ((0, nt), (0, ta), (ta, nt), (0, ta - 1), (ta - 1, ta))
    wd_rows = [pl.ds(lo * RING * tn, (hi - lo) * RING * tn) for lo, hi in spans]


    def wd_load(w, kind):
        slot = lax.rem(w, WD_SLOTS)
        return pltpu.make_async_copy(wd.at[wd_rows[kind], lanes(lax.rem(w, nz), zn)], wdbuf.at[slot, wd_rows[kind]], wdsem.at[slot])

    def wd_fetch(w):
        for kind in range(5):
            lo, hi = (nsum + (kind - 1) * nz, nsum + kind * nz) if kind else (0, nsum)

            @pl.when((w >= lo) & (w < hi))
            def _():
                wd_load(w, kind).start()

    def zin_load(z, slot):
        return pltpu.make_async_copy(zin.at[z // nz - 2, lax.rem(z, nz)], zinb.at[slot], zinsem.at[slot])

    def pairs(s):
        return jnp.maximum(early - s, 0)

    def item_of(s, h, t):
        m = pairs(s)
        return 2 * nt * s + jnp.where(t < m, 2 * t + h, 2 * m + h * (nt - m) + t - m)

    def place_of(i):
        s, v = i // (2 * nt), lax.rem(i, 2 * nt)
        m = pairs(s)
        w = jnp.maximum(v - 2 * m, 0)
        late = jnp.where(w >= nt - m, 1, 0)
        h = jnp.where(v < 2 * m, lax.rem(v, 2), late)
        t = jnp.where(v < 2 * m, v // 2, m + w - late * (nt - m))
        return s, h, t

    def h_write(g):
        slot = lax.rem(g, H_SLOTS)
        return pltpu.make_async_copy(hout.at[slot], hg.at[dest(g // nt), a, :, lax.rem(g, nt)], hws.at[lax.rem(g, 2)])

    def half_of(s, h, t):
        q = 2 * s + h
        first = jnp.where((q == first_q) & (t >= ta), 1, 0)
        last = jnp.where(q == last_q, 1 + jnp.where(t >= ta - 1, 1, 0) + jnp.where(t >= ta, 1, 0), 0)
        return q + first + last

    def h_long(i):
        s, h, t = place_of(i)
        return rc(hout.at[lax.rem(s * nt + t, H_SLOTS), h], hg.at[dest(s), a, h, t], ols.at[lax.rem(i, 8)], olr.at[i], xl)

    def h_short(i):
        s, h, t = place_of(i)
        return rc(hout.at[lax.rem(s * nt + t, H_SLOTS), h], hg.at[dest(s), a, h, t], oss.at[lax.rem(i, 8)], osr.at[half_of(s, h, t)], xs_)

    def h_fwd(i):
        s, h, t = place_of(i)
        blk = hg.at[dest(s), ash, h, t]
        return rc(blk, blk, fs.at[lax.rem(i, 8)], fr.at[half_of(s, h, t)], xl)

    def ready(tiles):
        s, r = tiles // nt, lax.rem(tiles, nt)
        m = pairs(s)
        return 2 * nt * s + jnp.where(r <= m, 2 * r, m + r)

    def issued(forwards, tiles):
        return jnp.minimum(forwards + AHEAD, ready(tiles))

    def send(lo, hi):
        def one(i, carry):
            h_long(i).start()
            h_short(i).start()
            return carry

        lax.fori_loop(lo, hi, one, 0)

    def forwards(g):
        return jnp.where(g < early, 0, jnp.minimum(jnp.maximum(early, 2 * (g - early) + 2), ni))

    def serve(j, tiles):
        h_long(j).wait_recv()
        h_fwd(j).start()
        send(issued(j, tiles), issued(j + 1, tiles))

        @pl.when(j >= 2)
        def _():
            h_long(j - 2).wait_send()
            h_short(j - 2).wait_send()

        @pl.when(j >= 4)
        def _():
            h_fwd(j - 4).wait_send()

    def pull(q, sem, lo, hi):
        s, h = q // 2, lax.rem(q, 2)
        arrived = hg.at[0, 0, 0, pl.ds(lo, hi - lo)]
        total(arrived, osr.at[sem])
        total(arrived, fr.at[sem])

        def one(t, carry):
            for k in range(RING):
                pltpu.make_async_copy(hg.at[dest(s), k, h, t], hz.at[lax.rem(q, 2), :, lanes(t * RING + k, tn)], hzsem.at[0]).start()
            return carry

        lax.fori_loop(lo, hi, one, 0)

    def pulled(q, lo, hi):
        total(hz.at[lax.rem(q, 2), :, pl.ds(lo * RING * tn, (hi - lo) * RING * tn)], hzsem.at[0])

    def z_send(z):
        slot = lax.rem(z, Z_SLOTS)
        return rc(zout.at[slot], zin.at[z // nz, lax.rem(z, nz)], zs.at[slot], zr.at[z // nz], yl)

    def o_write(z, slot):
        return pltpu.make_async_copy(ofin.at[slot], z_half.at[:, lanes(lax.rem(z, nz), zn)], osem.at[slot])

    def start_w(g):
        w_load(g, 0).start()
        w_load(g, 1).start()

    for k in range(RING):
        x_load(0, k).start()
    got_all(SW, wgu.at[:, :, pl.ds(p_dst[0], pc[0])])
    start_w(0)

    def z_tile(z, carry):
        q, wslot = z // nz, lax.rem(z, WD_SLOTS)
        wd_fetch(z + 2)

        @pl.when(lax.rem(z, nz) == 0)
        def _():
            with jax.named_scope("zinrecv"):
                @pl.when(q >= 2)
                def _():
                    total(zin.at[0], zr.at[q - 2])
                    for y in range(2):
                        zin_load(z + y, lax.rem(z + y, 3)).start()

            with jax.named_scope("harr"):
                pull(q, q, 0, nt)
            with jax.named_scope("hzload"):
                pulled(q, 0, nt)

        @pl.when((q >= 2) & ((z + 2) // nz == q))
        def _():
            zin_load(z + 2, lax.rem(z + 2, 3)).start()

        with jax.named_scope("wdwait"):
            wd_load(z, 0).wait()

        with jax.named_scope("zinwait"):
            @pl.when(q >= 2)
            def _():
                zin_load(z, lax.rem(z, 3)).wait()

        with jax.named_scope("zslot"):
            @pl.when(z >= Z_SLOTS)
            def _():
                z_send(z - Z_SLOTS).wait_send()

        with jax.named_scope("zmm"):
            acc = jnp.dot(hz[lax.rem(q, 2)], wdbuf[wslot], preferred_element_type=jnp.float32)
            zout[lax.rem(z, Z_SLOTS)] = acc + zinb[lax.rem(z, 3)]

        z_send(z).start()
        return carry

    def late(kind, hook=None):
        base = nsum + (kind - 1) * nz
        h = 0 if kind < 3 else 1

        def tile(n, carry):
            w = base + n
            wd_fetch(w + 2)
            if kind == 2:
                z = nsum + n

                @pl.when(n + 2 < nz)
                def _():
                    zin_load(z + 2, lax.rem(n + 2, 3)).start()

            if hook is not None:
                @pl.when(n == nz // 2)
                def _():
                    hook()

            wd_load(w, kind).wait()
            if kind == 2:
                zin_load(z, lax.rem(n, 3)).wait()

                @pl.when(n >= 2)
                def _():
                    o_write(n - 2, lax.rem(n, 2)).wait()

            with jax.named_scope(f"late{kind}"):
                acc = jnp.dot(hz[h, :, wd_rows[kind]], wdbuf[lax.rem(w, WD_SLOTS), wd_rows[kind]], preferred_element_type=jnp.float32)
                if kind in (1, 3):
                    zacc[n] = acc
                elif kind == 2:
                    ofin[lax.rem(n, 2)] = (acc + zacc[n] + zinb[lax.rem(n, 3)]).astype(jnp.bfloat16)
                else:
                    zacc[n] += acc
            if kind == 2:
                o_write(n, lax.rem(n, 2)).start()
            if kind == 4:
                pltpu.make_async_copy(zacc.at[n], z_part.at[n], osem.at[2]).start()
            return carry

        with jax.named_scope("harr"):
            pull(jnp.int32(first_q + h), first_q + kind - 1, *spans[kind])
            if kind == 2:
                total(zin.at[0], zr.at[2 * RING - 4])
                for y in range(2):
                    zin_load(jnp.int32(nsum + y), y).start()
        with jax.named_scope("hzload"):
            pulled(first_q + h, *spans[kind])
        lax.fori_loop(0, nz, tile, 0)

    def z_done(g):
        q, k = jnp.maximum(g - zstart, 0), g - zstart - 2 * nt + 1
        steady = 2 * nz * (q // nt) + 2 * nz * (lax.rem(q, nt) + 1) // nt
        ending = 4 * nz + jnp.where(g >= ng - 1, 2 * nz, nz * k // 2)
        return jnp.where(g < zstart, 0, jnp.where(k > 0, ending, steady))

    def body(g, carry):
        s, t = g // nt, lax.rem(g, nt)

        @pl.when(g == early - 1)
        def _():
            got_all(WN + 2, part_of(ws, 1))
            go(SW + 10, SW + 11)
            got(WL + 2)
            go(SW + 6)
            got(WF + 2)
            go(SW + 14)

        @pl.when(g == early)
        def _():
            got(WF + 3)
            go(SW + 15)
            got(WL + 3)
            go(SW + 7, YS + 2, YS + 3)

            def first(j, carry):
                serve(j, early)
                return carry

            lax.fori_loop(0, early, first, 0)
            got_all(SW + 2, wgu.at[:, :, pl.ds(p_dst[1], pc[1])])
            start_w(g)
            wd_load(0, 0).start()
            wd_load(1, 0).start()

        @pl.when(g < ng)
        def _():
            @pl.when((g + 1 < ng) & (g + 1 != early))
            def _():
                start_w(g + 1)

            @pl.when((t == nt - 1) & (g + 1 < ng))
            def _():
                @pl.when(s + 1 == 1)
                def _():
                    got_all(YF, xg.at[0])

                @pl.when(s + 1 == 2)
                def _():
                    got_all(YS, xg.at[0])

                for k in range(RING):
                    x_load(s + 1, k).start()

            with jax.named_scope("xwait"):
                @pl.when(t == 0)
                def _():
                    total(xbuf.at[lax.rem(s, 2)], xsem.at[lax.rem(s, 2)])

            with jax.named_scope("wwait"):
                total(wbuf.at[lax.rem(g, 2)], wsem.at[lax.rem(g, 2)])

            xslot, wslot, hslot = lax.rem(s, 2), lax.rem(g, 2), lax.rem(g, H_SLOTS)

            def part(h, carry):
                r = pl.ds(pl.multiple_of(h * part_rows, part_rows), part_rows)
                gu = jnp.dot(xbuf[xslot, r, :], wbuf[wslot], preferred_element_type=jnp.float32)
                gate = gu[:, :tn].astype(jnp.bfloat16).astype(jnp.float32)
                up = gu[:, tn:].astype(jnp.bfloat16).astype(jnp.float32)
                hout[hslot, h] = (jax.nn.silu(gate) * up).astype(jnp.bfloat16)
                return carry

            with jax.named_scope("gumm"):
                lax.fori_loop(0, 2, part, 0)
            h_write(g).start()

        @pl.when(g == 2 * nt)
        def _():
            all_sent()

        done, tiles = jnp.where(g == early, early, forwards(g - 1)), jnp.minimum(g + 1, ng)
        send(issued(done, jnp.minimum(g, ng)), issued(done, tiles))

        with jax.named_scope("fwd"):
            @pl.when(forwards(g) > done)
            def _():
                serve(done, tiles)

        @pl.when(g >= 1)
        def _():
            h_write(g - 1).wait()

        lax.fori_loop(z_done(g - 1), z_done(g), z_tile, 0)

        with jax.named_scope("fwd"):
            @pl.when(forwards(g) > done + 1)
            def _():
                serve(done + 1, tiles)

        return carry

    lax.fori_loop(0, ng, body, 0)

    tiles = jnp.int32(ng)

    def end_serve(j):
        with jax.named_scope("fwd"):
            serve(jnp.int32(j), tiles)

    for j in range(ni - 2 * early, ni - 3):
        end_serve(j)
    h_write(ng - 1).wait()
    late(1)
    end_serve(ni - 3)
    late(2)
    end_serve(ni - 2)
    late(3, lambda: end_serve(ni - 1))
    late(4)
    with jax.named_scope("harr"):
        arrived = hg.at[0, 0, 0, pl.ds(0, nt - ta)]
        total(arrived, osr.at[last_q + 3])
        total(arrived, fr.at[last_q + 3])
        total(zin.at[0], zr.at[2 * RING - 3])

    with jax.named_scope("drain"):
        for i in range(ni - 2, ni):
            h_long(jnp.int32(i)).wait_send()
            h_short(jnp.int32(i)).wait_send()
        for i in range(ni - 4, ni):
            h_fwd(jnp.int32(i)).wait_send()
        for z in range(max(0, nsum - Z_SLOTS), nsum):
            z_send(z).wait_send()
        for n in range(nz - 2, nz):
            o_write(jnp.int32(n), n % 2).wait()
        total(z_part, osem.at[2])


def _finish(hg, wd, zin, z_part, z_half, out, hz, wdb, zinb, accb, keep, res, hsem, wsem, zsem, asem, ksem, osem):
    rows, tn = hg.shape[4:]
    nz, _, zn = z_part.shape
    nt = hg.shape[3]
    ka = RING * tn * (nt - 2)
    b = lax.axis_index("dz")
    top, low = pl.ds(0, rows), pl.ds(rows, rows)

    for t in range(2):
        for k in range(RING):
            pltpu.make_async_copy(hg.at[b, k, 1, nt - 2 + t], hz.at[:, pl.ds((t * RING + k) * tn, tn)], hsem.at[0]).start()
    def cols(n):
        return pl.ds(pl.multiple_of(n * zn, 128), zn)

    def loads(n):
        return (
            pltpu.make_async_copy(wd.at[pl.ds(ka, 2 * RING * tn), cols(n)], wdb.at[n], wsem.at[n]),
            pltpu.make_async_copy(z_part.at[n], accb.at[n], asem.at[n]),
            pltpu.make_async_copy(zin.at[zin.shape[0] - 1, n], zinb.at[n], zsem.at[n]),
        )

    def fetch(n, carry):
        for copy in loads(n):
            copy.start()
        return carry

    lax.fori_loop(0, nz, fetch, 0)
    first = pltpu.make_async_copy(z_half, keep, ksem.at[0])
    first.start()
    pltpu.make_async_copy(hz, hz, hsem.at[0]).wait()

    def tile(n, carry):
        for copy in loads(n):
            copy.wait()
        acc = jnp.dot(hz[...], wdb[n], preferred_element_type=jnp.float32)
        res[n] = (acc + accb[n] + zinb[n]).astype(jnp.bfloat16)
        pltpu.make_async_copy(res.at[n], out.at[low, cols(n)], osem.at[0]).start()
        return carry

    lax.fori_loop(0, nz - 1, tile, 0)
    first.wait()
    second = pltpu.make_async_copy(keep, out.at[top], ksem.at[1])
    second.start()
    lax.fori_loop(nz - 1, nz, tile, 0)
    pltpu.make_async_copy(out.at[low], out.at[low], osem.at[0]).wait()
    second.wait()


def _local(x_blk, wg_blk, wu_blk, wd_blk):
    rows, kb = x_blk.shape
    hc = wg_blk.shape[1] // RING
    mc = wd_blk.shape[1]
    tn, zn = _tile(2 * hc, 256), _tile(2 * mc, 256)
    nt, nz = 2 * hc // tn, 2 * mc // zn
    bf16, f32 = jnp.bfloat16, jnp.float32
    hbm = pl.BlockSpec(memory_space=pl.ANY)
    half = rows // 2
    dma = pltpu.SemaphoreType.DMA
    flops = 2 * RING * rows * (RING * kb * 4 * hc + wd_blk.shape[0] * 2 * mc)
    res = pl.pallas_call(
        _kernel,
        name="ring_mlp",
        out_shape=(
            jax.ShapeDtypeStruct((half, 2 * mc), bf16),
            jax.ShapeDtypeStruct((nz, half, zn), f32),
            jax.ShapeDtypeStruct((RING, RING, rows, kb), bf16),
            jax.ShapeDtypeStruct((2, RING * kb, 2 * hc), bf16),
            jax.ShapeDtypeStruct((2, kb, hc), bf16),
            jax.ShapeDtypeStruct((RING, RING, 2, nt, half, tn), bf16),
            jax.ShapeDtypeStruct(wd_blk.shape, bf16),
            jax.ShapeDtypeStruct((wd_blk.shape[0], 2 * mc), bf16),
            jax.ShapeDtypeStruct((2 * (RING - 1), nz, half, zn), f32),
        ),
        in_specs=[hbm] * 4,
        out_specs=(hbm,) * 9,
        scratch_shapes=[
            pltpu.VMEM((2, rows, RING * kb), bf16),
            pltpu.VMEM((2, RING * kb, 2 * tn), bf16),
            pltpu.VMEM((2, half, wd_blk.shape[0]), bf16),
            pltpu.VMEM((WD_SLOTS, wd_blk.shape[0], zn), bf16),
            pltpu.VMEM((3, half, zn), f32),
            pltpu.VMEM((Z_SLOTS, half, zn), f32),
            pltpu.VMEM((nz, half, zn), f32),
            pltpu.VMEM((2, half, zn), bf16),
            pltpu.VMEM((H_SLOTS, 2, half, tn), bf16),
            dma((5,)), dma((N_RECV,)), dma((3,)), dma((3,)),
            dma((2,)), dma((2,)), dma((1,)), dma((WD_SLOTS,)), dma((3,)), dma((3,)),
            dma((8,)), dma((2 * RING * nt,)), dma((8,)), dma((2 * RING + 3,)),
            dma((8,)), dma((2 * RING + 3,)), dma((2,)),
            dma((Z_SLOTS,)), dma((2 * (RING - 1),)),
        ],
        compiler_params=pltpu.CompilerParams(collective_id=0, has_side_effects=True, vmem_limit_bytes=67043328),
        cost_estimate=pl.CostEstimate(flops=flops, bytes_accessed=flops // 500, transcendentals=0),
    )(x_blk, wg_blk, wu_blk, wd_blk)
    z_half, z_part, hg, wd, zin = res[0], res[1], res[5], res[7], res[8]
    flops = 2 * half * 2 * RING * tn * 2 * mc
    return pl.pallas_call(
        _finish,
        name="last_part",
        out_shape=jax.ShapeDtypeStruct((rows, 2 * mc), bf16),
        in_specs=[hbm] * 5,
        out_specs=hbm,
        scratch_shapes=[
            pltpu.VMEM((half, 2 * RING * tn), bf16),
            pltpu.VMEM((nz, 2 * RING * tn, zn), bf16),
            pltpu.VMEM((nz, half, zn), f32),
            pltpu.VMEM((nz, half, zn), f32),
            pltpu.VMEM((half, 2 * mc), bf16),
            pltpu.VMEM((nz, half, zn), bf16),
            dma((1,)), dma((nz,)), dma((nz,)), dma((nz,)), dma((2,)), dma((1,)),
        ],
        compiler_params=pltpu.CompilerParams(vmem_limit_bytes=67043328),
        cost_estimate=pl.CostEstimate(flops=flops, bytes_accessed=flops // 500, transcendentals=0),
    )(hg, wd, zin, z_part, z_half)


def solution(mesh):
    assert mesh.shape["dz"] == RING and mesh.shape["dy"] == RING and mesh.shape["dx"] == 2
    x_spec = P(("grp", "dx", "dz"), "dy")
    w_in_spec = P("dy", ("dz", "dx"))
    w_out_spec = P("dz", ("dy", "dx"))
    return jax.shard_map(_local, mesh=mesh, in_specs=(x_spec, w_in_spec, w_in_spec, w_out_spec), out_specs=x_spec, check_vma=False)
```

```python
import jax
import jax.numpy as jnp
from jax import lax
from jax.experimental import pallas as pl
from jax.experimental.pallas import tpu as pltpu
from jax.sharding import PartitionSpec as P

MESH = pl.DeviceIdType.MESH
RING = 4
H_SLOTS = 7
Z_SLOTS = 6
AHEAD, AHEAD_LAST = 3, 2
WD_SLOTS = 3
XL, XS, XF, YL, YS, YF, WN, W2, WF, WL, SW, SD, YH, P1 = 0, 2, 3, 5, 9, 13, 17, 21, 25, 29, 33, 49, 50, 52
JOINT = (
    (XF, XF + 1), (YH, YH + 1), tuple(range(YS, YF)), tuple(range(YF, WN)), (WN, WN + 1), (WN + 2, WN + 3), (WF, WF + 1),
    tuple(SW + 4 * j + u for j in range(RING) for u in range(2)), tuple(SW + 4 * j + 2 + u for j in range(RING) for u in range(2)),
)
RECV = {}
for _i in range(P1):
    _group = next((g for g in JOINT if _i in g), (_i,))
    RECV[_i] = RECV[_group[0]] if _i != _group[0] else len(set(RECV.values()))
N_RECV = len(set(RECV.values()))


def _tile(extent, most):
    return next(t for t in range(most, 0, -128) if extent % t == 0)


def _kernel(x_in, wg_in, wu_in, wd_in, z_half, z_part, xg, wgu, ws, hg, wds, wd, zin,
            xbuf, wbuf, hz, wdbuf, zinb, zout, zacc, ofin, hout,
            p1s, p1r, bin_s, bout_s, xsem, wsem, hzsem, wdsem, zinsem, osem,
            ols, olr, oss, osr, fs, fr, hws, zs, zr):
    rows, kb = x_in.shape
    hc = wg_in.shape[1] // RING
    nloc = wg_in.shape[1]
    hq = 2 * hc
    mc = wd_in.shape[1]
    part_rows, tn = hout.shape[2:]
    zn = zout.shape[2]
    nt = hq // tn
    nz = 2 * mc // zn
    ng = RING * nt
    ni = 2 * ng
    zstart = nt + 2
    early = (nt + 1) // 2
    pc = (early * tn // 2, hc - early * tn // 2)
    p_src, p_dst = (0, pc[0]), (0, 2 * pc[0])

    b = lax.axis_index("dz")
    a = lax.axis_index("dy")
    c = lax.axis_index("dx")
    step = 1 - 2 * c
    al = lax.rem(a + step + RING, RING)
    ash = lax.rem(a - step + RING, RING)
    a2 = lax.rem(a + 2, RING)
    bl = lax.rem(b + step + RING, RING)
    bsh = lax.rem(b - step + RING, RING)
    xl, xs_ = {"dy": al}, {"dy": ash}
    yl, ys_ = {"dz": bl}, {"dz": bsh}
    sib = {"dx": 1 - c}
    kbs = (a, ash, al, a2)
    w_in = (wg_in, wu_in)

    def dest(s):
        return lax.rem(b - step * (1 + s) + 2 * RING, RING)

    def rc(src, dst, ss, rs, dev):
        return pltpu.make_async_remote_copy(src_ref=src, dst_ref=dst, send_sem=ss, recv_sem=rs, device_id=dev, device_id_type=MESH)

    def lanes(i, n):
        return pl.ds(pl.multiple_of(i * n, 128), n)

    def krows(k):
        return pl.ds(pl.multiple_of(k * kb, 16), kb)

    half = rows // 2

    def w_piece(u, p, q):
        return w_in[u].at[:, pl.ds(pl.multiple_of(q * hc + p_src[p], 128), pc[p])]

    def w_place(u, p, k):
        return wgu.at[u, krows(k), pl.ds(pl.multiple_of(p_dst[p] + c * pc[p], 128), pc[p])]

    def p1(i):
        kind = 0 if i < YL else 1 if i < WN or i >= YH else 2 if i < SW else 3 if i < SD else 4
        sem = (p1s.at[kind], p1r.at[RECV[i]])
        if i >= YH:
            r = pl.ds((i - YH) * half, half)
            return rc(xg.at[b, ash, r], xg.at[b, ash, r], *sem, yl)
        if i < XS:
            r = pl.ds((i - XL) * half, half)
            return rc(x_in.at[r], xg.at[b, a, r], *sem, xl)
        if i < XF:
            return rc(x_in, xg.at[b, a], *sem, xs_)
        if i < YL:
            r = pl.ds((i - XF) * half, half)
            return rc(xg.at[b, ash, r], xg.at[b, ash, r], *sem, xl)
        if i < YF:
            j = (i - YL) % RING
            src = x_in if j == 0 else xg.at[b, kbs[j]]
            return rc(src, xg.at[b, kbs[j]], *sem, yl if i < YS else ys_)
        if i < WN:
            j = i - YF
            return rc(xg.at[bsh, kbs[j]], xg.at[bsh, kbs[j]], *sem, yl)
        if i < WF:
            u, p = (i - WN) % 2, (i - WN) % 4 // 2
            if i < W2:
                return rc(w_piece(u, p, ash), w_place(u, p, a), *sem, xs_)
            return rc(w_piece(u, p, a2), ws.at[u, :, pl.ds(p_src[p], pc[p])], *sem, xl)
        if i < WL:
            u, p = (i - WF) % 2, (i - WF) // 2
            return rc(ws.at[u, :, pl.ds(p_src[p], pc[p])], w_place(u, p, ash), *sem, xl)
        if i < SW:
            u, p = (i - WL) % 2, (i - WL) // 2
            return rc(w_piece(u, p, al), w_place(u, p, a), *sem, xl)
        if i < SD:
            j, p, u = (i - SW) // 4, (i - SW) % 4 // 2, (i - SW) % 2
            dst = w_place(u, p, kbs[j])
            return rc(w_piece(u, p, a) if j == 0 else dst, dst, *sem, sib)
        return rc(wd_in, wds, *sem, sib)

    def go(*idx):
        for i in idx:
            p1(i).start()

    def got(*idx):
        for i in idx:
            with jax.named_scope(f"got{i}"):
                p1(i).wait_recv()

    def total(ref, sem):
        pltpu.make_async_copy(ref, ref, sem).wait()

    def got_all(first, ref):
        with jax.named_scope(f"got{first}"):
            total(ref, p1r.at[RECV[first]])

    def part_of(u_refs, p):
        return u_refs.at[:, :, pl.ds(p_src[p], pc[p])]

    def all_sent():
        quarter = wgu.at[:, :, pl.ds(0, hc)]
        for kind, ref in enumerate((xg.at[0, pl.ds(0, 3)], xg.at[pl.ds(0, 3)], quarter, quarter, wds)):
            total(ref, p1s.at[kind])

    barrier = pltpu.get_barrier_semaphore()
    for dev in (xl, xs_, yl, ys_, sib):
        pl.semaphore_signal(barrier, inc=1, device_id=dev, device_id_type=MESH)
    with jax.named_scope("barrier"):
        pl.semaphore_wait(barrier, 5)

    go(XL, XL + 1, XS, YL, YS, SD, SW, SW + 1, SW + 2, SW + 3, WN, WN + 1)

    def bounce(*classes):
        for i, (size, moves) in enumerate(classes):
            for src, mid, _ in moves:
                pltpu.make_async_copy(src, mid, bin_s.at[i]).start()
        for i, (size, moves) in enumerate(classes):
            total(size, bin_s.at[i])
            for _, _, parts in moves:
                for piece, dst in parts:
                    pltpu.make_async_copy(piece, dst, bout_s.at[i]).start()
        for i, (size, moves) in enumerate(classes):
            total(size, bout_s.at[i])

    def w_down_moves(src, core):
        moves = []
        for cc in range(2):
            for k in range(RING):
                cols = pl.ds((cc * RING + k) * mc, mc)
                parts = []
                for p in range(2):
                    at, end = p_dst[p] + cc * pc[p], p_dst[p] + (cc + 1) * pc[p]
                    while at < end:
                        n = min(end, (at // tn + 1) * tn) - at
                        row = p_src[p] + at - p_dst[p] - cc * pc[p]
                        dst = wd.at[pl.ds((at // tn * RING + k) * tn + at % tn, n), lanes(core, mc)]
                        parts.append((xbuf.at[1, pl.ds(row, n), cols], dst))
                        at += n
                moves.append((src.at[pl.ds(cc * nloc + k * hc, hc)], xbuf.at[1, pl.ds(0, hc), cols], parts))
        return moves

    x_moves = [(x_in, xbuf.at[0, :, pl.ds(0, kb)], [(xbuf.at[0, :, pl.ds(0, kb)], xg.at[b, a])])]
    w_moves, col = [], kb
    for u in range(2):
        for r0 in range(0, kb, rows):
            n = min(rows, kb - r0)
            parts = []
            for p in range(2):
                dst = wgu.at[u, pl.ds(pl.multiple_of(a * kb + r0, 16), n), pl.ds(pl.multiple_of(p_dst[p] + c * pc[p], 128), pc[p])]
                parts.append((xbuf.at[0, pl.ds(0, n), pl.ds(col + p_src[p], pc[p])], dst))
            w_moves.append((w_in[u].at[pl.ds(r0, n), lanes(a, hc)], xbuf.at[0, pl.ds(0, n), pl.ds(col, hc)], parts))
            col += hc
    with jax.named_scope("bounce"):
        bounce((x_in, x_moves), (ws, w_moves), (wd_in, w_down_moves(wd_in, c)))
        zinb[...] = jnp.zeros_like(zinb)

    got(XL)
    go(XF, YH)
    got(XL + 1)
    go(XF + 1, W2, W2 + 1, YH + 1)
    got(XS)
    go(YL + 2, WN + 2, WN + 3)
    got(YL)
    go(YF)
    got_all(XF, xg.at[0, 0])
    go(YL + 3, WL)
    got_all(YH, xg.at[0, 0])
    go(YF + 1)
    got(SD)
    with jax.named_scope("bounce"):
        bounce((wds, w_down_moves(wds, 1 - c)))
    got(W2)
    go(WF)
    got(W2 + 1)
    go(WF + 1, WL + 1, W2 + 2, W2 + 3)
    got(YL + 2)
    go(YF + 2)
    got_all(WN, part_of(ws, 0))
    go(SW + 8, SW + 9)
    got(YL + 3)
    go(YF + 3)
    got(WL)
    go(SW + 4)
    got_all(WF, part_of(ws, 0))
    go(SW + 12, SW + 13)
    got(WL + 1)
    go(SW + 5, WL + 2, YS + 1)
    got(W2 + 2)
    go(WF + 2)
    got(W2 + 3)
    go(WF + 3, WL + 3)

    def x_load(s, k):
        return pltpu.make_async_copy(xg.at[dest(s), k], xbuf.at[lax.rem(s, 2), :, pl.ds(k * kb, kb)], xsem.at[lax.rem(s, 2)])

    def w_load(g, u):
        slot = lax.rem(g, 2)
        return pltpu.make_async_copy(wgu.at[u, :, lanes(lax.rem(g, nt), tn)], wbuf.at[slot, :, pl.ds(u * tn, tn)], wsem.at[slot])

    assert nt >= 4
    nsum = 2 * (RING - 1) * nz
    ta, first_q, last_q = nt - 2, 2 * RING - 2, 2 * RING - 1
    spans = ((0, nt), (0, ta), (ta, nt), (0, ta - 1), (ta - 1, ta))
    wd_rows = [pl.ds(lo * RING * tn, (hi - lo) * RING * tn) for lo, hi in spans]


    def wd_load(w, kind):
        slot = lax.rem(w, WD_SLOTS)
        return pltpu.make_async_copy(wd.at[wd_rows[kind], lanes(lax.rem(w, nz), zn)], wdbuf.at[slot, wd_rows[kind]], wdsem.at[slot])

    def wd_fetch(w):
        for kind in range(5):
            lo, hi = (nsum + (kind - 1) * nz, nsum + kind * nz) if kind else (0, nsum)

            @pl.when((w >= lo) & (w < hi))
            def _():
                wd_load(w, kind).start()

    def zin_load(z, slot):
        return pltpu.make_async_copy(zin.at[z // nz - 2, lax.rem(z, nz)], zinb.at[slot], zinsem.at[slot])

    def pairs(s):
        return jnp.maximum(early - s, 0)

    def item_of(s, h, t):
        m = pairs(s)
        return 2 * nt * s + jnp.where(t < m, 2 * t + h, 2 * m + h * (nt - m) + t - m)

    def place_of(i):
        s, v = i // (2 * nt), lax.rem(i, 2 * nt)
        m = pairs(s)
        w = jnp.maximum(v - 2 * m, 0)
        late = jnp.where(w >= nt - m, 1, 0)
        h = jnp.where(v < 2 * m, lax.rem(v, 2), late)
        t = jnp.where(v < 2 * m, v // 2, m + w - late * (nt - m))
        return s, h, t

    def h_write(g):
        slot = lax.rem(g, H_SLOTS)
        return pltpu.make_async_copy(hout.at[slot], hg.at[dest(g // nt), a, :, lax.rem(g, nt)], hws.at[lax.rem(g, 2)])

    def half_of(s, h, t):
        q = 2 * s + h
        first = jnp.where((q == first_q) & (t >= ta), 1, 0)
        last = jnp.where(q == last_q, 1 + jnp.where(t >= ta - 1, 1, 0) + jnp.where(t >= ta, 1, 0), 0)
        return q + first + last

    def h_long(i):
        s, h, t = place_of(i)
        return rc(hout.at[lax.rem(s * nt + t, H_SLOTS), h], hg.at[dest(s), a, h, t], ols.at[lax.rem(i, 8)], olr.at[i], xl)

    def h_short(i):
        s, h, t = place_of(i)
        return rc(hout.at[lax.rem(s * nt + t, H_SLOTS), h], hg.at[dest(s), a, h, t], oss.at[lax.rem(i, 8)], osr.at[half_of(s, h, t)], xs_)

    def h_fwd(i):
        s, h, t = place_of(i)
        blk = hg.at[dest(s), ash, h, t]
        return rc(blk, blk, fs.at[lax.rem(i, 8)], fr.at[half_of(s, h, t)], xl)

    def ready(tiles):
        s, r = tiles // nt, lax.rem(tiles, nt)
        m = pairs(s)
        return 2 * nt * s + jnp.where(r <= m, 2 * r, m + r)

    cut = ni - 12

    def issued(forwards, tiles):
        ahead = jnp.where(forwards < cut, forwards + AHEAD, jnp.maximum(forwards + AHEAD_LAST, cut + AHEAD - 1))
        return jnp.minimum(ahead, ready(tiles))

    def send(lo, hi):
        def one(i, carry):
            h_long(i).start()
            h_short(i).start()
            return carry

        lax.fori_loop(lo, hi, one, 0)

    def forwards(g):
        return jnp.where(g < early, 0, jnp.minimum(jnp.maximum(early, 2 * (g - early) + 2), ni))

    def serve(j, tiles):
        h_long(j).wait_recv()
        h_fwd(j).start()
        send(issued(j, tiles), issued(j + 1, tiles))

        @pl.when(j >= 2)
        def _():
            h_long(j - 2).wait_send()
            h_short(j - 2).wait_send()

        @pl.when(j >= 4)
        def _():
            h_fwd(j - 4).wait_send()

    def pull(q, sem, lo, hi):
        s, h = q // 2, lax.rem(q, 2)
        arrived = hg.at[0, 0, 0, pl.ds(lo, hi - lo)]
        total(arrived, osr.at[sem])
        total(arrived, fr.at[sem])

        def one(t, carry):
            for k in range(RING):
                pltpu.make_async_copy(hg.at[dest(s), k, h, t], hz.at[lax.rem(q, 2), :, lanes(t * RING + k, tn)], hzsem.at[0]).start()
            return carry

        lax.fori_loop(lo, hi, one, 0)

    def pulled(q, lo, hi):
        total(hz.at[lax.rem(q, 2), :, pl.ds(lo * RING * tn, (hi - lo) * RING * tn)], hzsem.at[0])

    def z_send(z):
        slot = lax.rem(z, Z_SLOTS)
        return rc(zout.at[slot], zin.at[z // nz, lax.rem(z, nz)], zs.at[slot], zr.at[z // nz], yl)

    def o_write(z, slot):
        return pltpu.make_async_copy(ofin.at[slot], z_half.at[:, lanes(lax.rem(z, nz), zn)], osem.at[slot])

    def start_w(g):
        w_load(g, 0).start()
        w_load(g, 1).start()

    for k in range(RING):
        x_load(0, k).start()
    got_all(SW, wgu.at[:, :, pl.ds(p_dst[0], pc[0])])
    start_w(0)

    def z_tile(z, carry):
        q, wslot = z // nz, lax.rem(z, WD_SLOTS)
        wd_fetch(z + 2)

        @pl.when(lax.rem(z, nz) == 0)
        def _():
            with jax.named_scope("zinrecv"):
                @pl.when(q >= 2)
                def _():
                    total(zin.at[0], zr.at[q - 2])
                    for y in range(2):
                        zin_load(z + y, lax.rem(z + y, 3)).start()

            with jax.named_scope("harr"):
                pull(q, q, 0, nt)
            with jax.named_scope("hzload"):
                pulled(q, 0, nt)

        @pl.when((q >= 2) & ((z + 2) // nz == q))
        def _():
            zin_load(z + 2, lax.rem(z + 2, 3)).start()

        with jax.named_scope("wdwait"):
            wd_load(z, 0).wait()

        with jax.named_scope("zinwait"):
            @pl.when(q >= 2)
            def _():
                zin_load(z, lax.rem(z, 3)).wait()

        with jax.named_scope("zslot"):
            @pl.when(z >= Z_SLOTS)
            def _():
                z_send(z - Z_SLOTS).wait_send()

        with jax.named_scope("zmm"):
            acc = jnp.dot(hz[lax.rem(q, 2)], wdbuf[wslot], preferred_element_type=jnp.float32)
            zout[lax.rem(z, Z_SLOTS)] = acc + zinb[lax.rem(z, 3)]

        z_send(z).start()
        return carry

    def late(kind):
        base = nsum + (kind - 1) * nz
        h = 0 if kind < 3 else 1

        def tile(n, carry):
            w = base + n
            wd_fetch(w + 2)
            if kind == 2:
                z = nsum + n

                @pl.when(n + 2 < nz)
                def _():
                    zin_load(z + 2, lax.rem(n + 2, 3)).start()

            wd_load(w, kind).wait()
            if kind == 2:
                zin_load(z, lax.rem(n, 3)).wait()

                @pl.when(n >= 2)
                def _():
                    o_write(n - 2, lax.rem(n, 2)).wait()

            with jax.named_scope(f"late{kind}"):
                acc = jnp.dot(hz[h, :, wd_rows[kind]], wdbuf[lax.rem(w, WD_SLOTS), wd_rows[kind]], preferred_element_type=jnp.float32)
                if kind in (1, 3):
                    zacc[n] = acc
                elif kind == 2:
                    ofin[lax.rem(n, 2)] = (acc + zacc[n] + zinb[lax.rem(n, 3)]).astype(jnp.bfloat16)
                else:
                    zacc[n] += acc
            if kind == 2:
                o_write(n, lax.rem(n, 2)).start()
            if kind == 4:
                pltpu.make_async_copy(zacc.at[n], z_part.at[n], osem.at[2]).start()
            return carry

        with jax.named_scope("harr"):
            pull(jnp.int32(first_q + h), first_q + kind - 1, *spans[kind])
            if kind == 2:
                total(zin.at[0], zr.at[2 * RING - 4])
                for y in range(2):
                    zin_load(jnp.int32(nsum + y), y).start()
        with jax.named_scope("hzload"):
            pulled(first_q + h, *spans[kind])
        lax.fori_loop(0, nz, tile, 0)

    def z_done(g):
        q, k = jnp.maximum(g - zstart, 0), g - zstart - 2 * nt + 1
        steady = 2 * nz * (q // nt) + 2 * nz * (lax.rem(q, nt) + 1) // nt
        ending = 4 * nz + nz * k // 2
        return jnp.where(g < zstart, 0, jnp.where(k > 0, ending, steady))

    def body(g, carry):
        s, t = g // nt, lax.rem(g, nt)

        @pl.when(g == early - 1)
        def _():
            got_all(WN + 2, part_of(ws, 1))
            go(SW + 10, SW + 11)
            got(WL + 2)
            go(SW + 6)
            got(WF + 2)
            go(SW + 14)

        @pl.when(g == early)
        def _():
            got(WF + 3)
            go(SW + 15)
            got(WL + 3)
            go(SW + 7, YS + 2, YS + 3)

            def first(j, carry):
                serve(j, early)
                return carry

            lax.fori_loop(0, early, first, 0)
            got_all(SW + 2, wgu.at[:, :, pl.ds(p_dst[1], pc[1])])
            start_w(g)
            wd_load(0, 0).start()
            wd_load(1, 0).start()

        @pl.when(g < ng)
        def _():
            @pl.when((g + 1 < ng) & (g + 1 != early))
            def _():
                start_w(g + 1)

            @pl.when((t == nt - 1) & (g + 1 < ng))
            def _():
                @pl.when(s + 1 == 1)
                def _():
                    got_all(YF, xg.at[0])

                @pl.when(s + 1 == 2)
                def _():
                    got_all(YS, xg.at[0])

                for k in range(RING):
                    x_load(s + 1, k).start()

            with jax.named_scope("xwait"):
                @pl.when(t == 0)
                def _():
                    total(xbuf.at[lax.rem(s, 2)], xsem.at[lax.rem(s, 2)])

            with jax.named_scope("wwait"):
                total(wbuf.at[lax.rem(g, 2)], wsem.at[lax.rem(g, 2)])

            xslot, wslot, hslot = lax.rem(s, 2), lax.rem(g, 2), lax.rem(g, H_SLOTS)

            def part(h, carry):
                r = pl.ds(pl.multiple_of(h * part_rows, part_rows), part_rows)
                gu = jnp.dot(xbuf[xslot, r, :], wbuf[wslot], preferred_element_type=jnp.float32)
                gate = gu[:, :tn].astype(jnp.bfloat16).astype(jnp.float32)
                up = gu[:, tn:].astype(jnp.bfloat16).astype(jnp.float32)
                hout[hslot, h] = (jax.nn.silu(gate) * up).astype(jnp.bfloat16)
                return carry

            with jax.named_scope("gumm"):
                lax.fori_loop(0, 2, part, 0)
            h_write(g).start()

        @pl.when(g == 2 * nt)
        def _():
            all_sent()

        done, tiles = jnp.where(g == early, early, forwards(g - 1)), jnp.minimum(g + 1, ng)
        send(issued(done, jnp.minimum(g, ng)), issued(done, tiles))

        with jax.named_scope("fwd"):
            @pl.when(forwards(g) > done)
            def _():
                serve(done, tiles)

        @pl.when(g >= 1)
        def _():
            h_write(g - 1).wait()

        lax.fori_loop(z_done(g - 1), z_done(g), z_tile, 0)

        with jax.named_scope("fwd"):
            @pl.when(forwards(g) > done + 1)
            def _():
                serve(done + 1, tiles)

        return carry

    lax.fori_loop(0, ng, body, 0)

    tiles = jnp.int32(ng)

    def end_serve(j):
        with jax.named_scope("fwd"):
            serve(jnp.int32(j), tiles)

    lax.fori_loop(z_done(jnp.int32(ng - 1)), nsum, z_tile, 0)
    for j in range(ni - 2 * early, ni - 4):
        end_serve(j)
    h_write(ng - 1).wait()
    late(1)
    end_serve(ni - 4)
    late(2)
    end_serve(ni - 3)
    late(3)
    end_serve(ni - 2)
    end_serve(ni - 1)
    late(4)
    with jax.named_scope("harr"):
        arrived = hg.at[0, 0, 0, pl.ds(0, nt - ta)]
        total(arrived, osr.at[last_q + 3])
        total(arrived, fr.at[last_q + 3])
        total(zin.at[0], zr.at[2 * RING - 3])

    with jax.named_scope("drain"):
        for i in range(ni - 2, ni):
            h_long(jnp.int32(i)).wait_send()
            h_short(jnp.int32(i)).wait_send()
        for i in range(ni - 4, ni):
            h_fwd(jnp.int32(i)).wait_send()
        for z in range(max(0, nsum - Z_SLOTS), nsum):
            z_send(z).wait_send()
        for n in range(nz - 2, nz):
            o_write(jnp.int32(n), n % 2).wait()
        total(z_part, osem.at[2])


def _finish(hg, wd, zin, z_part, z_half, out, hz, wdb, zinb, accb, keep, res, hsem, wsem, zsem, asem, ksem, osem):
    rows, tn = hg.shape[4:]
    nz, _, zn = z_part.shape
    nt = hg.shape[3]
    ka = RING * tn * (nt - 2)
    b = lax.axis_index("dz")
    top, low = pl.ds(0, rows), pl.ds(rows, rows)

    for t in range(2):
        for k in range(RING):
            pltpu.make_async_copy(hg.at[b, k, 1, nt - 2 + t], hz.at[:, pl.ds((t * RING + k) * tn, tn)], hsem.at[0]).start()
    def cols(n):
        return pl.ds(pl.multiple_of(n * zn, 128), zn)

    def loads(n):
        return (
            pltpu.make_async_copy(wd.at[pl.ds(ka, 2 * RING * tn), cols(n)], wdb.at[n], wsem.at[n]),
            pltpu.make_async_copy(z_part.at[n], accb.at[n], asem.at[n]),
            pltpu.make_async_copy(zin.at[zin.shape[0] - 1, n], zinb.at[n], zsem.at[n]),
        )

    def fetch(n, carry):
        for copy in loads(n):
            copy.start()
        return carry

    lax.fori_loop(0, nz, fetch, 0)
    first = pltpu.make_async_copy(z_half, keep, ksem.at[0])
    first.start()
    pltpu.make_async_copy(hz, hz, hsem.at[0]).wait()

    def tile(n, carry):
        for copy in loads(n):
            copy.wait()
        acc = jnp.dot(hz[...], wdb[n], preferred_element_type=jnp.float32)
        res[n] = (acc + accb[n] + zinb[n]).astype(jnp.bfloat16)
        pltpu.make_async_copy(res.at[n], out.at[low, cols(n)], osem.at[0]).start()
        return carry

    lax.fori_loop(0, nz - 1, tile, 0)
    first.wait()
    second = pltpu.make_async_copy(keep, out.at[top], ksem.at[1])
    second.start()
    lax.fori_loop(nz - 1, nz, tile, 0)
    pltpu.make_async_copy(out.at[low], out.at[low], osem.at[0]).wait()
    second.wait()


def _local(x_blk, wg_blk, wu_blk, wd_blk):
    rows, kb = x_blk.shape
    hc = wg_blk.shape[1] // RING
    mc = wd_blk.shape[1]
    tn, zn = _tile(2 * hc, 256), _tile(2 * mc, 256)
    nt, nz = 2 * hc // tn, 2 * mc // zn
    bf16, f32 = jnp.bfloat16, jnp.float32
    hbm = pl.BlockSpec(memory_space=pl.ANY)
    half = rows // 2
    dma = pltpu.SemaphoreType.DMA
    flops = 2 * RING * rows * (RING * kb * 4 * hc + wd_blk.shape[0] * 2 * mc)
    res = pl.pallas_call(
        _kernel,
        name="ring_mlp",
        out_shape=(
            jax.ShapeDtypeStruct((half, 2 * mc), bf16),
            jax.ShapeDtypeStruct((nz, half, zn), f32),
            jax.ShapeDtypeStruct((RING, RING, rows, kb), bf16),
            jax.ShapeDtypeStruct((2, RING * kb, 2 * hc), bf16),
            jax.ShapeDtypeStruct((2, kb, hc), bf16),
            jax.ShapeDtypeStruct((RING, RING, 2, nt, half, tn), bf16),
            jax.ShapeDtypeStruct(wd_blk.shape, bf16),
            jax.ShapeDtypeStruct((wd_blk.shape[0], 2 * mc), bf16),
            jax.ShapeDtypeStruct((2 * (RING - 1), nz, half, zn), f32),
        ),
        in_specs=[hbm] * 4,
        out_specs=(hbm,) * 9,
        scratch_shapes=[
            pltpu.VMEM((2, rows, RING * kb), bf16),
            pltpu.VMEM((2, RING * kb, 2 * tn), bf16),
            pltpu.VMEM((2, half, wd_blk.shape[0]), bf16),
            pltpu.VMEM((WD_SLOTS, wd_blk.shape[0], zn), bf16),
            pltpu.VMEM((3, half, zn), f32),
            pltpu.VMEM((Z_SLOTS, half, zn), f32),
            pltpu.VMEM((nz, half, zn), f32),
            pltpu.VMEM((2, half, zn), bf16),
            pltpu.VMEM((H_SLOTS, 2, half, tn), bf16),
            dma((5,)), dma((N_RECV,)), dma((3,)), dma((3,)),
            dma((2,)), dma((2,)), dma((1,)), dma((WD_SLOTS,)), dma((3,)), dma((3,)),
            dma((8,)), dma((2 * RING * nt,)), dma((8,)), dma((2 * RING + 3,)),
            dma((8,)), dma((2 * RING + 3,)), dma((2,)),
            dma((Z_SLOTS,)), dma((2 * (RING - 1),)),
        ],
        compiler_params=pltpu.CompilerParams(collective_id=0, has_side_effects=True, vmem_limit_bytes=67043328),
        cost_estimate=pl.CostEstimate(flops=flops, bytes_accessed=flops // 500, transcendentals=0),
    )(x_blk, wg_blk, wu_blk, wd_blk)
    z_half, z_part, hg, wd, zin = res[0], res[1], res[5], res[7], res[8]
    flops = 2 * half * 2 * RING * tn * 2 * mc
    return pl.pallas_call(
        _finish,
        name="last_part",
        out_shape=jax.ShapeDtypeStruct((rows, 2 * mc), bf16),
        in_specs=[hbm] * 5,
        out_specs=hbm,
        scratch_shapes=[
            pltpu.VMEM((half, 2 * RING * tn), bf16),
            pltpu.VMEM((nz, 2 * RING * tn, zn), bf16),
            pltpu.VMEM((nz, half, zn), f32),
            pltpu.VMEM((nz, half, zn), f32),
            pltpu.VMEM((half, 2 * mc), bf16),
            pltpu.VMEM((nz, half, zn), bf16),
            dma((1,)), dma((nz,)), dma((nz,)), dma((nz,)), dma((2,)), dma((1,)),
        ],
        compiler_params=pltpu.CompilerParams(vmem_limit_bytes=67043328),
        cost_estimate=pl.CostEstimate(flops=flops, bytes_accessed=flops // 500, transcendentals=0),
    )(hg, wd, zin, z_part, z_half)


def solution(mesh):
    assert mesh.shape["dz"] == RING and mesh.shape["dy"] == RING and mesh.shape["dx"] == 2
    x_spec = P(("grp", "dx", "dz"), "dy")
    w_in_spec = P("dy", ("dz", "dx"))
    w_out_spec = P("dz", ("dy", "dx"))
    return jax.shard_map(_local, mesh=mesh, in_specs=(x_spec, w_in_spec, w_in_spec, w_out_spec), out_specs=x_spec, check_vma=False)
```

```python
import jax
import jax.numpy as jnp
from jax import lax
from jax.experimental import pallas as pl
from jax.experimental.pallas import tpu as pltpu
from jax.sharding import PartitionSpec as P

MESH = pl.DeviceIdType.MESH
RING = 4
H_SLOTS = 7
Z_SLOTS = 6
AHEAD, AHEAD_LAST = 3, 2
WD_SLOTS = 3
XL, XS, XF, YL, YS, YF, WN, W2, WF, WL, SW, SD, YH, P1 = 0, 2, 3, 5, 9, 13, 17, 21, 25, 29, 33, 49, 50, 52
JOINT = (
    (XF, XF + 1), (YH, YH + 1), tuple(range(YS, YF)), tuple(range(YF, WN)), (WN, WN + 1), (WN + 2, WN + 3), (WF, WF + 1),
    tuple(SW + 4 * j + u for j in range(RING) for u in range(2)), tuple(SW + 4 * j + 2 + u for j in range(RING) for u in range(2)),
)
RECV = {}
for _i in range(P1):
    _group = next((g for g in JOINT if _i in g), (_i,))
    RECV[_i] = RECV[_group[0]] if _i != _group[0] else len(set(RECV.values()))
N_RECV = len(set(RECV.values()))


def _tile(extent, most):
    return next(t for t in range(most, 0, -128) if extent % t == 0)


def _kernel(x_in, wg_in, wu_in, wd_in, z_half, z_part, xg, wgu, ws, hg, wds, wd, zin,
            xbuf, wbuf, hz, wdbuf, zinb, zout, zacc, ofin, hout,
            p1s, p1r, bin_s, bout_s, xsem, wsem, hzsem, wdsem, zinsem, osem,
            os, olr, fs, hr, hws, zs, zr):
    rows, kb = x_in.shape
    hc = wg_in.shape[1] // RING
    nloc = wg_in.shape[1]
    hq = 2 * hc
    mc = wd_in.shape[1]
    part_rows, tn = hout.shape[2:]
    zn = zout.shape[2]
    nt = hq // tn
    nz = 2 * mc // zn
    ng = RING * nt
    ni = 2 * ng
    zstart = nt + 2
    early = (nt + 1) // 2
    pc = (early * tn // 2, hc - early * tn // 2)
    p_src, p_dst = (0, pc[0]), (0, 2 * pc[0])

    b = lax.axis_index("dz")
    a = lax.axis_index("dy")
    c = lax.axis_index("dx")
    step = 1 - 2 * c
    al = lax.rem(a + step + RING, RING)
    ash = lax.rem(a - step + RING, RING)
    a2 = lax.rem(a + 2, RING)
    bl = lax.rem(b + step + RING, RING)
    bsh = lax.rem(b - step + RING, RING)
    xl, xs_ = {"dy": al}, {"dy": ash}
    yl, ys_ = {"dz": bl}, {"dz": bsh}
    sib = {"dx": 1 - c}
    kbs = (a, ash, al, a2)
    w_in = (wg_in, wu_in)

    def dest(s):
        return lax.rem(b - step * (1 + s) + 2 * RING, RING)

    def rc(src, dst, ss, rs, dev):
        return pltpu.make_async_remote_copy(src_ref=src, dst_ref=dst, send_sem=ss, recv_sem=rs, device_id=dev, device_id_type=MESH)

    def lanes(i, n):
        return pl.ds(pl.multiple_of(i * n, 128), n)

    def krows(k):
        return pl.ds(pl.multiple_of(k * kb, 16), kb)

    half = rows // 2

    def w_piece(u, p, q):
        return w_in[u].at[:, pl.ds(pl.multiple_of(q * hc + p_src[p], 128), pc[p])]

    def w_place(u, p, k):
        return wgu.at[u, krows(k), pl.ds(pl.multiple_of(p_dst[p] + c * pc[p], 128), pc[p])]

    def p1(i):
        kind = 0 if i < YL else 1 if i < WN or i >= YH else 2 if i < SW else 3 if i < SD else 4
        sem = (p1s.at[kind], p1r.at[RECV[i]])
        if i >= YH:
            r = pl.ds((i - YH) * half, half)
            return rc(xg.at[b, ash, r], xg.at[b, ash, r], *sem, yl)
        if i < XS:
            r = pl.ds((i - XL) * half, half)
            return rc(x_in.at[r], xg.at[b, a, r], *sem, xl)
        if i < XF:
            return rc(x_in, xg.at[b, a], *sem, xs_)
        if i < YL:
            r = pl.ds((i - XF) * half, half)
            return rc(xg.at[b, ash, r], xg.at[b, ash, r], *sem, xl)
        if i < YF:
            j = (i - YL) % RING
            src = x_in if j == 0 else xg.at[b, kbs[j]]
            return rc(src, xg.at[b, kbs[j]], *sem, yl if i < YS else ys_)
        if i < WN:
            j = i - YF
            return rc(xg.at[bsh, kbs[j]], xg.at[bsh, kbs[j]], *sem, yl)
        if i < WF:
            u, p = (i - WN) % 2, (i - WN) % 4 // 2
            if i < W2:
                return rc(w_piece(u, p, ash), w_place(u, p, a), *sem, xs_)
            return rc(w_piece(u, p, a2), ws.at[u, :, pl.ds(p_src[p], pc[p])], *sem, xl)
        if i < WL:
            u, p = (i - WF) % 2, (i - WF) // 2
            return rc(ws.at[u, :, pl.ds(p_src[p], pc[p])], w_place(u, p, ash), *sem, xl)
        if i < SW:
            u, p = (i - WL) % 2, (i - WL) // 2
            return rc(w_piece(u, p, al), w_place(u, p, a), *sem, xl)
        if i < SD:
            j, p, u = (i - SW) // 4, (i - SW) % 4 // 2, (i - SW) % 2
            dst = w_place(u, p, kbs[j])
            return rc(w_piece(u, p, a) if j == 0 else dst, dst, *sem, sib)
        return rc(wd_in, wds, *sem, sib)

    def go(*idx):
        for i in idx:
            p1(i).start()

    def got(*idx):
        for i in idx:
            with jax.named_scope(f"got{i}"):
                p1(i).wait_recv()

    def total(ref, sem):
        pltpu.make_async_copy(ref, ref, sem).wait()

    def got_all(first, ref):
        with jax.named_scope(f"got{first}"):
            total(ref, p1r.at[RECV[first]])

    def part_of(u_refs, p):
        return u_refs.at[:, :, pl.ds(p_src[p], pc[p])]

    def all_sent():
        quarter = wgu.at[:, :, pl.ds(0, hc)]
        for kind, ref in enumerate((xg.at[0, pl.ds(0, 3)], xg.at[pl.ds(0, 3)], quarter, quarter, wds)):
            total(ref, p1s.at[kind])

    barrier = pltpu.get_barrier_semaphore()
    for dev in (xl, xs_, yl, ys_, sib):
        pl.semaphore_signal(barrier, inc=1, device_id=dev, device_id_type=MESH)
    with jax.named_scope("barrier"):
        pl.semaphore_wait(barrier, 5)

    go(XL, XL + 1, XS, YL, YS, SD, SW, SW + 1, SW + 2, SW + 3, WN, WN + 1)

    def bounce(*classes):
        for i, (size, moves) in enumerate(classes):
            for src, mid, _ in moves:
                pltpu.make_async_copy(src, mid, bin_s.at[i]).start()
        for i, (size, moves) in enumerate(classes):
            total(size, bin_s.at[i])
            for _, _, parts in moves:
                for piece, dst in parts:
                    pltpu.make_async_copy(piece, dst, bout_s.at[i]).start()
        for i, (size, moves) in enumerate(classes):
            total(size, bout_s.at[i])

    def w_down_moves(src, core):
        moves = []
        for cc in range(2):
            for k in range(RING):
                cols = pl.ds((cc * RING + k) * mc, mc)
                parts = []
                for p in range(2):
                    at, end = p_dst[p] + cc * pc[p], p_dst[p] + (cc + 1) * pc[p]
                    while at < end:
                        n = min(end, (at // tn + 1) * tn) - at
                        row = p_src[p] + at - p_dst[p] - cc * pc[p]
                        dst = wd.at[pl.ds((at // tn * RING + k) * tn + at % tn, n), lanes(core, mc)]
                        parts.append((xbuf.at[1, pl.ds(row, n), cols], dst))
                        at += n
                moves.append((src.at[pl.ds(cc * nloc + k * hc, hc)], xbuf.at[1, pl.ds(0, hc), cols], parts))
        return moves

    x_moves = [(x_in, xbuf.at[0, :, pl.ds(0, kb)], [(xbuf.at[0, :, pl.ds(0, kb)], xg.at[b, a])])]
    w_moves, col = [], kb
    for u in range(2):
        for r0 in range(0, kb, rows):
            n = min(rows, kb - r0)
            parts = []
            for p in range(2):
                dst = wgu.at[u, pl.ds(pl.multiple_of(a * kb + r0, 16), n), pl.ds(pl.multiple_of(p_dst[p] + c * pc[p], 128), pc[p])]
                parts.append((xbuf.at[0, pl.ds(0, n), pl.ds(col + p_src[p], pc[p])], dst))
            w_moves.append((w_in[u].at[pl.ds(r0, n), lanes(a, hc)], xbuf.at[0, pl.ds(0, n), pl.ds(col, hc)], parts))
            col += hc
    with jax.named_scope("bounce"):
        bounce((x_in, x_moves), (ws, w_moves), (wd_in, w_down_moves(wd_in, c)))
        zinb[...] = jnp.zeros_like(zinb)

    got(XL)
    go(XF, YH)
    got(XL + 1)
    go(XF + 1, W2, W2 + 1, YH + 1)
    got(XS)
    go(YL + 2, WN + 2, WN + 3)
    got(YL)
    go(YF)
    got_all(XF, xg.at[0, 0])
    go(YL + 3, WL)
    got_all(YH, xg.at[0, 0])
    go(YF + 1)
    got(SD)
    with jax.named_scope("bounce"):
        bounce((wds, w_down_moves(wds, 1 - c)))
    got(W2)
    go(WF)
    got(W2 + 1)
    go(WF + 1, WL + 1, W2 + 2, W2 + 3)
    got(YL + 2)
    go(YF + 2)
    got_all(WN, part_of(ws, 0))
    go(SW + 8, SW + 9)
    got(YL + 3)
    go(YF + 3)
    got(WL)
    go(SW + 4)
    got_all(WF, part_of(ws, 0))
    go(SW + 12, SW + 13)
    got(WL + 1)
    go(SW + 5, WL + 2, YS + 1)
    got(W2 + 2)
    go(WF + 2)
    got(W2 + 3)
    go(WF + 3, WL + 3)

    def x_load(s, k):
        return pltpu.make_async_copy(xg.at[dest(s), k], xbuf.at[lax.rem(s, 2), :, pl.ds(k * kb, kb)], xsem.at[lax.rem(s, 2)])

    def w_load(g, u):
        slot = lax.rem(g, 2)
        return pltpu.make_async_copy(wgu.at[u, :, lanes(lax.rem(g, nt), tn)], wbuf.at[slot, :, pl.ds(u * tn, tn)], wsem.at[slot])

    assert nt >= 4
    nsum = 2 * (RING - 1) * nz
    ta, first_q, last_q = nt - 2, 2 * RING - 2, 2 * RING - 1
    spans = ((0, nt), (0, ta), (ta, nt), (0, ta - 1), (ta - 1, ta))
    wd_rows = [pl.ds(lo * RING * tn, (hi - lo) * RING * tn) for lo, hi in spans]


    def wd_load(w, kind):
        slot = lax.rem(w, WD_SLOTS)
        return pltpu.make_async_copy(wd.at[wd_rows[kind], lanes(lax.rem(w, nz), zn)], wdbuf.at[slot, wd_rows[kind]], wdsem.at[slot])

    def wd_fetch(w):
        for kind in range(5):
            lo, hi = (nsum + (kind - 1) * nz, nsum + kind * nz) if kind else (0, nsum)

            @pl.when((w >= lo) & (w < hi))
            def _():
                wd_load(w, kind).start()

    def zin_load(z, slot):
        return pltpu.make_async_copy(zin.at[z // nz - 2, lax.rem(z, nz)], zinb.at[slot], zinsem.at[slot])

    def pairs(s):
        return jnp.maximum(early - s, 0)

    def item_of(s, h, t):
        m = pairs(s)
        return 2 * nt * s + jnp.where(t < m, 2 * t + h, 2 * m + h * (nt - m) + t - m)

    def place_of(i):
        s, v = i // (2 * nt), lax.rem(i, 2 * nt)
        m = pairs(s)
        w = jnp.maximum(v - 2 * m, 0)
        late = jnp.where(w >= nt - m, 1, 0)
        h = jnp.where(v < 2 * m, lax.rem(v, 2), late)
        t = jnp.where(v < 2 * m, v // 2, m + w - late * (nt - m))
        return s, h, t

    def h_write(g):
        slot = lax.rem(g, H_SLOTS)
        return pltpu.make_async_copy(hout.at[slot], hg.at[dest(g // nt), a, :, lax.rem(g, nt)], hws.at[lax.rem(g, 2)])

    def half_of(s, h, t):
        q = 2 * s + h
        first = jnp.where((q == first_q) & (t >= ta), 1, 0)
        last = jnp.where(q == last_q, 1 + jnp.where(t >= ta - 1, 1, 0) + jnp.where(t >= ta, 1, 0), 0)
        return q + first + last

    def h_long(i):
        s, h, t = place_of(i)
        return rc(hout.at[lax.rem(s * nt + t, H_SLOTS), h], hg.at[dest(s), a, h, t], os.at[lax.rem(i, 8)], olr.at[i], xl)

    def h_short(i):
        s, h, t = place_of(i)
        return rc(hout.at[lax.rem(s * nt + t, H_SLOTS), h], hg.at[dest(s), a, h, t], os.at[lax.rem(i, 8)], hr.at[half_of(s, h, t)], xs_)

    def h_fwd(i):
        s, h, t = place_of(i)
        blk = hg.at[dest(s), ash, h, t]
        return rc(blk, blk, fs.at[lax.rem(i, 8)], hr.at[half_of(s, h, t)], xl)

    def ready(tiles):
        s, r = tiles // nt, lax.rem(tiles, nt)
        m = pairs(s)
        return 2 * nt * s + jnp.where(r <= m, 2 * r, m + r)

    cut = ni - 12

    def issued(forwards, tiles):
        ahead = jnp.where(forwards < cut, forwards + AHEAD, jnp.maximum(forwards + AHEAD_LAST, cut + AHEAD - 1))
        return jnp.minimum(ahead, ready(tiles))

    def send(lo, hi):
        def one(i, carry):
            h_long(i).start()
            h_short(i).start()
            return carry

        lax.fori_loop(lo, hi, one, 0)

    def forwards(g):
        return jnp.where(g < early, 0, jnp.minimum(jnp.maximum(early, 2 * (g - early) + 2), ni))

    def serve(j, tiles):
        h_long(j).wait_recv()
        h_fwd(j).start()
        send(issued(j, tiles), issued(j + 1, tiles))

        @pl.when(j >= 2)
        def _():
            total(hout.at[0], os.at[lax.rem(j - 2, 8)])

        @pl.when(j >= 4)
        def _():
            h_fwd(j - 4).wait_send()

    def pull(q, sem, lo, hi):
        s, h = q // 2, lax.rem(q, 2)
        total(hg.at[0, 0, :, pl.ds(lo, hi - lo)], hr.at[sem])

        def one(t, carry):
            for k in range(RING):
                pltpu.make_async_copy(hg.at[dest(s), k, h, t], hz.at[lax.rem(q, 2), :, lanes(t * RING + k, tn)], hzsem.at[0]).start()
            return carry

        lax.fori_loop(lo, hi, one, 0)

    def pulled(q, lo, hi):
        total(hz.at[lax.rem(q, 2), :, pl.ds(lo * RING * tn, (hi - lo) * RING * tn)], hzsem.at[0])

    def z_send(z):
        slot = lax.rem(z, Z_SLOTS)
        return rc(zout.at[slot], zin.at[z // nz, lax.rem(z, nz)], zs.at[slot], zr.at[z // nz], yl)

    def o_write(z, slot):
        return pltpu.make_async_copy(ofin.at[slot], z_half.at[:, lanes(lax.rem(z, nz), zn)], osem.at[slot])

    def start_w(g):
        w_load(g, 0).start()
        w_load(g, 1).start()

    for k in range(RING):
        x_load(0, k).start()
    got_all(SW, wgu.at[:, :, pl.ds(p_dst[0], pc[0])])
    start_w(0)

    def z_tile(z, carry):
        q, wslot = z // nz, lax.rem(z, WD_SLOTS)
        wd_fetch(z + 2)

        @pl.when(lax.rem(z, nz) == 0)
        def _():
            with jax.named_scope("zinrecv"):
                @pl.when(q >= 2)
                def _():
                    total(zin.at[0], zr.at[q - 2])
                    for y in range(2):
                        zin_load(z + y, lax.rem(z + y, 3)).start()

            with jax.named_scope("harr"):
                pull(q, q, 0, nt)
            with jax.named_scope("hzload"):
                pulled(q, 0, nt)

        @pl.when((q >= 2) & ((z + 2) // nz == q))
        def _():
            zin_load(z + 2, lax.rem(z + 2, 3)).start()

        with jax.named_scope("wdwait"):
            wd_load(z, 0).wait()

        with jax.named_scope("zinwait"):
            @pl.when(q >= 2)
            def _():
                zin_load(z, lax.rem(z, 3)).wait()

        with jax.named_scope("zslot"):
            @pl.when(z >= Z_SLOTS)
            def _():
                z_send(z - Z_SLOTS).wait_send()

        with jax.named_scope("zmm"):
            acc = jnp.dot(hz[lax.rem(q, 2)], wdbuf[wslot], preferred_element_type=jnp.float32)
            zout[lax.rem(z, Z_SLOTS)] = acc + zinb[lax.rem(z, 3)]

        z_send(z).start()
        return carry

    def late(kind):
        base = nsum + (kind - 1) * nz
        h = 0 if kind < 3 else 1

        def tile(n, carry):
            w = base + n
            wd_fetch(w + 2)
            if kind == 2:
                z = nsum + n

                @pl.when(n + 2 < nz)
                def _():
                    zin_load(z + 2, lax.rem(n + 2, 3)).start()

            wd_load(w, kind).wait()
            if kind == 2:
                zin_load(z, lax.rem(n, 3)).wait()

                @pl.when(n >= 2)
                def _():
                    o_write(n - 2, lax.rem(n, 2)).wait()

            with jax.named_scope(f"late{kind}"):
                acc = jnp.dot(hz[h, :, wd_rows[kind]], wdbuf[lax.rem(w, WD_SLOTS), wd_rows[kind]], preferred_element_type=jnp.float32)
                if kind in (1, 3):
                    zacc[n] = acc
                elif kind == 2:
                    ofin[lax.rem(n, 2)] = (acc + zacc[n] + zinb[lax.rem(n, 3)]).astype(jnp.bfloat16)
                else:
                    zacc[n] += acc
            if kind == 2:
                o_write(n, lax.rem(n, 2)).start()
            if kind == 4:
                pltpu.make_async_copy(zacc.at[n], z_part.at[n], osem.at[2]).start()
            return carry

        with jax.named_scope("harr"):
            pull(jnp.int32(first_q + h), first_q + kind - 1, *spans[kind])
            if kind == 2:
                total(zin.at[0], zr.at[2 * RING - 4])
                for y in range(2):
                    zin_load(jnp.int32(nsum + y), y).start()
        with jax.named_scope("hzload"):
            pulled(first_q + h, *spans[kind])
        lax.fori_loop(0, nz, tile, 0)

    def z_done(g):
        q, k = jnp.maximum(g - zstart, 0), g - zstart - 2 * nt + 1
        steady = 2 * nz * (q // nt) + 2 * nz * (lax.rem(q, nt) + 1) // nt
        ending = 4 * nz + nz * k // 2
        return jnp.where(g < zstart, 0, jnp.where(k > 0, ending, steady))

    def body(g, carry):
        s, t = g // nt, lax.rem(g, nt)

        @pl.when(g == early - 1)
        def _():
            got_all(WN + 2, part_of(ws, 1))
            go(SW + 10, SW + 11)
            got(WL + 2)
            go(SW + 6)
            got(WF + 2)
            go(SW + 14)

        @pl.when(g == early)
        def _():
            got(WF + 3)
            go(SW + 15)
            got(WL + 3)
            go(SW + 7, YS + 2, YS + 3)

            def first(j, carry):
                serve(j, early)
                return carry

            lax.fori_loop(0, early, first, 0)
            got_all(SW + 2, wgu.at[:, :, pl.ds(p_dst[1], pc[1])])
            start_w(g)
            wd_load(0, 0).start()
            wd_load(1, 0).start()

        @pl.when(g < ng)
        def _():
            @pl.when((g + 1 < ng) & (g + 1 != early))
            def _():
                start_w(g + 1)

            @pl.when((t == nt - 1) & (g + 1 < ng))
            def _():
                @pl.when(s + 1 == 1)
                def _():
                    got_all(YF, xg.at[0])

                @pl.when(s + 1 == 2)
                def _():
                    got_all(YS, xg.at[0])

                for k in range(RING):
                    x_load(s + 1, k).start()

            with jax.named_scope("xwait"):
                @pl.when(t == 0)
                def _():
                    total(xbuf.at[lax.rem(s, 2)], xsem.at[lax.rem(s, 2)])

            with jax.named_scope("wwait"):
                total(wbuf.at[lax.rem(g, 2)], wsem.at[lax.rem(g, 2)])

            xslot, wslot, hslot = lax.rem(s, 2), lax.rem(g, 2), lax.rem(g, H_SLOTS)

            def part(h, carry):
                r = pl.ds(pl.multiple_of(h * part_rows, part_rows), part_rows)
                gu = jnp.dot(xbuf[xslot, r, :], wbuf[wslot], preferred_element_type=jnp.float32)
                gate = gu[:, :tn].astype(jnp.bfloat16).astype(jnp.float32)
                up = gu[:, tn:].astype(jnp.bfloat16).astype(jnp.float32)
                hout[hslot, h] = (jax.nn.silu(gate) * up).astype(jnp.bfloat16)
                return carry

            with jax.named_scope("gumm"):
                lax.fori_loop(0, 2, part, 0)
            h_write(g).start()

        @pl.when(g == 2 * nt)
        def _():
            all_sent()

        done, tiles = jnp.where(g == early, early, forwards(g - 1)), jnp.minimum(g + 1, ng)
        send(issued(done, jnp.minimum(g, ng)), issued(done, tiles))

        with jax.named_scope("fwd"):
            @pl.when(forwards(g) > done)
            def _():
                serve(done, tiles)

        @pl.when(g >= 1)
        def _():
            h_write(g - 1).wait()

        lax.fori_loop(z_done(g - 1), z_done(g), z_tile, 0)

        with jax.named_scope("fwd"):
            @pl.when(forwards(g) > done + 1)
            def _():
                serve(done + 1, tiles)

        return carry

    lax.fori_loop(0, ng, body, 0)

    tiles = jnp.int32(ng)

    def end_serve(j):
        with jax.named_scope("fwd"):
            serve(jnp.int32(j), tiles)

    lax.fori_loop(z_done(jnp.int32(ng - 1)), nsum, z_tile, 0)
    for j in range(ni - 2 * early, ni - 4):
        end_serve(j)
    h_write(ng - 1).wait()
    late(1)
    end_serve(ni - 4)
    late(2)
    end_serve(ni - 3)
    late(3)
    end_serve(ni - 2)
    end_serve(ni - 1)
    late(4)
    with jax.named_scope("harr"):
        total(hg.at[0, 0, :, pl.ds(ta, nt - ta)], hr.at[last_q + 3])
        total(zin.at[0], zr.at[2 * RING - 3])

    with jax.named_scope("drain"):
        for i in range(ni - 2, ni):
            total(hout.at[0], os.at[i % 8])
        for i in range(ni - 4, ni):
            h_fwd(jnp.int32(i)).wait_send()
        for z in range(max(0, nsum - Z_SLOTS), nsum):
            z_send(z).wait_send()
        for n in range(nz - 2, nz):
            o_write(jnp.int32(n), n % 2).wait()
        total(z_part, osem.at[2])


def _finish(hg, wd, zin, z_part, z_half, out, hz, wdb, zinb, accb, keep, res, hsem, wsem, zsem, asem, ksem, osem):
    rows, tn = hg.shape[4:]
    nz, _, zn = z_part.shape
    nt = hg.shape[3]
    ka = RING * tn * (nt - 2)
    b = lax.axis_index("dz")
    top, low = pl.ds(0, rows), pl.ds(rows, rows)

    for t in range(2):
        for k in range(RING):
            pltpu.make_async_copy(hg.at[b, k, 1, nt - 2 + t], hz.at[:, pl.ds((t * RING + k) * tn, tn)], hsem.at[0]).start()
    def cols(n):
        return pl.ds(pl.multiple_of(n * zn, 128), zn)

    def loads(n):
        return (
            pltpu.make_async_copy(wd.at[pl.ds(ka, 2 * RING * tn), cols(n)], wdb.at[n], wsem.at[n]),
            pltpu.make_async_copy(z_part.at[n], accb.at[n], asem.at[n]),
            pltpu.make_async_copy(zin.at[zin.shape[0] - 1, n], zinb.at[n], zsem.at[n]),
        )

    def fetch(n, carry):
        for copy in loads(n):
            copy.start()
        return carry

    lax.fori_loop(0, 2, fetch, 0)
    first = pltpu.make_async_copy(z_half, keep, ksem.at[0])
    pltpu.make_async_copy(hz, hz, hsem.at[0]).wait()

    def tile(n, carry):
        @pl.when(n + 2 < nz)
        def _():
            fetch(n + 2, 0)

        @pl.when(n == nz // 2)
        def _():
            first.start()

        for copy in loads(n):
            copy.wait()
        acc = jnp.dot(hz[...], wdb[n], preferred_element_type=jnp.float32)
        res[n] = (acc + accb[n] + zinb[n]).astype(jnp.bfloat16)
        pltpu.make_async_copy(res.at[n], out.at[low, cols(n)], osem.at[0]).start()
        return carry

    lax.fori_loop(0, nz - 1, tile, 0)
    first.wait()
    second = pltpu.make_async_copy(keep, out.at[top], ksem.at[1])
    second.start()
    lax.fori_loop(nz - 1, nz, tile, 0)
    pltpu.make_async_copy(out.at[low], out.at[low], osem.at[0]).wait()
    second.wait()


def _local(x_blk, wg_blk, wu_blk, wd_blk):
    rows, kb = x_blk.shape
    hc = wg_blk.shape[1] // RING
    mc = wd_blk.shape[1]
    tn, zn = _tile(2 * hc, 256), _tile(2 * mc, 256)
    nt, nz = 2 * hc // tn, 2 * mc // zn
    bf16, f32 = jnp.bfloat16, jnp.float32
    hbm = pl.BlockSpec(memory_space=pl.ANY)
    half = rows // 2
    dma = pltpu.SemaphoreType.DMA
    flops = 2 * RING * rows * (RING * kb * 4 * hc + wd_blk.shape[0] * 2 * mc)
    res = pl.pallas_call(
        _kernel,
        name="ring_mlp",
        out_shape=(
            jax.ShapeDtypeStruct((half, 2 * mc), bf16),
            jax.ShapeDtypeStruct((nz, half, zn), f32),
            jax.ShapeDtypeStruct((RING, RING, rows, kb), bf16),
            jax.ShapeDtypeStruct((2, RING * kb, 2 * hc), bf16),
            jax.ShapeDtypeStruct((2, kb, hc), bf16),
            jax.ShapeDtypeStruct((RING, RING, 2, nt, half, tn), bf16),
            jax.ShapeDtypeStruct(wd_blk.shape, bf16),
            jax.ShapeDtypeStruct((wd_blk.shape[0], 2 * mc), bf16),
            jax.ShapeDtypeStruct((2 * (RING - 1), nz, half, zn), f32),
        ),
        in_specs=[hbm] * 4,
        out_specs=(hbm,) * 9,
        scratch_shapes=[
            pltpu.VMEM((2, rows, RING * kb), bf16),
            pltpu.VMEM((2, RING * kb, 2 * tn), bf16),
            pltpu.VMEM((2, half, wd_blk.shape[0]), bf16),
            pltpu.VMEM((WD_SLOTS, wd_blk.shape[0], zn), bf16),
            pltpu.VMEM((3, half, zn), f32),
            pltpu.VMEM((Z_SLOTS, half, zn), f32),
            pltpu.VMEM((nz, half, zn), f32),
            pltpu.VMEM((2, half, zn), bf16),
            pltpu.VMEM((H_SLOTS, 2, half, tn), bf16),
            dma((5,)), dma((N_RECV,)), dma((3,)), dma((3,)),
            dma((2,)), dma((2,)), dma((1,)), dma((WD_SLOTS,)), dma((3,)), dma((3,)),
            dma((8,)), dma((2 * RING * nt,)), dma((8,)), dma((2 * RING + 3,)), dma((2,)),
            dma((Z_SLOTS,)), dma((2 * (RING - 1),)),
        ],
        compiler_params=pltpu.CompilerParams(collective_id=0, has_side_effects=True, vmem_limit_bytes=67043328),
        cost_estimate=pl.CostEstimate(flops=flops, bytes_accessed=flops // 500, transcendentals=0),
    )(x_blk, wg_blk, wu_blk, wd_blk)
    z_half, z_part, hg, wd, zin = res[0], res[1], res[5], res[7], res[8]
    flops = 2 * half * 2 * RING * tn * 2 * mc
    return pl.pallas_call(
        _finish,
        name="last_part",
        out_shape=jax.ShapeDtypeStruct((rows, 2 * mc), bf16),
        in_specs=[hbm] * 5,
        out_specs=hbm,
        scratch_shapes=[
            pltpu.VMEM((half, 2 * RING * tn), bf16),
            pltpu.VMEM((nz, 2 * RING * tn, zn), bf16),
            pltpu.VMEM((nz, half, zn), f32),
            pltpu.VMEM((nz, half, zn), f32),
            pltpu.VMEM((half, 2 * mc), bf16),
            pltpu.VMEM((nz, half, zn), bf16),
            dma((1,)), dma((nz,)), dma((nz,)), dma((nz,)), dma((2,)), dma((1,)),
        ],
        compiler_params=pltpu.CompilerParams(vmem_limit_bytes=67043328),
        cost_estimate=pl.CostEstimate(flops=flops, bytes_accessed=flops // 500, transcendentals=0),
    )(hg, wd, zin, z_part, z_half)


def solution(mesh):
    assert mesh.shape["dz"] == RING and mesh.shape["dy"] == RING and mesh.shape["dx"] == 2
    x_spec = P(("grp", "dx", "dz"), "dy")
    w_in_spec = P("dy", ("dz", "dx"))
    w_out_spec = P("dz", ("dy", "dx"))
    return jax.shard_map(_local, mesh=mesh, in_specs=(x_spec, w_in_spec, w_in_spec, w_out_spec), out_specs=x_spec, check_vma=False)
```

```python
import jax
import jax.numpy as jnp
from jax import lax
from jax.experimental import pallas as pl
from jax.experimental.pallas import tpu as pltpu
from jax.sharding import PartitionSpec as P

MESH = pl.DeviceIdType.MESH
RING = 4
H_SLOTS = 7
Z_SLOTS = 6
AHEAD, AHEAD_LAST = 3, 2
WD_SLOTS = 3
XL, XS, XF, YL, YS, YF, WN, W2, WF, WL, SW, SD, YH, P1 = 0, 2, 3, 5, 9, 13, 17, 21, 25, 29, 33, 49, 50, 52
JOINT = (
    (XF, XF + 1), (YH, YH + 1), tuple(range(YS, YF)), tuple(range(YF, WN)), (WN, WN + 1), (WN + 2, WN + 3), (WF, WF + 1),
    tuple(SW + 4 * j + u for j in range(RING) for u in range(2)), tuple(SW + 4 * j + 2 + u for j in range(RING) for u in range(2)),
)
RECV = {}
for _i in range(P1):
    _group = next((g for g in JOINT if _i in g), (_i,))
    RECV[_i] = RECV[_group[0]] if _i != _group[0] else len(set(RECV.values()))
N_RECV = len(set(RECV.values()))


def _tile(extent, most):
    return next(t for t in range(most, 0, -128) if extent % t == 0)


def _kernel(x_in, wg_in, wu_in, wd_in, z_half, z_part, xg, wgu, ws, hg, wds, wd, zin,
            xbuf, wbuf, hz, wdbuf, zinb, zout, zacc, ofin, hout,
            p1s, p1r, bin_s, bout_s, xsem, wsem, hzsem, wdsem, zinsem, osem,
            os, olr, fs, hr, hws, zs, zr):
    rows, kb = x_in.shape
    hc = wg_in.shape[1] // RING
    nloc = wg_in.shape[1]
    hq = 2 * hc
    mc = wd_in.shape[1]
    part_rows, tn = hout.shape[2:]
    zn = zout.shape[2]
    nt = hq // tn
    nz = 2 * mc // zn
    ng = RING * nt
    ni = 2 * ng
    zstart = nt + 2
    early = (nt + 1) // 2
    pc = (early * tn // 2, hc - early * tn // 2)
    p_src, p_dst = (0, pc[0]), (0, 2 * pc[0])

    b = lax.axis_index("dz")
    a = lax.axis_index("dy")
    c = lax.axis_index("dx")
    step = 1 - 2 * c
    al = lax.rem(a + step + RING, RING)
    ash = lax.rem(a - step + RING, RING)
    a2 = lax.rem(a + 2, RING)
    bl = lax.rem(b + step + RING, RING)
    bsh = lax.rem(b - step + RING, RING)
    xl, xs_ = {"dy": al}, {"dy": ash}
    yl, ys_ = {"dz": bl}, {"dz": bsh}
    sib = {"dx": 1 - c}
    kbs = (a, ash, al, a2)
    w_in = (wg_in, wu_in)

    def dest(s):
        return lax.rem(b - step * (1 + s) + 2 * RING, RING)

    def rc(src, dst, ss, rs, dev):
        return pltpu.make_async_remote_copy(src_ref=src, dst_ref=dst, send_sem=ss, recv_sem=rs, device_id=dev, device_id_type=MESH)

    def lanes(i, n):
        return pl.ds(pl.multiple_of(i * n, 128), n)

    def krows(k):
        return pl.ds(pl.multiple_of(k * kb, 16), kb)

    half = rows // 2

    def w_piece(u, p, q):
        return w_in[u].at[:, pl.ds(pl.multiple_of(q * hc + p_src[p], 128), pc[p])]

    def w_place(u, p, k):
        return wgu.at[u, krows(k), pl.ds(pl.multiple_of(p_dst[p] + c * pc[p], 128), pc[p])]

    def p1(i):
        kind = 0 if i < YL else 1 if i < WN or i >= YH else 2 if i < SW else 3 if i < SD else 4
        sem = (p1s.at[kind], p1r.at[RECV[i]])
        if i >= YH:
            r = pl.ds((i - YH) * half, half)
            return rc(xg.at[b, ash, r], xg.at[b, ash, r], *sem, yl)
        if i < XS:
            r = pl.ds((i - XL) * half, half)
            return rc(x_in.at[r], xg.at[b, a, r], *sem, xl)
        if i < XF:
            return rc(x_in, xg.at[b, a], *sem, xs_)
        if i < YL:
            r = pl.ds((i - XF) * half, half)
            return rc(xg.at[b, ash, r], xg.at[b, ash, r], *sem, xl)
        if i < YF:
            j = (i - YL) % RING
            src = x_in if j == 0 else xg.at[b, kbs[j]]
            return rc(src, xg.at[b, kbs[j]], *sem, yl if i < YS else ys_)
        if i < WN:
            j = i - YF
            return rc(xg.at[bsh, kbs[j]], xg.at[bsh, kbs[j]], *sem, yl)
        if i < WF:
            u, p = (i - WN) % 2, (i - WN) % 4 // 2
            if i < W2:
                return rc(w_piece(u, p, ash), w_place(u, p, a), *sem, xs_)
            return rc(w_piece(u, p, a2), ws.at[u, :, pl.ds(p_src[p], pc[p])], *sem, xl)
        if i < WL:
            u, p = (i - WF) % 2, (i - WF) // 2
            return rc(ws.at[u, :, pl.ds(p_src[p], pc[p])], w_place(u, p, ash), *sem, xl)
        if i < SW:
            u, p = (i - WL) % 2, (i - WL) // 2
            return rc(w_piece(u, p, al), w_place(u, p, a), *sem, xl)
        if i < SD:
            j, p, u = (i - SW) // 4, (i - SW) % 4 // 2, (i - SW) % 2
            dst = w_place(u, p, kbs[j])
            return rc(w_piece(u, p, a) if j == 0 else dst, dst, *sem, sib)
        return rc(wd_in, wds, *sem, sib)

    def go(*idx):
        for i in idx:
            p1(i).start()

    def got(*idx):
        for i in idx:
            with jax.named_scope(f"got{i}"):
                p1(i).wait_recv()

    def total(ref, sem):
        pltpu.make_async_copy(ref, ref, sem).wait()

    def got_all(first, ref):
        with jax.named_scope(f"got{first}"):
            total(ref, p1r.at[RECV[first]])

    def part_of(u_refs, p):
        return u_refs.at[:, :, pl.ds(p_src[p], pc[p])]

    def all_sent():
        quarter = wgu.at[:, :, pl.ds(0, hc)]
        for kind, ref in enumerate((xg.at[0, pl.ds(0, 3)], xg.at[pl.ds(0, 3)], quarter, quarter, wds)):
            total(ref, p1s.at[kind])

    barrier = pltpu.get_barrier_semaphore()
    for dev in (xl, xs_, yl, ys_, sib):
        pl.semaphore_signal(barrier, inc=1, device_id=dev, device_id_type=MESH)
    with jax.named_scope("barrier"):
        pl.semaphore_wait(barrier, 5)

    go(XL, XL + 1, XS, YL, YS, SD, SW, SW + 1, SW + 2, SW + 3, WN, WN + 1)

    def bounce(*classes):
        for i, (size, moves) in enumerate(classes):
            for src, mid, _ in moves:
                pltpu.make_async_copy(src, mid, bin_s.at[i]).start()
        for i, (size, moves) in enumerate(classes):
            total(size, bin_s.at[i])
            for _, _, parts in moves:
                for piece, dst in parts:
                    pltpu.make_async_copy(piece, dst, bout_s.at[i]).start()
        for i, (size, moves) in enumerate(classes):
            total(size, bout_s.at[i])

    def w_down_moves(src, core):
        moves = []
        for cc in range(2):
            for k in range(RING):
                cols = pl.ds((cc * RING + k) * mc, mc)
                parts = []
                for p in range(2):
                    at, end = p_dst[p] + cc * pc[p], p_dst[p] + (cc + 1) * pc[p]
                    while at < end:
                        n = min(end, (at // tn + 1) * tn) - at
                        row = p_src[p] + at - p_dst[p] - cc * pc[p]
                        dst = wd.at[pl.ds((at // tn * RING + k) * tn + at % tn, n), lanes(core, mc)]
                        parts.append((xbuf.at[1, pl.ds(row, n), cols], dst))
                        at += n
                moves.append((src.at[pl.ds(cc * nloc + k * hc, hc)], xbuf.at[1, pl.ds(0, hc), cols], parts))
        return moves

    x_moves = [(x_in, xbuf.at[0, :, pl.ds(0, kb)], [(xbuf.at[0, :, pl.ds(0, kb)], xg.at[b, a])])]
    w_moves, col = [], kb
    for u in range(2):
        for r0 in range(0, kb, rows):
            n = min(rows, kb - r0)
            parts = []
            for p in range(2):
                dst = wgu.at[u, pl.ds(pl.multiple_of(a * kb + r0, 16), n), pl.ds(pl.multiple_of(p_dst[p] + c * pc[p], 128), pc[p])]
                parts.append((xbuf.at[0, pl.ds(0, n), pl.ds(col + p_src[p], pc[p])], dst))
            w_moves.append((w_in[u].at[pl.ds(r0, n), lanes(a, hc)], xbuf.at[0, pl.ds(0, n), pl.ds(col, hc)], parts))
            col += hc
    with jax.named_scope("bounce"):
        bounce((x_in, x_moves), (ws, w_moves), (wd_in, w_down_moves(wd_in, c)))
        zinb[...] = jnp.zeros_like(zinb)

    got(XL)
    go(XF, YH)
    got(XL + 1)
    go(XF + 1, W2, W2 + 1, YH + 1)
    got(XS)
    go(YL + 2, WN + 2, WN + 3)
    got(YL)
    go(YF)
    got_all(XF, xg.at[0, 0])
    go(YL + 3, WL)
    got_all(YH, xg.at[0, 0])
    go(YF + 1)
    got(SD)
    with jax.named_scope("bounce"):
        bounce((wds, w_down_moves(wds, 1 - c)))
    got(W2)
    go(WF)
    got(W2 + 1)
    go(WF + 1, WL + 1, W2 + 2, W2 + 3)
    got(YL + 2)
    go(YF + 2)
    got_all(WN, part_of(ws, 0))
    go(SW + 8, SW + 9)
    got(YL + 3)
    go(YF + 3)
    got(WL)
    go(SW + 4)
    got_all(WF, part_of(ws, 0))
    go(SW + 12, SW + 13)
    got(WL + 1)
    go(SW + 5, WL + 2, YS + 1)
    got(W2 + 2)
    go(WF + 2)
    got(W2 + 3)
    go(WF + 3, WL + 3)

    def x_load(s, k):
        return pltpu.make_async_copy(xg.at[dest(s), k], xbuf.at[lax.rem(s, 2), :, pl.ds(k * kb, kb)], xsem.at[lax.rem(s, 2)])

    def w_load(g, u):
        slot = lax.rem(g, 2)
        return pltpu.make_async_copy(wgu.at[u, :, lanes(lax.rem(g, nt), tn)], wbuf.at[slot, :, pl.ds(u * tn, tn)], wsem.at[slot])

    assert nt >= 4
    nsum = 2 * (RING - 1) * nz
    ta, first_q, last_q = nt - 2, 2 * RING - 2, 2 * RING - 1
    spans = ((0, nt), (0, ta), (ta, nt), (0, ta - 1), (ta - 1, ta))
    wd_rows = [pl.ds(lo * RING * tn, (hi - lo) * RING * tn) for lo, hi in spans]


    def wd_load(w, kind):
        slot = lax.rem(w, WD_SLOTS)
        return pltpu.make_async_copy(wd.at[wd_rows[kind], lanes(lax.rem(w, nz), zn)], wdbuf.at[slot, wd_rows[kind]], wdsem.at[slot])

    def wd_fetch(w):
        for kind in range(5):
            lo, hi = (nsum + (kind - 1) * nz, nsum + kind * nz) if kind else (0, nsum)

            @pl.when((w >= lo) & (w < hi))
            def _():
                wd_load(w, kind).start()

    def zin_load(z, slot):
        return pltpu.make_async_copy(zin.at[z // nz - 2, lax.rem(z, nz)], zinb.at[slot], zinsem.at[slot])

    def pairs(s):
        return jnp.maximum(early - s, 0)

    def item_of(s, h, t):
        m = pairs(s)
        return 2 * nt * s + jnp.where(t < m, 2 * t + h, 2 * m + h * (nt - m) + t - m)

    def place_of(i):
        s, v = i // (2 * nt), lax.rem(i, 2 * nt)
        m = pairs(s)
        w = jnp.maximum(v - 2 * m, 0)
        late = jnp.where(w >= nt - m, 1, 0)
        h = jnp.where(v < 2 * m, lax.rem(v, 2), late)
        t = jnp.where(v < 2 * m, v // 2, m + w - late * (nt - m))
        return s, h, t

    def h_write(g):
        slot = lax.rem(g, H_SLOTS)
        return pltpu.make_async_copy(hout.at[slot], hg.at[dest(g // nt), a, :, lax.rem(g, nt)], hws.at[lax.rem(g, 2)])

    def half_of(s, h, t):
        q = 2 * s + h
        first = jnp.where((q == first_q) & (t >= ta), 1, 0)
        last = jnp.where(q == last_q, 1 + jnp.where(t >= ta - 1, 1, 0) + jnp.where(t >= ta, 1, 0), 0)
        return q + first + last

    def h_long(i):
        s, h, t = place_of(i)
        return rc(hout.at[lax.rem(s * nt + t, H_SLOTS), h], hg.at[dest(s), a, h, t], os.at[lax.rem(i, 8)], olr.at[i], xl)

    def h_short(i):
        s, h, t = place_of(i)
        return rc(hout.at[lax.rem(s * nt + t, H_SLOTS), h], hg.at[dest(s), a, h, t], os.at[lax.rem(i, 8)], hr.at[half_of(s, h, t)], xs_)

    def h_fwd(i):
        s, h, t = place_of(i)
        blk = hg.at[dest(s), ash, h, t]
        return rc(blk, blk, fs.at[lax.rem(i, 8)], hr.at[half_of(s, h, t)], xl)

    def ready(tiles):
        s, r = tiles // nt, lax.rem(tiles, nt)
        m = pairs(s)
        return 2 * nt * s + jnp.where(r <= m, 2 * r, m + r)

    cut = ni - 12

    def issued(forwards, tiles):
        ahead = jnp.where(forwards < cut, forwards + AHEAD, jnp.maximum(forwards + AHEAD_LAST, cut + AHEAD - 1))
        return jnp.minimum(ahead, ready(tiles))

    def send(lo, hi):
        def one(i, carry):
            h_long(i).start()
            h_short(i).start()
            return carry

        lax.fori_loop(lo, hi, one, 0)

    def forwards(g):
        return jnp.where(g < early, 0, jnp.minimum(jnp.maximum(early, 2 * (g - early) + 2), ni))

    def serve(j, tiles):
        h_long(j).wait_recv()
        h_fwd(j).start()
        send(issued(j, tiles), issued(j + 1, tiles))

        @pl.when(j >= 2)
        def _():
            total(hout.at[0], os.at[lax.rem(j - 2, 8)])

        @pl.when(j >= 4)
        def _():
            h_fwd(j - 4).wait_send()

    def pull(q, sem, lo, hi):
        s, h = q // 2, lax.rem(q, 2)
        total(hg.at[0, 0, :, pl.ds(lo, hi - lo)], hr.at[sem])

        def one(t, carry):
            for k in range(RING):
                pltpu.make_async_copy(hg.at[dest(s), k, h, t], hz.at[lax.rem(q, 2), :, lanes(t * RING + k, tn)], hzsem.at[0]).start()
            return carry

        lax.fori_loop(lo, hi, one, 0)

    def pulled(q, lo, hi):
        total(hz.at[lax.rem(q, 2), :, pl.ds(lo * RING * tn, (hi - lo) * RING * tn)], hzsem.at[0])

    def z_send(z):
        slot = lax.rem(z, Z_SLOTS)
        return rc(zout.at[slot], zin.at[z // nz, lax.rem(z, nz)], zs.at[slot], zr.at[z // nz], yl)

    def o_write(z, slot):
        return pltpu.make_async_copy(ofin.at[slot], z_half.at[:, lanes(lax.rem(z, nz), zn)], osem.at[slot])

    def start_w(g):
        w_load(g, 0).start()
        w_load(g, 1).start()

    for k in range(RING):
        x_load(0, k).start()
    got_all(SW, wgu.at[:, :, pl.ds(p_dst[0], pc[0])])
    start_w(0)

    def z_tile(z, carry):
        q, wslot = z // nz, lax.rem(z, WD_SLOTS)
        wd_fetch(z + 2)

        @pl.when(lax.rem(z, nz) == 0)
        def _():
            with jax.named_scope("zinrecv"):
                @pl.when(q >= 2)
                def _():
                    total(zin.at[0], zr.at[q - 2])
                    for y in range(2):
                        zin_load(z + y, lax.rem(z + y, 3)).start()

            with jax.named_scope("harr"):
                pull(q, q, 0, nt)
            with jax.named_scope("hzload"):
                pulled(q, 0, nt)

        @pl.when((q >= 2) & ((z + 2) // nz == q))
        def _():
            zin_load(z + 2, lax.rem(z + 2, 3)).start()

        with jax.named_scope("wdwait"):
            wd_load(z, 0).wait()

        with jax.named_scope("zinwait"):
            @pl.when(q >= 2)
            def _():
                zin_load(z, lax.rem(z, 3)).wait()

        with jax.named_scope("zslot"):
            @pl.when(z >= Z_SLOTS)
            def _():
                z_send(z - Z_SLOTS).wait_send()

        with jax.named_scope("zmm"):
            acc = jnp.dot(hz[lax.rem(q, 2)], wdbuf[wslot], preferred_element_type=jnp.float32)
            zout[lax.rem(z, Z_SLOTS)] = acc + zinb[lax.rem(z, 3)]

        z_send(z).start()
        return carry

    def late(kind):
        base = nsum + (kind - 1) * nz
        h = 0 if kind < 3 else 1

        def tile(n, carry):
            w = base + n
            wd_fetch(w + 2)
            if kind == 2:
                z = nsum + n

                @pl.when(n + 2 < nz)
                def _():
                    zin_load(z + 2, lax.rem(n + 2, 3)).start()

            wd_load(w, kind).wait()
            if kind == 2:
                zin_load(z, lax.rem(n, 3)).wait()

                @pl.when(n >= 2)
                def _():
                    o_write(n - 2, lax.rem(n, 2)).wait()

            with jax.named_scope(f"late{kind}"):
                acc = jnp.dot(hz[h, :, wd_rows[kind]], wdbuf[lax.rem(w, WD_SLOTS), wd_rows[kind]], preferred_element_type=jnp.float32)
                if kind in (1, 3):
                    zacc[n] = acc
                elif kind == 2:
                    ofin[lax.rem(n, 2)] = (acc + zacc[n] + zinb[lax.rem(n, 3)]).astype(jnp.bfloat16)
                else:
                    zacc[n] += acc
            if kind == 2:
                o_write(n, lax.rem(n, 2)).start()
            if kind == 4:
                pltpu.make_async_copy(zacc.at[n], z_part.at[n], osem.at[2]).start()
            return carry

        with jax.named_scope("harr"):
            pull(jnp.int32(first_q + h), first_q + kind - 1, *spans[kind])
            if kind == 2:
                total(zin.at[0], zr.at[2 * RING - 4])
                for y in range(2):
                    zin_load(jnp.int32(nsum + y), y).start()
        with jax.named_scope("hzload"):
            pulled(first_q + h, *spans[kind])
        lax.fori_loop(0, nz, tile, 0)

    def z_done(g):
        q, k = jnp.maximum(g - zstart, 0), g - zstart - 2 * nt + 1
        steady = 2 * nz * (q // nt) + 2 * nz * (lax.rem(q, nt) + 1) // nt
        ending = 4 * nz + nz * k // 2
        return jnp.where(g < zstart, 0, jnp.where(k > 0, ending, steady))

    def body(g, carry):
        s, t = g // nt, lax.rem(g, nt)

        @pl.when(g == early - 1)
        def _():
            got_all(WN + 2, part_of(ws, 1))
            go(SW + 10, SW + 11)
            got(WL + 2)
            go(SW + 6)
            got(WF + 2)
            go(SW + 14)

        @pl.when(g == early)
        def _():
            got(WF + 3)
            go(SW + 15)
            got(WL + 3)
            go(SW + 7, YS + 2, YS + 3)

            def first(j, carry):
                serve(j, early)
                return carry

            lax.fori_loop(0, early, first, 0)
            got_all(SW + 2, wgu.at[:, :, pl.ds(p_dst[1], pc[1])])
            start_w(g)
            wd_load(0, 0).start()
            wd_load(1, 0).start()

        @pl.when(g < ng)
        def _():
            @pl.when((g + 1 < ng) & (g + 1 != early))
            def _():
                start_w(g + 1)

            @pl.when((t == nt - 1) & (g + 1 < ng))
            def _():
                @pl.when(s + 1 == 1)
                def _():
                    got_all(YF, xg.at[0])

                @pl.when(s + 1 == 2)
                def _():
                    got_all(YS, xg.at[0])

                for k in range(RING):
                    x_load(s + 1, k).start()

            with jax.named_scope("xwait"):
                @pl.when(t == 0)
                def _():
                    total(xbuf.at[lax.rem(s, 2)], xsem.at[lax.rem(s, 2)])

            with jax.named_scope("wwait"):
                total(wbuf.at[lax.rem(g, 2)], wsem.at[lax.rem(g, 2)])

            xslot, wslot, hslot = lax.rem(s, 2), lax.rem(g, 2), lax.rem(g, H_SLOTS)

            def part(h, carry):
                r = pl.ds(pl.multiple_of(h * part_rows, part_rows), part_rows)
                gu = jnp.dot(xbuf[xslot, r, :], wbuf[wslot], preferred_element_type=jnp.float32)
                gate = gu[:, :tn].astype(jnp.bfloat16).astype(jnp.float32)
                up = gu[:, tn:].astype(jnp.bfloat16).astype(jnp.float32)
                hout[hslot, h] = (jax.nn.silu(gate) * up).astype(jnp.bfloat16)
                return carry

            with jax.named_scope("gumm"):
                lax.fori_loop(0, 2, part, 0)
            h_write(g).start()

        @pl.when(g == 2 * nt)
        def _():
            all_sent()

        done, tiles = jnp.where(g == early, early, forwards(g - 1)), jnp.minimum(g + 1, ng)
        send(issued(done, jnp.minimum(g, ng)), issued(done, tiles))

        with jax.named_scope("fwd"):
            @pl.when(forwards(g) > done)
            def _():
                serve(done, tiles)

        @pl.when(g >= 1)
        def _():
            h_write(g - 1).wait()

        lax.fori_loop(z_done(g - 1), z_done(g), z_tile, 0)

        with jax.named_scope("fwd"):
            @pl.when(forwards(g) > done + 1)
            def _():
                serve(done + 1, tiles)

        return carry

    lax.fori_loop(0, ng, body, 0)

    tiles = jnp.int32(ng)

    def end_serve(j):
        with jax.named_scope("fwd"):
            serve(jnp.int32(j), tiles)

    lax.fori_loop(z_done(jnp.int32(ng - 1)), nsum, z_tile, 0)
    for j in range(ni - 2 * early, ni - 4):
        end_serve(j)
    h_write(ng - 1).wait()
    late(1)
    end_serve(ni - 4)
    late(2)
    end_serve(ni - 3)
    late(3)
    end_serve(ni - 2)
    end_serve(ni - 1)
    late(4)
    with jax.named_scope("harr"):
        total(hg.at[0, 0, :, pl.ds(ta, nt - ta)], hr.at[last_q + 3])
        total(zin.at[0], zr.at[2 * RING - 3])

    with jax.named_scope("drain"):
        for i in range(ni - 2, ni):
            total(hout.at[0], os.at[i % 8])
        for i in range(ni - 4, ni):
            h_fwd(jnp.int32(i)).wait_send()
        for z in range(max(0, nsum - Z_SLOTS), nsum):
            z_send(z).wait_send()
        for n in range(nz - 2, nz):
            o_write(jnp.int32(n), n % 2).wait()
        total(z_part, osem.at[2])


def _finish(hg, wd, zin, z_part, z_half, out, hz, wdb, zinb, accb, keep, res, hsem, wsem, zsem, asem, ksem, osem):
    rows, tn = hg.shape[4:]
    nz, _, zn = z_part.shape
    nt = hg.shape[3]
    ka = RING * tn * (nt - 2)
    b = lax.axis_index("dz")
    top, low = pl.ds(0, rows), pl.ds(rows, rows)

    for t in range(2):
        for k in range(RING):
            pltpu.make_async_copy(hg.at[b, k, 1, nt - 2 + t], hz.at[:, pl.ds((t * RING + k) * tn, tn)], hsem.at[0]).start()
    def cols(n):
        return pl.ds(pl.multiple_of(n * zn, 128), zn)

    def loads(n):
        return (
            pltpu.make_async_copy(wd.at[pl.ds(ka, 2 * RING * tn), cols(n)], wdb.at[n], wsem.at[n]),
            pltpu.make_async_copy(z_part.at[n], accb.at[n], asem.at[n]),
            pltpu.make_async_copy(zin.at[zin.shape[0] - 1, n], zinb.at[n], zsem.at[n]),
        )

    def fetch(n, carry):
        for copy in loads(n):
            copy.start()
        return carry

    lax.fori_loop(0, nz, fetch, 0)
    first = pltpu.make_async_copy(z_half, keep, ksem.at[0])
    first.start()
    pltpu.make_async_copy(hz, hz, hsem.at[0]).wait()

    def tile(n, carry):
        for copy in loads(n):
            copy.wait()
        acc = jnp.dot(hz[...], wdb[n], preferred_element_type=jnp.float32)
        res[n] = (acc + accb[n] + zinb[n]).astype(jnp.bfloat16)
        pltpu.make_async_copy(res.at[n], out.at[low, cols(n)], osem.at[0]).start()
        return carry

    lax.fori_loop(0, nz - 1, tile, 0)
    first.wait()
    second = pltpu.make_async_copy(keep, out.at[top], ksem.at[1])
    second.start()
    lax.fori_loop(nz - 1, nz, tile, 0)
    pltpu.make_async_copy(out.at[low], out.at[low], osem.at[0]).wait()
    second.wait()


def _local(x_blk, wg_blk, wu_blk, wd_blk):
    rows, kb = x_blk.shape
    hc = wg_blk.shape[1] // RING
    mc = wd_blk.shape[1]
    tn, zn = _tile(2 * hc, 256), _tile(2 * mc, 256)
    nt, nz = 2 * hc // tn, 2 * mc // zn
    bf16, f32 = jnp.bfloat16, jnp.float32
    hbm = pl.BlockSpec(memory_space=pl.ANY)
    half = rows // 2
    dma = pltpu.SemaphoreType.DMA
    flops = 2 * RING * rows * (RING * kb * 4 * hc + wd_blk.shape[0] * 2 * mc)
    res = pl.pallas_call(
        _kernel,
        name="ring_mlp",
        out_shape=(
            jax.ShapeDtypeStruct((half, 2 * mc), bf16),
            jax.ShapeDtypeStruct((nz, half, zn), f32),
            jax.ShapeDtypeStruct((RING, RING, rows, kb), bf16),
            jax.ShapeDtypeStruct((2, RING * kb, 2 * hc), bf16),
            jax.ShapeDtypeStruct((2, kb, hc), bf16),
            jax.ShapeDtypeStruct((RING, RING, 2, nt, half, tn), bf16),
            jax.ShapeDtypeStruct(wd_blk.shape, bf16),
            jax.ShapeDtypeStruct((wd_blk.shape[0], 2 * mc), bf16),
            jax.ShapeDtypeStruct((2 * (RING - 1), nz, half, zn), f32),
        ),
        in_specs=[hbm] * 4,
        out_specs=(hbm,) * 9,
        scratch_shapes=[
            pltpu.VMEM((2, rows, RING * kb), bf16),
            pltpu.VMEM((2, RING * kb, 2 * tn), bf16),
            pltpu.VMEM((2, half, wd_blk.shape[0]), bf16),
            pltpu.VMEM((WD_SLOTS, wd_blk.shape[0], zn), bf16),
            pltpu.VMEM((3, half, zn), f32),
            pltpu.VMEM((Z_SLOTS, half, zn), f32),
            pltpu.VMEM((nz, half, zn), f32),
            pltpu.VMEM((2, half, zn), bf16),
            pltpu.VMEM((H_SLOTS, 2, half, tn), bf16),
            dma((5,)), dma((N_RECV,)), dma((3,)), dma((3,)),
            dma((2,)), dma((2,)), dma((1,)), dma((WD_SLOTS,)), dma((3,)), dma((3,)),
            dma((8,)), dma((2 * RING * nt,)), dma((8,)), dma((2 * RING + 3,)), dma((2,)),
            dma((Z_SLOTS,)), dma((2 * (RING - 1),)),
        ],
        compiler_params=pltpu.CompilerParams(collective_id=0, has_side_effects=True, vmem_limit_bytes=67043328),
        cost_estimate=pl.CostEstimate(flops=flops, bytes_accessed=flops // 500, transcendentals=0),
    )(x_blk, wg_blk, wu_blk, wd_blk)
    z_half, z_part, hg, wd, zin = res[0], res[1], res[5], res[7], res[8]
    flops = 2 * half * 2 * RING * tn * 2 * mc
    return pl.pallas_call(
        _finish,
        name="last_part",
        out_shape=jax.ShapeDtypeStruct((rows, 2 * mc), bf16),
        in_specs=[hbm] * 5,
        out_specs=hbm,
        scratch_shapes=[
            pltpu.VMEM((half, 2 * RING * tn), bf16),
            pltpu.VMEM((nz, 2 * RING * tn, zn), bf16),
            pltpu.VMEM((nz, half, zn), f32),
            pltpu.VMEM((nz, half, zn), f32),
            pltpu.VMEM((half, 2 * mc), bf16),
            pltpu.VMEM((nz, half, zn), bf16),
            dma((1,)), dma((nz,)), dma((nz,)), dma((nz,)), dma((2,)), dma((1,)),
        ],
        compiler_params=pltpu.CompilerParams(vmem_limit_bytes=67043328),
        cost_estimate=pl.CostEstimate(flops=flops, bytes_accessed=flops // 500, transcendentals=0),
    )(hg, wd, zin, z_part, z_half)


def solution(mesh):
    assert mesh.shape["dz"] == RING and mesh.shape["dy"] == RING and mesh.shape["dx"] == 2
    x_spec = P(("grp", "dx", "dz"), "dy")
    w_in_spec = P("dy", ("dz", "dx"))
    w_out_spec = P("dz", ("dy", "dx"))
    return jax.shard_map(_local, mesh=mesh, in_specs=(x_spec, w_in_spec, w_in_spec, w_out_spec), out_specs=x_spec, check_vma=False)
```

```python
import jax
import jax.numpy as jnp
from jax import lax
from jax.experimental import pallas as pl
from jax.experimental.pallas import tpu as pltpu
from jax.sharding import PartitionSpec as P

MESH = pl.DeviceIdType.MESH
RING = 4
H_SLOTS = 7
Z_SLOTS = 6
AHEAD, AHEAD_LAST = 3, 2
WD_SLOTS = 3
XL, XS, XF, YL, YS, YF, WN, W2, WF, WL, SW, SD, YH, P1 = 0, 2, 3, 5, 9, 13, 17, 21, 25, 29, 33, 49, 50, 52
JOINT = (
    (XF, XF + 1), (YH, YH + 1), tuple(range(YS, YF)), tuple(range(YF, WN)), (WN, WN + 1), (WN + 2, WN + 3), (WF, WF + 1),
    tuple(SW + 4 * j + u for j in range(RING) for u in range(2)), tuple(SW + 4 * j + 2 + u for j in range(RING) for u in range(2)),
)
RECV = {}
for _i in range(P1):
    _group = next((g for g in JOINT if _i in g), (_i,))
    RECV[_i] = RECV[_group[0]] if _i != _group[0] else len(set(RECV.values()))
N_RECV = len(set(RECV.values()))


def _tile(extent, most):
    return next(t for t in range(most, 0, -128) if extent % t == 0)


def _kernel(x_in, wg_in, wu_in, wd_in, z_half, z_part, xg, wgu, ws, hg, wds, wd, zin,
            xbuf, wbuf, hz, wdbuf, zinb, zout, zacc, ofin, hout,
            p1s, p1r, bin_s, bout_s, xsem, wsem, hzsem, wdsem, zinsem, osem,
            os, olr, fs, hr, hws, zs, zr):
    rows, kb = x_in.shape
    hc = wg_in.shape[1] // RING
    nloc = wg_in.shape[1]
    hq = 2 * hc
    mc = wd_in.shape[1]
    part_rows, tn = hout.shape[2:]
    zn = zout.shape[2]
    nt = hq // tn
    nz = 2 * mc // zn
    ng = RING * nt
    ni = 2 * ng
    zstart = nt + 2
    early = (nt + 1) // 2
    pc = (early * tn // 2, hc - early * tn // 2)
    p_src, p_dst = (0, pc[0]), (0, 2 * pc[0])

    b = lax.axis_index("dz")
    a = lax.axis_index("dy")
    c = lax.axis_index("dx")
    step = 1 - 2 * c
    al = lax.rem(a + step + RING, RING)
    ash = lax.rem(a - step + RING, RING)
    a2 = lax.rem(a + 2, RING)
    bl = lax.rem(b + step + RING, RING)
    bsh = lax.rem(b - step + RING, RING)
    xl, xs_ = {"dy": al}, {"dy": ash}
    yl, ys_ = {"dz": bl}, {"dz": bsh}
    sib = {"dx": 1 - c}
    kbs = (a, ash, al, a2)
    w_in = (wg_in, wu_in)

    def dest(s):
        return lax.rem(b - step * (1 + s) + 2 * RING, RING)

    def rc(src, dst, ss, rs, dev):
        return pltpu.make_async_remote_copy(src_ref=src, dst_ref=dst, send_sem=ss, recv_sem=rs, device_id=dev, device_id_type=MESH)

    def lanes(i, n):
        return pl.ds(pl.multiple_of(i * n, 128), n)

    def krows(k):
        return pl.ds(pl.multiple_of(k * kb, 16), kb)

    half = rows // 2

    def w_piece(u, p, q):
        return w_in[u].at[:, pl.ds(pl.multiple_of(q * hc + p_src[p], 128), pc[p])]

    def w_place(u, p, k):
        return wgu.at[u, krows(k), pl.ds(pl.multiple_of(p_dst[p] + c * pc[p], 128), pc[p])]

    def p1(i):
        kind = 0 if i < YL else 1 if i < WN or i >= YH else 2 if i < SW else 3 if i < SD else 4
        sem = (p1s.at[kind], p1r.at[RECV[i]])
        if i >= YH:
            r = pl.ds((i - YH) * half, half)
            return rc(xg.at[b, ash, r], xg.at[b, ash, r], *sem, yl)
        if i < XS:
            r = pl.ds((i - XL) * half, half)
            return rc(x_in.at[r], xg.at[b, a, r], *sem, xl)
        if i < XF:
            return rc(x_in, xg.at[b, a], *sem, xs_)
        if i < YL:
            r = pl.ds((i - XF) * half, half)
            return rc(xg.at[b, ash, r], xg.at[b, ash, r], *sem, xl)
        if i < YF:
            j = (i - YL) % RING
            src = x_in if j == 0 else xg.at[b, kbs[j]]
            return rc(src, xg.at[b, kbs[j]], *sem, yl if i < YS else ys_)
        if i < WN:
            j = i - YF
            return rc(xg.at[bsh, kbs[j]], xg.at[bsh, kbs[j]], *sem, yl)
        if i < WF:
            u, p = (i - WN) % 2, (i - WN) % 4 // 2
            if i < W2:
                return rc(w_piece(u, p, ash), w_place(u, p, a), *sem, xs_)
            return rc(w_piece(u, p, a2), ws.at[u, :, pl.ds(p_src[p], pc[p])], *sem, xl)
        if i < WL:
            u, p = (i - WF) % 2, (i - WF) // 2
            return rc(ws.at[u, :, pl.ds(p_src[p], pc[p])], w_place(u, p, ash), *sem, xl)
        if i < SW:
            u, p = (i - WL) % 2, (i - WL) // 2
            return rc(w_piece(u, p, al), w_place(u, p, a), *sem, xl)
        if i < SD:
            j, p, u = (i - SW) // 4, (i - SW) % 4 // 2, (i - SW) % 2
            dst = w_place(u, p, kbs[j])
            return rc(w_piece(u, p, a) if j == 0 else dst, dst, *sem, sib)
        return rc(wd_in, wds, *sem, sib)

    def go(*idx):
        for i in idx:
            p1(i).start()

    def got(*idx):
        for i in idx:
            with jax.named_scope(f"got{i}"):
                p1(i).wait_recv()

    def total(ref, sem):
        pltpu.make_async_copy(ref, ref, sem).wait()

    def got_all(first, ref):
        with jax.named_scope(f"got{first}"):
            total(ref, p1r.at[RECV[first]])

    def part_of(u_refs, p):
        return u_refs.at[:, :, pl.ds(p_src[p], pc[p])]

    def all_sent():
        quarter = wgu.at[:, :, pl.ds(0, hc)]
        for kind, ref in enumerate((xg.at[0, pl.ds(0, 3)], xg.at[pl.ds(0, 3)], quarter, quarter, wds)):
            total(ref, p1s.at[kind])

    barrier = pltpu.get_barrier_semaphore()
    for dev in (xl, xs_, yl, ys_, sib):
        pl.semaphore_signal(barrier, inc=1, device_id=dev, device_id_type=MESH)
    with jax.named_scope("barrier"):
        pl.semaphore_wait(barrier, 5)

    go(XL, XL + 1, XS, YL, YS, SD, SW, SW + 1, SW + 2, SW + 3, WN, WN + 1)

    def bounce(*classes):
        for i, (size, moves) in enumerate(classes):
            for src, mid, _ in moves:
                pltpu.make_async_copy(src, mid, bin_s.at[i]).start()
        for i, (size, moves) in enumerate(classes):
            total(size, bin_s.at[i])
            for _, _, parts in moves:
                for piece, dst in parts:
                    pltpu.make_async_copy(piece, dst, bout_s.at[i]).start()
        for i, (size, moves) in enumerate(classes):
            total(size, bout_s.at[i])

    def w_down_moves(src, core):
        moves = []
        for cc in range(2):
            for k in range(RING):
                cols = pl.ds((cc * RING + k) * mc, mc)
                parts = []
                for p in range(2):
                    at, end = p_dst[p] + cc * pc[p], p_dst[p] + (cc + 1) * pc[p]
                    while at < end:
                        n = min(end, (at // tn + 1) * tn) - at
                        row = p_src[p] + at - p_dst[p] - cc * pc[p]
                        dst = wd.at[pl.ds((at // tn * RING + k) * tn + at % tn, n), lanes(core, mc)]
                        parts.append((xbuf.at[1, pl.ds(row, n), cols], dst))
                        at += n
                moves.append((src.at[pl.ds(cc * nloc + k * hc, hc)], xbuf.at[1, pl.ds(0, hc), cols], parts))
        return moves

    x_moves = [(x_in, xbuf.at[0, :, pl.ds(0, kb)], [(xbuf.at[0, :, pl.ds(0, kb)], xg.at[b, a])])]
    w_moves, col = [], kb
    for u in range(2):
        for r0 in range(0, kb, rows):
            n = min(rows, kb - r0)
            parts = []
            for p in range(2):
                dst = wgu.at[u, pl.ds(pl.multiple_of(a * kb + r0, 16), n), pl.ds(pl.multiple_of(p_dst[p] + c * pc[p], 128), pc[p])]
                parts.append((xbuf.at[0, pl.ds(0, n), pl.ds(col + p_src[p], pc[p])], dst))
            w_moves.append((w_in[u].at[pl.ds(r0, n), lanes(a, hc)], xbuf.at[0, pl.ds(0, n), pl.ds(col, hc)], parts))
            col += hc
    with jax.named_scope("bounce"):
        bounce((x_in, x_moves), (ws, w_moves), (wd_in, w_down_moves(wd_in, c)))
        zinb[...] = jnp.zeros_like(zinb)

    got(XL)
    go(XF, YH)
    got(XL + 1)
    go(XF + 1, W2, W2 + 1, YH + 1)
    got(XS)
    go(YL + 2, WN + 2, WN + 3)
    got(YL)
    go(YF)
    got_all(XF, xg.at[0, 0])
    go(YL + 3, WL)
    got_all(YH, xg.at[0, 0])
    go(YF + 1)
    got(SD)
    with jax.named_scope("bounce"):
        bounce((wds, w_down_moves(wds, 1 - c)))
    got(W2)
    go(WF)
    got(W2 + 1)
    go(WF + 1, WL + 1, W2 + 2, W2 + 3)
    got(YL + 2)
    go(YF + 2)
    got_all(WN, part_of(ws, 0))
    go(SW + 8, SW + 9)
    got(YL + 3)
    go(YF + 3)
    got(WL)
    go(SW + 4)
    got_all(WF, part_of(ws, 0))
    go(SW + 12, SW + 13)
    got(WL + 1)
    go(SW + 5, WL + 2, YS + 1)
    got(W2 + 2)
    go(WF + 2)
    got(W2 + 3)
    go(WF + 3, WL + 3)

    def x_load(s, k):
        return pltpu.make_async_copy(xg.at[dest(s), k], xbuf.at[lax.rem(s, 2), :, pl.ds(k * kb, kb)], xsem.at[lax.rem(s, 2)])

    def w_load(g, u):
        slot = lax.rem(g, 2)
        return pltpu.make_async_copy(wgu.at[u, :, lanes(lax.rem(g, nt), tn)], wbuf.at[slot, :, pl.ds(u * tn, tn)], wsem.at[slot])

    assert nt >= 4
    nsum = 2 * (RING - 1) * nz
    ta, first_q, last_q = nt - 2, 2 * RING - 2, 2 * RING - 1
    spans = ((0, nt), (0, ta), (ta, nt), (0, ta - 1), (ta - 1, ta))
    wd_rows = [pl.ds(lo * RING * tn, (hi - lo) * RING * tn) for lo, hi in spans]


    def wd_load(w, kind):
        slot = lax.rem(w, WD_SLOTS)
        return pltpu.make_async_copy(wd.at[wd_rows[kind], lanes(lax.rem(w, nz), zn)], wdbuf.at[slot, wd_rows[kind]], wdsem.at[slot])

    def wd_fetch(w):
        for kind in range(5):
            lo, hi = (nsum + (kind - 1) * nz, nsum + kind * nz) if kind else (0, nsum)

            @pl.when((w >= lo) & (w < hi))
            def _():
                wd_load(w, kind).start()

    def zin_load(z, slot):
        return pltpu.make_async_copy(zin.at[z // nz - 2, lax.rem(z, nz)], zinb.at[slot], zinsem.at[slot])

    def pairs(s):
        return jnp.maximum(early - s, 0)

    def item_of(s, h, t):
        m = pairs(s)
        return 2 * nt * s + jnp.where(t < m, 2 * t + h, 2 * m + h * (nt - m) + t - m)

    def place_of(i):
        s, v = i // (2 * nt), lax.rem(i, 2 * nt)
        m = pairs(s)
        w = jnp.maximum(v - 2 * m, 0)
        late = jnp.where(w >= nt - m, 1, 0)
        h = jnp.where(v < 2 * m, lax.rem(v, 2), late)
        t = jnp.where(v < 2 * m, v // 2, m + w - late * (nt - m))
        return s, h, t

    def h_write(g):
        slot = lax.rem(g, H_SLOTS)
        return pltpu.make_async_copy(hout.at[slot], hg.at[dest(g // nt), a, :, lax.rem(g, nt)], hws.at[lax.rem(g, 2)])

    def half_of(s, h, t):
        q = 2 * s + h
        first = jnp.where((q == first_q) & (t >= ta), 1, 0)
        last = jnp.where(q == last_q, 1 + jnp.where(t >= ta - 1, 1, 0) + jnp.where(t >= ta, 1, 0), 0)
        return q + first + last

    def h_long(i):
        s, h, t = place_of(i)
        return rc(hout.at[lax.rem(s * nt + t, H_SLOTS), h], hg.at[dest(s), a, h, t], os.at[lax.rem(i, 8)], olr.at[i], xl)

    def h_short(i):
        s, h, t = place_of(i)
        return rc(hout.at[lax.rem(s * nt + t, H_SLOTS), h], hg.at[dest(s), a, h, t], os.at[lax.rem(i, 8)], hr.at[half_of(s, h, t)], xs_)

    def h_fwd(i):
        s, h, t = place_of(i)
        blk = hg.at[dest(s), ash, h, t]
        return rc(blk, blk, fs.at[lax.rem(i, 8)], hr.at[half_of(s, h, t)], xl)

    def ready(tiles):
        s, r = tiles // nt, lax.rem(tiles, nt)
        m = pairs(s)
        return 2 * nt * s + jnp.where(r <= m, 2 * r, m + r)

    cut = ni - 12

    def issued(forwards, tiles):
        ahead = jnp.where(forwards < cut, forwards + AHEAD, jnp.maximum(forwards + AHEAD_LAST, cut + AHEAD - 1))
        return jnp.minimum(ahead, ready(tiles))

    def send(lo, hi):
        def one(i, carry):
            h_long(i).start()
            h_short(i).start()
            return carry

        lax.fori_loop(lo, hi, one, 0)

    def forwards(g):
        return jnp.where(g < early, 0, jnp.minimum(jnp.maximum(early, 2 * (g - early) + 2), ni))

    def serve(j, tiles):
        h_long(j).wait_recv()
        h_fwd(j).start()
        send(issued(j, tiles), issued(j + 1, tiles))

        @pl.when(j >= 2)
        def _():
            total(hout.at[0], os.at[lax.rem(j - 2, 8)])

        @pl.when(j >= 4)
        def _():
            h_fwd(j - 4).wait_send()

    def pull(q, sem, lo, hi):
        s, h = q // 2, lax.rem(q, 2)
        total(hg.at[0, 0, :, pl.ds(lo, hi - lo)], hr.at[sem])

        def one(t, carry):
            for k in range(RING):
                pltpu.make_async_copy(hg.at[dest(s), k, h, t], hz.at[lax.rem(q, 2), :, lanes(t * RING + k, tn)], hzsem.at[0]).start()
            return carry

        lax.fori_loop(lo, hi, one, 0)

    def pulled(q, lo, hi):
        total(hz.at[lax.rem(q, 2), :, pl.ds(lo * RING * tn, (hi - lo) * RING * tn)], hzsem.at[0])

    def z_send(z):
        slot = lax.rem(z, Z_SLOTS)
        return rc(zout.at[slot], zin.at[z // nz, lax.rem(z, nz)], zs.at[slot], zr.at[z // nz], yl)

    def o_write(z, slot):
        return pltpu.make_async_copy(ofin.at[slot], z_half.at[:, lanes(lax.rem(z, nz), zn)], osem.at[slot])

    def start_w(g):
        w_load(g, 0).start()
        w_load(g, 1).start()

    for k in range(RING):
        x_load(0, k).start()
    got_all(SW, wgu.at[:, :, pl.ds(p_dst[0], pc[0])])
    start_w(0)

    def z_tile(z, carry):
        q, wslot = z // nz, lax.rem(z, WD_SLOTS)
        wd_fetch(z + 2)

        @pl.when(lax.rem(z, nz) == 0)
        def _():
            with jax.named_scope("zinrecv"):
                @pl.when(q >= 2)
                def _():
                    total(zin.at[0], zr.at[q - 2])
                    for y in range(2):
                        zin_load(z + y, lax.rem(z + y, 3)).start()

            with jax.named_scope("harr"):
                pull(q, q, 0, nt)
            with jax.named_scope("hzload"):
                pulled(q, 0, nt)

        @pl.when((q >= 2) & ((z + 2) // nz == q))
        def _():
            zin_load(z + 2, lax.rem(z + 2, 3)).start()

        with jax.named_scope("wdwait"):
            wd_load(z, 0).wait()

        with jax.named_scope("zinwait"):
            @pl.when(q >= 2)
            def _():
                zin_load(z, lax.rem(z, 3)).wait()

        with jax.named_scope("zslot"):
            @pl.when(z >= Z_SLOTS)
            def _():
                z_send(z - Z_SLOTS).wait_send()

        with jax.named_scope("zmm"):
            acc = jnp.dot(hz[lax.rem(q, 2)], wdbuf[wslot], preferred_element_type=jnp.float32)
            zout[lax.rem(z, Z_SLOTS)] = acc + zinb[lax.rem(z, 3)]

        z_send(z).start()
        return carry

    def late(kind):
        base = nsum + (kind - 1) * nz
        h = 0 if kind < 3 else 1

        def tile(n, carry):
            w = base + n
            wd_fetch(w + 2)
            if kind == 2:
                z = nsum + n

                @pl.when(n + 2 < nz)
                def _():
                    zin_load(z + 2, lax.rem(n + 2, 3)).start()

            wd_load(w, kind).wait()
            if kind == 2:
                zin_load(z, lax.rem(n, 3)).wait()

                @pl.when(n >= 2)
                def _():
                    o_write(n - 2, lax.rem(n, 2)).wait()

            with jax.named_scope(f"late{kind}"):
                acc = jnp.dot(hz[h, :, wd_rows[kind]], wdbuf[lax.rem(w, WD_SLOTS), wd_rows[kind]], preferred_element_type=jnp.float32)
                if kind in (1, 3):
                    zacc[n] = acc
                elif kind == 2:
                    ofin[lax.rem(n, 2)] = (acc + zacc[n] + zinb[lax.rem(n, 3)]).astype(jnp.bfloat16)
                else:
                    zacc[n] += acc
            if kind == 2:
                o_write(n, lax.rem(n, 2)).start()
            if kind == 4:
                pltpu.make_async_copy(zacc.at[n], z_part.at[n], osem.at[2]).start()
            return carry

        with jax.named_scope("harr"):
            pull(jnp.int32(first_q + h), first_q + kind - 1, *spans[kind])
            if kind == 2:
                total(zin.at[0], zr.at[2 * RING - 4])
                for y in range(2):
                    zin_load(jnp.int32(nsum + y), y).start()
        with jax.named_scope("hzload"):
            pulled(first_q + h, *spans[kind])
        lax.fori_loop(0, nz, tile, 0)

    def z_done(g):
        q, k = jnp.maximum(g - zstart, 0), g - zstart - 2 * nt + 1
        steady = 2 * nz * (q // nt) + 2 * nz * (lax.rem(q, nt) + 1) // nt
        ending = 4 * nz + nz * k // 2
        return jnp.where(g < zstart, 0, jnp.where(k > 0, ending, steady))

    def body(g, carry):
        s, t = g // nt, lax.rem(g, nt)

        @pl.when(g == early - 1)
        def _():
            got_all(WN + 2, part_of(ws, 1))
            go(SW + 10, SW + 11)
            got(WL + 2)
            go(SW + 6)
            got(WF + 2)
            go(SW + 14)

        @pl.when(g == early)
        def _():
            got(WF + 3)
            go(SW + 15)
            got(WL + 3)
            go(SW + 7, YS + 2, YS + 3)

            def first(j, carry):
                serve(j, early)
                return carry

            lax.fori_loop(0, early, first, 0)
            got_all(SW + 2, wgu.at[:, :, pl.ds(p_dst[1], pc[1])])
            start_w(g)
            wd_load(0, 0).start()
            wd_load(1, 0).start()

        @pl.when(g < ng)
        def _():
            @pl.when((g + 1 < ng) & (g + 1 != early))
            def _():
                start_w(g + 1)

            @pl.when((t == nt - 1) & (g + 1 < ng))
            def _():
                @pl.when(s + 1 == 1)
                def _():
                    got_all(YF, xg.at[0])

                @pl.when(s + 1 == 2)
                def _():
                    got_all(YS, xg.at[0])

                for k in range(RING):
                    x_load(s + 1, k).start()

            with jax.named_scope("xwait"):
                @pl.when(t == 0)
                def _():
                    total(xbuf.at[lax.rem(s, 2)], xsem.at[lax.rem(s, 2)])

            with jax.named_scope("wwait"):
                total(wbuf.at[lax.rem(g, 2)], wsem.at[lax.rem(g, 2)])

            xslot, wslot, hslot = lax.rem(s, 2), lax.rem(g, 2), lax.rem(g, H_SLOTS)

            def part(h, carry):
                r = pl.ds(pl.multiple_of(h * part_rows, part_rows), part_rows)
                gu = jnp.dot(xbuf[xslot, r, :], wbuf[wslot], preferred_element_type=jnp.float32)
                gate = gu[:, :tn].astype(jnp.bfloat16).astype(jnp.float32)
                up = gu[:, tn:].astype(jnp.bfloat16).astype(jnp.float32)
                hout[hslot, h] = (jax.nn.silu(gate) * up).astype(jnp.bfloat16)
                return carry

            with jax.named_scope("gumm"):
                lax.fori_loop(0, 2, part, 0)
            h_write(g).start()

        @pl.when(g == 2 * nt)
        def _():
            all_sent()

        done, tiles = jnp.where(g == early, early, forwards(g - 1)), jnp.minimum(g + 1, ng)
        send(issued(done, jnp.minimum(g, ng)), issued(done, tiles))

        with jax.named_scope("fwd"):
            @pl.when(forwards(g) > done)
            def _():
                serve(done, tiles)

        @pl.when(g >= 1)
        def _():
            h_write(g - 1).wait()

        lax.fori_loop(z_done(g - 1), z_done(g), z_tile, 0)

        with jax.named_scope("fwd"):
            @pl.when(forwards(g) > done + 1)
            def _():
                serve(done + 1, tiles)

        return carry

    lax.fori_loop(0, ng, body, 0)

    tiles = jnp.int32(ng)

    def end_serve(j):
        with jax.named_scope("fwd"):
            serve(jnp.int32(j), tiles)

    lax.fori_loop(z_done(jnp.int32(ng - 1)), nsum, z_tile, 0)
    for j in range(ni - 2 * early, ni - 4):
        end_serve(j)
    h_write(ng - 1).wait()
    late(1)
    end_serve(ni - 4)
    late(2)
    end_serve(ni - 3)
    late(3)
    end_serve(ni - 2)
    end_serve(ni - 1)
    late(4)
    with jax.named_scope("drain"):
        for i in range(ni - 2, ni):
            total(hout.at[0], os.at[i % 8])
        for i in range(ni - 4, ni):
            h_fwd(jnp.int32(i)).wait_send()
        for z in range(max(0, nsum - Z_SLOTS), nsum):
            z_send(z).wait_send()
        for n in range(nz - 2, nz):
            o_write(jnp.int32(n), n % 2).wait()

    with jax.named_scope("harr"):
        total(hg.at[0, 0, :, pl.ds(ta, nt - ta)], hr.at[last_q + 3])
        total(zin.at[0], zr.at[2 * RING - 3])
        total(z_part, osem.at[2])


def _finish(hg, wd, zin, z_part, z_half, out, hz, wdb, zinb, accb, keep, res, hsem, wsem, zsem, asem, ksem, osem):
    rows, tn = hg.shape[4:]
    nz, _, zn = z_part.shape
    nt = hg.shape[3]
    ka = RING * tn * (nt - 2)
    b = lax.axis_index("dz")
    top, low = pl.ds(0, rows), pl.ds(rows, rows)

    for t in range(2):
        for k in range(RING):
            pltpu.make_async_copy(hg.at[b, k, 1, nt - 2 + t], hz.at[:, pl.ds((t * RING + k) * tn, tn)], hsem.at[0]).start()
    def cols(n):
        return pl.ds(pl.multiple_of(n * zn, 128), zn)

    def loads(n):
        return (
            pltpu.make_async_copy(wd.at[pl.ds(ka, 2 * RING * tn), cols(n)], wdb.at[n], wsem.at[n]),
            pltpu.make_async_copy(z_part.at[n], accb.at[n], asem.at[n]),
            pltpu.make_async_copy(zin.at[zin.shape[0] - 1, n], zinb.at[n], zsem.at[n]),
        )

    def fetch(n, carry):
        for copy in loads(n):
            copy.start()
        return carry

    lax.fori_loop(0, nz, fetch, 0)
    first = pltpu.make_async_copy(z_half, keep, ksem.at[0])
    first.start()
    pltpu.make_async_copy(hz, hz, hsem.at[0]).wait()

    def tile(n, carry):
        for copy in loads(n):
            copy.wait()
        acc = jnp.dot(hz[...], wdb[n], preferred_element_type=jnp.float32)
        res[n] = (acc + accb[n] + zinb[n]).astype(jnp.bfloat16)
        pltpu.make_async_copy(res.at[n], out.at[low, cols(n)], osem.at[0]).start()
        return carry

    lax.fori_loop(0, nz - 1, tile, 0)
    first.wait()
    second = pltpu.make_async_copy(keep, out.at[top], ksem.at[1])
    second.start()
    lax.fori_loop(nz - 1, nz, tile, 0)
    pltpu.make_async_copy(out.at[low], out.at[low], osem.at[0]).wait()
    second.wait()


def _local(x_blk, wg_blk, wu_blk, wd_blk):
    rows, kb = x_blk.shape
    hc = wg_blk.shape[1] // RING
    mc = wd_blk.shape[1]
    tn, zn = _tile(2 * hc, 256), _tile(2 * mc, 256)
    nt, nz = 2 * hc // tn, 2 * mc // zn
    bf16, f32 = jnp.bfloat16, jnp.float32
    hbm = pl.BlockSpec(memory_space=pl.ANY)
    half = rows // 2
    dma = pltpu.SemaphoreType.DMA
    flops = 2 * RING * rows * (RING * kb * 4 * hc + wd_blk.shape[0] * 2 * mc)
    res = pl.pallas_call(
        _kernel,
        name="ring_mlp",
        out_shape=(
            jax.ShapeDtypeStruct((half, 2 * mc), bf16),
            jax.ShapeDtypeStruct((nz, half, zn), f32),
            jax.ShapeDtypeStruct((RING, RING, rows, kb), bf16),
            jax.ShapeDtypeStruct((2, RING * kb, 2 * hc), bf16),
            jax.ShapeDtypeStruct((2, kb, hc), bf16),
            jax.ShapeDtypeStruct((RING, RING, 2, nt, half, tn), bf16),
            jax.ShapeDtypeStruct(wd_blk.shape, bf16),
            jax.ShapeDtypeStruct((wd_blk.shape[0], 2 * mc), bf16),
            jax.ShapeDtypeStruct((2 * (RING - 1), nz, half, zn), f32),
        ),
        in_specs=[hbm] * 4,
        out_specs=(hbm,) * 9,
        scratch_shapes=[
            pltpu.VMEM((2, rows, RING * kb), bf16),
            pltpu.VMEM((2, RING * kb, 2 * tn), bf16),
            pltpu.VMEM((2, half, wd_blk.shape[0]), bf16),
            pltpu.VMEM((WD_SLOTS, wd_blk.shape[0], zn), bf16),
            pltpu.VMEM((3, half, zn), f32),
            pltpu.VMEM((Z_SLOTS, half, zn), f32),
            pltpu.VMEM((nz, half, zn), f32),
            pltpu.VMEM((2, half, zn), bf16),
            pltpu.VMEM((H_SLOTS, 2, half, tn), bf16),
            dma((5,)), dma((N_RECV,)), dma((3,)), dma((3,)),
            dma((2,)), dma((2,)), dma((1,)), dma((WD_SLOTS,)), dma((3,)), dma((3,)),
            dma((8,)), dma((2 * RING * nt,)), dma((8,)), dma((2 * RING + 3,)), dma((2,)),
            dma((Z_SLOTS,)), dma((2 * (RING - 1),)),
        ],
        compiler_params=pltpu.CompilerParams(collective_id=0, has_side_effects=True, vmem_limit_bytes=67043328),
        cost_estimate=pl.CostEstimate(flops=flops, bytes_accessed=flops // 500, transcendentals=0),
    )(x_blk, wg_blk, wu_blk, wd_blk)
    z_half, z_part, hg, wd, zin = res[0], res[1], res[5], res[7], res[8]
    flops = 2 * half * 2 * RING * tn * 2 * mc
    return pl.pallas_call(
        _finish,
        name="last_part",
        out_shape=jax.ShapeDtypeStruct((rows, 2 * mc), bf16),
        in_specs=[hbm] * 5,
        out_specs=hbm,
        scratch_shapes=[
            pltpu.VMEM((half, 2 * RING * tn), bf16),
            pltpu.VMEM((nz, 2 * RING * tn, zn), bf16),
            pltpu.VMEM((nz, half, zn), f32),
            pltpu.VMEM((nz, half, zn), f32),
            pltpu.VMEM((half, 2 * mc), bf16),
            pltpu.VMEM((nz, half, zn), bf16),
            dma((1,)), dma((nz,)), dma((nz,)), dma((nz,)), dma((2,)), dma((1,)),
        ],
        compiler_params=pltpu.CompilerParams(vmem_limit_bytes=67043328),
        cost_estimate=pl.CostEstimate(flops=flops, bytes_accessed=flops // 500, transcendentals=0),
    )(hg, wd, zin, z_part, z_half)


def solution(mesh):
    assert mesh.shape["dz"] == RING and mesh.shape["dy"] == RING and mesh.shape["dx"] == 2
    x_spec = P(("grp", "dx", "dz"), "dy")
    w_in_spec = P("dy", ("dz", "dx"))
    w_out_spec = P("dz", ("dy", "dx"))
    return jax.shard_map(_local, mesh=mesh, in_specs=(x_spec, w_in_spec, w_in_spec, w_out_spec), out_specs=x_spec, check_vma=False)
```
